32 devices in a mesh: group: 4 (over y, core), dev: 8 (over z, x).
Axes of the slice: x: 2, y: 2, z: 4, core: 2. Of those that a mesh axis runs over, the one named last changes fastest.
Arguments:
- solution: float32 [4, 16, 16, 512], P('group', 'dev'), may hold values from -6 to 6
- residual: float32 [4, 16, 16, 512], P('group', 'dev'), may hold values from -6 to 6
- direction: float32 [4, 16, 16, 512], P('group', 'dev'), may hold values from -0.03 to 0.03
- geometry: bfloat16 [3, 4, 16, 16, 512], P(None, 'group', 'dev'), may hold values from 0.5 to 2
- mass: bfloat16 [4, 16, 16, 512], P('group', 'dev'), may hold values from 50 to 500
Outputs:
- solution_out: float32 [4, 16, 16, 512], P('group', 'dev')
- residual_out: float32 [4, 16, 16, 512], P('group', 'dev')
- direction_out: float32 [4, 16, 16, 512], P('group', 'dev')
The draws below stay inside these ranges and needn't reach their ends.
All inputs are finite; a program needn't handle non-finite values.
Results may differ from the reference program's by a relative error of at most 0.0003.
Values sent between devices are 32-bit elements; how exact they have to be, the bound alone decides.
A program may use at most 64 MiB of HBM per device.

```python
import math
import jax
import jax.numpy as jnp
import numpy as np
from jax import lax

NP = 8
EZ = 16
EA = 4
EB = 16


def draw_direction(key, part):
    position = jnp.arange(EA, dtype=jnp.float32) / max(EA - 1, 1)
    shape = (EA, EB, EZ, NP ** 3)
    noise = jnp.clip(jax.random.normal(key, shape, jnp.float32), -6.0, 6.0)
    rise = jnp.power(4.0, position)
    return (0.001 * rise[:, None, None, None] * noise).astype(jnp.float32)


def level_of(stream_key, dims, split, least, largest):
    factor_of, own = 1.0, jax.random.fold_in(stream_key, 6)
    for dim, parts in split:
        steps = jnp.exp(jax.random.uniform(jax.random.fold_in(own, dim), (parts,), jnp.float32, least / len(split), largest / len(split)))
        factor_of = factor_of * jnp.repeat(steps, dims[dim] // parts).reshape([-1 if axis == dim else 1 for axis in range(len(dims))])
    return factor_of


def centred(key, dims, deviation, limit, shards=(), kind=jnp.bfloat16):
    entries = deviation * jax.random.normal(key, dims, jnp.float32)
    if shards:
        entries = entries * level_of(key, dims, shards, -0.22, 0.18)
    return jnp.clip(entries, -limit, limit).astype(kind)


def setup_inputs(seed: int = 0) -> dict:
    splits = jax.random.split(jax.random.key(seed), 6)
    solution = centred(splits[0], (EA, EB, EZ, NP ** 3), 1.0, 6.0, ((0, 4), (1, 8)), jnp.float32)
    residual = centred(splits[1], (EA, EB, EZ, NP ** 3), 1.0, 6.0, ((0, 4), (1, 8)), jnp.float32)
    direction = draw_direction(jax.random.fold_in(splits[5], 71), 0)
    geometry = jnp.clip(jnp.exp(math.log(2.0) - 1.3862944 * jax.random.uniform(splits[3], (3, EA, EB, EZ, NP ** 3), jnp.float32) ** level_of(splits[3], (3, EA, EB, EZ, NP ** 3), ((1, 4), (2, 8)), -0.2, 0.2)), 0.5, 2.0).astype(jnp.bfloat16)
    mass = jnp.clip(jnp.exp(math.log(500.0) - 2.3025851 * jax.random.uniform(splits[4], (EA, EB, EZ, NP ** 3), jnp.float32) ** level_of(splits[4], (EA, EB, EZ, NP ** 3), ((0, 4), (1, 8)), -0.2, 0.2)), 50.0, 500.0).astype(jnp.bfloat16)
    return {"solution": solution, "residual": residual, "direction": direction, "geometry": geometry, "mass": mass}


lobatto_nodes = [-1.0, -0.8717401485096066, -0.5917001814331423, -0.2092992179024789,
                 0.2092992179024789, 0.5917001814331423, 0.8717401485096066, 1.0]


def derivative_table():
    nodes = np.array(lobatto_nodes)
    identity = np.eye(NP)
    offset = nodes[:, None] - nodes[None, :] + identity
    barycentric = 1.0 / np.prod(offset, axis=1)
    derivative = (barycentric[None, :] / barycentric[:, None]) / offset * (1.0 - identity)
    return derivative - identity * np.sum(derivative, axis=1)[:, None]


def operator_tables():
    derivative = derivative_table()
    identity = np.eye(NP)
    kron_list = [np.kron(np.kron(derivative, identity), identity),
                 np.kron(np.kron(identity, derivative), identity),
                 np.kron(np.kron(identity, identity), derivative)]
    forward = np.concatenate([matrix.T for matrix in kron_list], axis=1)
    backward = np.concatenate(kron_list, axis=0)
    squares = np.concatenate([matrix * matrix for matrix in kron_list], axis=0)
    return (jnp.asarray(forward, dtype=jnp.float32), jnp.asarray(backward, dtype=jnp.float32),
            jnp.asarray(squares, dtype=jnp.float32))


def point_weights():
    edge = np.where(np.arange(NP) % (NP - 1) == 0, 0.5, 1.0)
    return jnp.asarray(np.kron(np.kron(edge, edge), edge), dtype=jnp.float32)


def highest(left, right):
    return jnp.dot(left, right, precision=lax.Precision.HIGHEST, preferred_element_type=jnp.float32)


def face_pass(field, elem_dim, node_dim):
    lower = lax.index_in_dim(field, 0, node_dim, keepdims=True)
    upper = lax.index_in_dim(field, NP - 1, node_dim, keepdims=True)
    summed = upper + jnp.roll(lower, -1, axis=elem_dim)
    middle = lax.slice_in_dim(field, 1, NP - 1, axis=node_dim)
    return jnp.concatenate([jnp.roll(summed, 1, axis=elem_dim), middle, summed], axis=node_dim)


def assemble(field):
    shaped = field.reshape(field.shape[:3] + (NP, NP, NP))
    shaped = face_pass(shaped, 0, 3)
    shaped = face_pass(shaped, 1, 4)
    shaped = face_pass(shaped, 2, 5)
    return shaped.reshape(field.shape)


def reference(solution, residual, direction, geometry, mass):
    forward, backward, squares = operator_tables()
    weights = point_weights()
    points = NP ** 3
    geometry_rows = jnp.moveaxis(geometry.astype(jnp.float32), 0, -2)
    geometry_rows = geometry_rows.reshape(solution.shape[:3] + (3 * points,))
    mass_coef = mass.astype(jnp.float32)

    def diagonal_block(pair):
        geo_block, mass_block = pair
        flat = geo_block.reshape(-1, 3 * points)
        return (highest(flat, squares).reshape(mass_block.shape) + mass_block)

    def operator_block(triple):
        field_block, geo_block, mass_block = triple
        flat = field_block.reshape(-1, points)
        gradients = highest(flat, forward)
        fluxes = geo_block.reshape(-1, 3 * points) * gradients
        result = highest(fluxes, backward) + mass_block.reshape(-1, points) * flat
        return result.reshape(field_block.shape)

    diagonal = assemble(lax.map(diagonal_block, (geometry_rows, mass_coef)))
    smooth = assemble(weights * direction)
    scaled = residual / diagonal
    norm_now = jnp.sum(weights * residual * scaled)
    applied = assemble(lax.map(operator_block, (smooth, geometry_rows, mass_coef)))
    curvature = jnp.sum(weights * smooth * applied)
    step_size = norm_now / curvature
    solution_out = solution + step_size * smooth
    residual_out = residual - step_size * applied
    norm_next = jnp.sum(weights * residual_out * residual_out / diagonal)
    direction_out = residual_out / diagonal + (norm_next / norm_now) * smooth
    return (solution_out, residual_out, direction_out)
```

```python
import functools

import jax
import jax.numpy as jnp
import numpy as np
from jax import lax
from jax.experimental import pallas as pl
from jax.experimental.pallas import tpu as pltpu
from jax.sharding import PartitionSpec as P

NP = 8
LANES = 128
MESH = pl.DeviceIdType.MESH

lobatto_nodes = [
    -1.0,
    -0.8717401485096066,
    -0.5917001814331423,
    -0.2092992179024789,
    0.2092992179024789,
    0.5917001814331423,
    0.8717401485096066,
    1.0,
]


def derivative_table():
    nodes = np.array(lobatto_nodes)
    identity = np.eye(NP)
    offset = nodes[:, None] - nodes[None, :] + identity
    barycentric = 1.0 / np.prod(offset, axis=1)
    derivative = barycentric[None, :] / barycentric[:, None] / offset * (1.0 - identity)
    return derivative - identity * np.sum(derivative, axis=1)[:, None]


def split_table(table):
    table = np.asarray(table, np.float32)
    high = table.astype(jnp.bfloat16)
    low = (table - high.astype(np.float32)).astype(jnp.bfloat16)
    return high, low


def tables():
    d = derivative_table().astype(np.float32)
    along_j = np.kron(np.kron(np.eye(2), d), np.eye(NP))
    along_k = np.kron(np.eye(16), d)
    high, low = split_table(np.concatenate([along_j.T, along_k.T], axis=1))
    forward = np.concatenate([np.concatenate([high, high], 0), np.concatenate([low, low], 0)], 1)
    high, low = split_table(np.concatenate([along_j, along_k], axis=0))
    backward = np.concatenate([high, low], axis=1)
    high, low = split_table(np.concatenate([along_j * along_j, along_k * along_k], axis=0))
    squares = np.concatenate([high, low], axis=1)
    return np.concatenate([forward, backward, squares], axis=1)


def roll(x, shift):
    shift %= LANES
    return x if shift == 0 else pltpu.roll(x, shift, 1)


def lane_of(shape):
    return lax.broadcasted_iota(jnp.int32, shape, 1)


def along_i(table, blocks):
    low = lane_of(blocks[0].shape) < 64
    swapped = [roll(x, 64) for x in blocks]
    outs = []
    for b in range(4):
        total = None
        for c in range(4):
            same = jnp.where(low, float(table[2 * b, 2 * c]), float(table[2 * b + 1, 2 * c + 1]))
            other = jnp.where(low, float(table[2 * b, 2 * c + 1]), float(table[2 * b + 1, 2 * c]))
            term = same * blocks[c] + other * swapped[c]
            total = term if total is None else total + term
        outs.append(total)
    return outs


def weights_of(rows):
    lane = lane_of((rows, LANES))
    k, j = lane & 7, (lane >> 3) & 7
    half = lambda cond: jnp.where(cond, 0.5, 1.0)
    base = half((k == 0) | (k == 7)) * half((j == 0) | (j == 7))
    return [base * half(lane < 64), base, base, base * half(lane >= 64)]


def pack_i_face(x, side):
    h = x.shape[0] // 2
    top, bottom = x[:h], x[h:]
    low = lane_of(top.shape) < 64
    if side == 0:
        return jnp.where(low, top, roll(bottom, 64))
    return jnp.where(low, roll(top, 64), bottom)


def unpack_i_face(m, side):
    other = roll(m, 64)
    return jnp.concatenate([m, other] if side == 0 else [other, m], axis=0)


def pack_j_face(blocks, ez, side):
    half = ez // 2
    lane = lane_of((half, LANES))
    slot = (lane & 63) >> 3
    out = jnp.zeros((half, LANES), jnp.float32)
    for b in range(4):
        rows = blocks[b][:ez] if side == 0 else blocks[b][-ez:]
        for n in range(2):
            moved = roll(rows[n * half : (n + 1) * half], 8 * b + 32 * n - (0 if side == 0 else 56))
            out = jnp.where(slot == b + 4 * n, moved, out)
    return out


def unpack_j_face(m, b, shift):
    return jnp.concatenate([roll(m, shift - 8 * b), roll(m, shift - 8 * b - 32)], axis=0)


def join_j_faces(mine, before, after):
    lane = lane_of(mine.shape)
    first = (lane < 64) & ((lane & 31) < 8)
    last = (lane >= 64) & ((lane & 31) >= 24)
    return mine + jnp.where(first, roll(before, 40), jnp.where(last, roll(after, 88), 0.0))


def finish_assembly(blocks, ez, i_prev, i_next, j_prev, j_next):
    rows = blocks[0].shape[0]
    lane = lane_of((rows, LANES))
    low = lane < 64
    j, k = (lane >> 3) & 7, lane & 7
    blocks = list(blocks)
    blocks[0] = blocks[0] + jnp.where(low, unpack_i_face(i_prev, 0), 0.0)
    blocks[3] = blocks[3] + jnp.where(low, 0.0, unpack_i_face(i_next, 1))
    outs = []
    for b, x in enumerate(blocks):
        after, before = unpack_j_face(j_next, b, 56), unpack_j_face(j_prev, b, 0)
        if rows > ez:
            after = jnp.concatenate([roll(x[ez:], 56), after], axis=0)
            before = jnp.concatenate([before, roll(x[:-ez], -56)], axis=0)
        x = x + jnp.where(j == 7, after, jnp.where(j == 0, before, 0.0))
        up, down = roll(x, 7), roll(x, -7)
        after = [pltpu.roll(up[e : e + ez], ez - 1, 0) for e in range(0, rows, ez)]
        before = [pltpu.roll(down[e : e + ez], 1, 0) for e in range(0, rows, ez)]
        after, before = jnp.concatenate(after, 0), jnp.concatenate(before, 0)
        outs.append(x + jnp.where(k == 7, after, jnp.where(k == 0, before, 0.0)))
    return outs


def halves(x):
    high = x.astype(jnp.bfloat16)
    return high, (x - high.astype(jnp.float32)).astype(jnp.bfloat16)


def dot(left, right):
    return jnp.dot(left, right, preferred_element_type=jnp.float32)


def stack(blocks):
    return jnp.concatenate(blocks, axis=0)


def total_of(blocks):
    x = blocks[0] + blocks[1] + (blocks[2] + blocks[3])
    return jnp.sum(jnp.sum(x, axis=0, keepdims=True), axis=1, keepdims=True)


def kernel(
    ng, nd, ez,
    sol_h, res_h, dir_h, geo_h, mass_h, tab_h,
    outs,
    sol_v, res_v, dir_v, geo_v, mass_v, tab_v,
    face_out, face_in, part, parts,
    load_sem, send_sem, recv_sem, part_send, part_recv,
):
    me_g, me_d = lax.axis_index("group"), lax.axis_index("dev")

    def at(a, b):
        return (lax.rem(me_g + (a + ng), ng), lax.rem(me_d + (b + nd), nd))

    others = [(a, b) for a in range(ng) for b in range(nd) if (a, b) != (0, 0)]
    others.sort(key=lambda t: (min(t[1], nd - t[1]) != 1, min(t[0], ng - t[0]) > 1))

    pairs = ((dir_h, dir_v), (geo_h, geo_v), (mass_h, mass_v), (tab_h, tab_v), (res_h, res_v), (sol_h, sol_v))
    loads = [pltpu.make_async_copy(h, v, load_sem.at[n]) for n, (h, v) in enumerate(pairs)]
    loads[0].start()
    barrier = pltpu.get_barrier_semaphore()
    for a, b in others:
        pl.semaphore_signal(barrier, inc=1, device_id=at(a, b), device_id_type=MESH)

    for load in loads[1:]:
        load.start()

    rows = dir_v.shape[0]
    h, q = rows // 2, ez // 2

    def window(ref, phase, start, size):
        return ref.at[phase, pl.ds(start, size)]

    def i_out(phase, side):
        return window(face_out, phase, h * side, h)

    def i_in(phase, side):
        return window(face_in, phase, h * side, h)

    def j_out(phase, side):
        return window(face_out, phase, 2 * h + q * side, q)

    def j_in(phase, side, turn):
        return window(face_in, phase, 2 * h + q * (3 * side + turn), q)

    def all_of(phase, sem):
        pltpu.make_async_copy(face_in.at[phase], face_in.at[phase], sem.at[phase]).wait()

    weights = weights_of(rows)
    cut = [slice(LANES * b, LANES * b + LANES) for b in range(4)]

    def exchange(phase, blocks, started=True):
        made = []

        def give(src, dst, target):
            made.append(
                pltpu.make_async_remote_copy(
                    src_ref=src, dst_ref=dst,
                    send_sem=send_sem.at[phase], recv_sem=recv_sem.at[phase],
                    device_id=target, device_id_type=MESH,
                )
            )
            if started:
                made[-1].start()

        for side, step in ((0, -1), (1, 1)):
            i_out(phase, side)[...] = pack_i_face(blocks[3 * side], side)
            give(i_out(phase, side), i_in(phase, side), at(step, 0))
        for side, step in ((1, 1), (0, -1)):
            j_out(phase, side)[...] = pack_j_face(blocks, ez, side)
            for turn, a in ((0, -1), (2, 1), (1, 0)):
                give(j_out(phase, side), j_in(phase, side, turn), at(a, step))
        return made

    def assembled(phase, blocks):
        j_prev = join_j_faces(*(j_in(phase, 1, turn)[...] for turn in (1, 2, 0)))
        j_next = join_j_faces(*(j_in(phase, 0, turn)[...] for turn in (1, 2, 0)))
        return finish_assembly(blocks, ez, i_in(phase, 1)[...], i_in(phase, 0)[...], j_prev, j_next)

    d = derivative_table().astype(np.float32)
    loads[0].wait()
    weighted = [weights[b] * dir_v[:, cut[b]] for b in range(4)]
    first = exchange(0, weighted, started=False)
    pl.semaphore_wait(barrier, len(others))
    for copy in first:
        copy.start()
    for load in loads[1:4]:
        load.wait()
    geo_rows = stack([jnp.concatenate([geo_v[1, :, c], geo_v[2, :, c]], axis=1) for c in cut])
    squared = dot(geo_rows, tab_v[:, 768:1024])
    squared = squared[:, :LANES] + squared[:, LANES:]
    geo = [[geo_v[c, :, cut[b]].astype(jnp.float32) for b in range(4)] for c in range(3)]
    mass = [mass_v[:, c].astype(jnp.float32) for c in cut]
    diag = along_i((d * d).T, geo[0])
    diag = [diag[b] + squared[rows * b : rows * b + rows] + mass[b] for b in range(4)]
    exchange(1, diag)
    loads[4].wait()
    loads[5].wait()
    all_of(0, recv_sem)
    smooth = assembled(0, weighted)

    high, low = halves(stack(smooth))
    grads = dot(jnp.concatenate([high, low], axis=1), tab_v[:, :512])
    grads = grads[:, :256] + grads[:, 256:]
    grad_i = along_i(d, smooth)
    flux_i = [geo[0][b] * grad_i[b] for b in range(4)]
    flux = jnp.concatenate(
        [stack(geo[1]) * grads[:, :LANES], stack(geo[2]) * grads[:, LANES:]], axis=1
    )
    high, low = halves(flux)
    back = dot(jnp.concatenate([high, low], axis=0), tab_v[:, 512:768])
    back = back[: 4 * rows] + back[4 * rows :]
    back = back[:, :LANES] + back[:, LANES:]
    local = along_i(d.T, flux_i)
    local = [local[b] + back[rows * b : rows * b + rows] + mass[b] * smooth[b] for b in range(4)]

    exchange(2, local)
    all_of(1, recv_sem)
    inverse = [1.0 / x for x in assembled(1, diag)]
    residual = [res_v[:, c] for c in cut]
    scaled = [residual[b] * inverse[b] for b in range(4)]
    norm_now = total_of([weights[b] * residual[b] * scaled[b] for b in range(4)])
    curvature = total_of([smooth[b] * local[b] for b in range(4)])
    all_of(2, recv_sem)
    applied = assembled(2, local)
    shared = [weights[b] * applied[b] for b in range(4)]
    cross = total_of([shared[b] * scaled[b] for b in range(4)])
    quad = total_of([shared[b] * applied[b] * inverse[b] for b in range(4)])

    lane = lane_of((1, LANES))
    mine = jnp.where(
        lane < 32, norm_now, jnp.where(lane < 64, curvature, jnp.where(lane < 96, cross, quad))
    )
    part[0] = mine
    order = sorted(range(len(others)), key=lambda n: (others[n][1] != 0, others[n][1] != 1))
    for n in order:
        a, b = others[n]
        pltpu.make_async_remote_copy(
            src_ref=part.at[0], dst_ref=parts.at[n],
            send_sem=part_send, recv_sem=part_recv,
            device_id=at(a, b), device_id_type=MESH,
        ).start()
    pltpu.make_async_copy(parts, parts, part_recv).wait()
    everyone = mine + jnp.sum(parts[...], axis=0)
    norm_now, curvature, cross, quad = (everyone[:, 32 * n : 32 * n + 1] for n in range(4))
    step = norm_now / curvature
    norm_next = norm_now - 2.0 * step * cross + step * step * quad
    ratio = norm_next / norm_now
    for b, c in enumerate(cut):
        outs[0, :, c] = sol_v[:, c] + step * smooth[b]
        out = residual[b] - step * applied[b]
        outs[1, :, c] = out
        outs[2, :, c] = out * inverse[b] + ratio * smooth[b]
    for phase in range(3):
        all_of(phase, send_sem)
    pltpu.make_async_copy(parts, parts, part_send).wait()


def deliver(stacked, *refs):
    for n in range(3):
        pltpu.make_async_copy(stacked.at[n], refs[n], refs[3]).start()
    pltpu.make_async_copy(stacked, stacked, refs[3]).wait()


def on_device(solution, residual, direction, geometry, mass):
    dims = solution.shape
    ng, nd = lax.axis_size("group"), lax.axis_size("dev")
    ez, points = dims[2], dims[3]
    rows = dims[0] * dims[1] * ez
    flat = (rows, points)
    f32, bf16 = jnp.float32, jnp.bfloat16
    table = jnp.asarray(tables())
    h = rows // 2
    stacked = pl.pallas_call(
        functools.partial(kernel, ng, nd, ez),
        out_shape=pltpu.VMEM((3,) + flat, f32),
        in_specs=[pl.BlockSpec(memory_space=pltpu.HBM)] * 6,
        out_specs=pl.BlockSpec(memory_space=pltpu.VMEM),
        scratch_shapes=[
            pltpu.VMEM(flat, f32),
            pltpu.VMEM(flat, f32),
            pltpu.VMEM(flat, f32),
            pltpu.VMEM((3,) + flat, bf16),
            pltpu.VMEM(flat, bf16),
            pltpu.VMEM(table.shape, bf16),
            pltpu.VMEM((3, 2 * h + ez, LANES), f32),
            pltpu.VMEM((3, 2 * h + 3 * ez, LANES), f32),
            pltpu.VMEM((1, 1, LANES), f32),
            pltpu.VMEM((ng * nd - 1, 1, LANES), f32),
            pltpu.SemaphoreType.DMA((6,)),
            pltpu.SemaphoreType.DMA((3,)),
            pltpu.SemaphoreType.DMA((3,)),
            pltpu.SemaphoreType.DMA,
            pltpu.SemaphoreType.DMA,
        ],
        compiler_params=pltpu.CompilerParams(collective_id=0, has_side_effects=True, vmem_limit_bytes=8 << 20),
    )(
        pltpu.with_memory_space_constraint(solution.reshape(flat), pltpu.HBM),
        pltpu.with_memory_space_constraint(residual.reshape(flat), pltpu.HBM),
        pltpu.with_memory_space_constraint(direction.reshape(flat), pltpu.HBM),
        pltpu.with_memory_space_constraint(geometry.reshape((3,) + flat), pltpu.HBM),
        pltpu.with_memory_space_constraint(mass.reshape(flat), pltpu.HBM),
        pltpu.with_memory_space_constraint(table, pltpu.HBM),
    )
    outs = pl.pallas_call(
        deliver,
        out_shape=[jax.ShapeDtypeStruct(flat, f32)] * 3,
        in_specs=[pl.BlockSpec(memory_space=pl.ANY)],
        out_specs=[pl.BlockSpec(memory_space=pltpu.HBM)] * 3,
        scratch_shapes=[pltpu.SemaphoreType.DMA],
        compiler_params=pltpu.CompilerParams(vmem_limit_bytes=8 << 20),
    )(stacked)
    return tuple(x.reshape(dims) for x in outs)


def solution(mesh):
    spec = P("group", "dev", None, None)
    return jax.shard_map(
        on_device,
        mesh=mesh,
        in_specs=(spec, spec, spec, P(None, "group", "dev", None, None), spec),
        out_specs=(spec, spec, spec),
        check_vma=False,
    )
```

```python
import functools

import jax
import jax.numpy as jnp
import numpy as np
from jax import lax
from jax.experimental import pallas as pl
from jax.experimental.pallas import tpu as pltpu
from jax.sharding import PartitionSpec as P

NP = 8
LANES = 128
MESH = pl.DeviceIdType.MESH

lobatto_nodes = [
    -1.0,
    -0.8717401485096066,
    -0.5917001814331423,
    -0.2092992179024789,
    0.2092992179024789,
    0.5917001814331423,
    0.8717401485096066,
    1.0,
]


def derivative_table():
    nodes = np.array(lobatto_nodes)
    identity = np.eye(NP)
    offset = nodes[:, None] - nodes[None, :] + identity
    barycentric = 1.0 / np.prod(offset, axis=1)
    derivative = barycentric[None, :] / barycentric[:, None] / offset * (1.0 - identity)
    return derivative - identity * np.sum(derivative, axis=1)[:, None]


def split_table(table):
    table = np.asarray(table, np.float32)
    high = table.astype(jnp.bfloat16)
    low = (table - high.astype(np.float32)).astype(jnp.bfloat16)
    return high, low


def tables():
    d = derivative_table().astype(np.float32)
    along_j = np.kron(np.kron(np.eye(2), d), np.eye(NP))
    along_k = np.kron(np.eye(16), d)
    high, low = split_table(np.concatenate([along_j.T, along_k.T], axis=1))
    forward = np.concatenate([np.concatenate([high, high], 0), np.concatenate([low, low], 0)], 1)
    high, low = split_table(np.concatenate([along_j, along_k], axis=0))
    backward = np.concatenate([high, low], axis=1)
    high, low = split_table(np.concatenate([along_j * along_j, along_k * along_k], axis=0))
    squares = np.concatenate([high, low], axis=1)
    return np.concatenate([forward, backward, squares], axis=1)


def roll(x, shift):
    shift %= LANES
    return x if shift == 0 else pltpu.roll(x, shift, 1)


def lane_of(shape):
    return lax.broadcasted_iota(jnp.int32, shape, 1)


def along_i(table, blocks):
    low = lane_of(blocks[0].shape) < 64
    swapped = [roll(x, 64) for x in blocks]
    outs = []
    for b in range(4):
        total = None
        for c in range(4):
            same = jnp.where(low, float(table[2 * b, 2 * c]), float(table[2 * b + 1, 2 * c + 1]))
            other = jnp.where(low, float(table[2 * b, 2 * c + 1]), float(table[2 * b + 1, 2 * c]))
            term = same * blocks[c] + other * swapped[c]
            total = term if total is None else total + term
        outs.append(total)
    return outs


def weights_of(rows):
    lane = lane_of((rows, LANES))
    k, j = lane & 7, (lane >> 3) & 7
    half = lambda cond: jnp.where(cond, 0.5, 1.0)
    base = half((k == 0) | (k == 7)) * half((j == 0) | (j == 7))
    return [base * half(lane < 64), base, base, base * half(lane >= 64)]


def pack_i_face(x, side):
    h = x.shape[0] // 2
    top, bottom = x[:h], x[h:]
    low = lane_of(top.shape) < 64
    if side == 0:
        return jnp.where(low, top, roll(bottom, 64))
    return jnp.where(low, roll(top, 64), bottom)


def unpack_i_face(m, side):
    other = roll(m, 64)
    return jnp.concatenate([m, other] if side == 0 else [other, m], axis=0)


def pack_j_face(blocks, ez, side):
    half = ez // 2
    lane = lane_of((half, LANES))
    slot = (lane & 63) >> 3
    out = jnp.zeros((half, LANES), jnp.float32)
    for b in range(4):
        rows = blocks[b][:ez] if side == 0 else blocks[b][-ez:]
        for n in range(2):
            moved = roll(rows[n * half : (n + 1) * half], 8 * b + 32 * n - (0 if side == 0 else 56))
            out = jnp.where(slot == b + 4 * n, moved, out)
    return out


def assemble_inside(blocks, ez):
    rows = blocks[0].shape[0]
    lane = lane_of((rows, LANES))
    j, k = (lane >> 3) & 7, lane & 7
    outs = []
    for x in blocks:
        if rows > ez:
            edge = jnp.zeros((ez, LANES), jnp.float32)
            after = jnp.concatenate([roll(x[ez:], 56), edge], axis=0)
            before = jnp.concatenate([edge, roll(x[:-ez], -56)], axis=0)
            x = x + jnp.where(j == 7, after, jnp.where(j == 0, before, 0.0))
        up, down = roll(x, 7), roll(x, -7)
        after = [pltpu.roll(up[e : e + ez], ez - 1, 0) for e in range(0, rows, ez)]
        before = [pltpu.roll(down[e : e + ez], 1, 0) for e in range(0, rows, ez)]
        after, before = jnp.concatenate(after, 0), jnp.concatenate(before, 0)
        outs.append(x + jnp.where(k == 7, after, jnp.where(k == 0, before, 0.0)))
    return outs


def add_i_face(blocks, message, side):
    blocks = list(blocks)
    low = lane_of(blocks[0].shape) < 64
    face = unpack_i_face(message, side)
    blocks[3 * side] = blocks[3 * side] + jnp.where(low if side == 0 else ~low, face, 0.0)
    return blocks


def add_j_face(blocks, ez, same, before, after, side):
    lane = lane_of((ez, LANES))
    here = ((lane >> 3) & 7) == 7 * side

    def spread(message, shift):
        return jnp.concatenate([roll(message, shift), roll(message, shift - 32)], axis=0)

    outs = []
    for b, x in enumerate(blocks):
        shift = 56 * side - 8 * b
        face = jnp.where(here, spread(same, shift), 0.0)
        if b == 0:
            face = face + jnp.where(here & (lane < 64), spread(before, shift + 40), 0.0)
        if b == 3:
            face = face + jnp.where(here & (lane >= 64), spread(after, shift + 88), 0.0)
        if x.shape[0] == ez:
            outs.append(x + face)
        elif side == 0:
            outs.append(jnp.concatenate([x[:ez] + face, x[ez:]], axis=0))
        else:
            outs.append(jnp.concatenate([x[:-ez], x[-ez:] + face], axis=0))
    return outs


def halves(x):
    high = x.astype(jnp.bfloat16)
    return high, (x - high.astype(jnp.float32)).astype(jnp.bfloat16)


def dot(left, right):
    return jnp.dot(left, right, preferred_element_type=jnp.float32)


def stack(blocks):
    return jnp.concatenate(blocks, axis=0)


def total_of(blocks):
    x = blocks[0] + blocks[1] + (blocks[2] + blocks[3])
    return jnp.sum(jnp.sum(x, axis=0, keepdims=True), axis=1, keepdims=True)


def owner_weights(rows, ez, first_owned, last_owned):
    lane = lane_of((rows, LANES))
    row = lax.broadcasted_iota(jnp.int32, (rows, LANES), 0)
    k, j = lane & 7, (lane >> 3) & 7
    base = jnp.where((k == 0) | (k == 7), 0.5, 1.0)
    first = jnp.where(row < ez, jnp.where(first_owned, 1.0, 0.0), 0.5)
    last = jnp.where(row >= rows - ez, jnp.where(last_owned, 1.0, 0.0), 0.5)
    base = base * jnp.where(j == 0, first, jnp.where(j == 7, last, 1.0))
    return [jnp.where(lane < 64, 0.0, base), base, base, base]


def kernel(
    ng, nd, ez,
    sol_h, res_h, dir_h, geo_h, mass_h, tab_h,
    outs,
    sol_v, res_v, dir_v, geo_v, mass_v, tab_v,
    face_out, face_in, wrap_in, root_in, prev_v, next_v, part, parts, late_out, late,
    load_sem, send_sem, recv_sem, last_recv, root_send, root_recv, part_send, part_recv, late_send, go,
):
    me_g, me_d = lax.axis_index("group"), lax.axis_index("dev")

    def at(a, b):
        return (lax.rem(me_g + (a + ng), ng), lax.rem(me_d + (b + nd), nd))

    others = [(a, b) for a in range(ng) for b in range(nd) if (a, b) != (0, 0)]
    others.sort(key=lambda t: (min(t[1], nd - t[1]) != 1, min(t[0], ng - t[0]) > 1))

    pairs = ((dir_h, dir_v), (geo_h, geo_v), (mass_h, mass_v), (tab_h, tab_v), (res_h, res_v), (sol_h, sol_v))
    loads = [pltpu.make_async_copy(h, v, load_sem.at[n]) for n, (h, v) in enumerate(pairs)]
    loads[0].start()
    barrier = pltpu.get_barrier_semaphore()
    partners = [t for t in others if min(t[0], ng - t[0]) < 2 and min(t[1], nd - t[1]) < 2]
    hub = (1 % ng, nd // 2)
    hub_a, hub_b = lax.rem(me_g - hub[0] + ng, ng), lax.rem(me_d - hub[1] + nd, nd)
    at_hub = (hub_a == 0) & (hub_b == 0)
    near_hub = ((hub_a < 2) | (hub_a == ng - 1)) & ((hub_b < 2) | (hub_b == nd - 1))
    for a, b in partners:
        pl.semaphore_signal(barrier, inc=1, device_id=at(a, b), device_id_type=MESH)

    @pl.when(jnp.logical_not(near_hub))
    def _():
        pl.semaphore_signal(barrier, inc=1, device_id=hub, device_id_type=MESH)

    for load in loads[1:]:
        load.start()

    rows = dir_v.shape[0]
    h, q = rows // 2, ez // 2
    is_first, is_last = me_d == 0, me_d == nd - 1
    owns_next = me_d < nd - 2

    def i_out(phase, side):
        return face_out.at[phase, pl.ds(h * side, h)]

    def i_in(phase, side):
        return face_in.at[phase, pl.ds(h * side, h)]

    def j_out(phase, side):
        return face_out.at[phase, pl.ds(2 * h + q * side, q)]

    def j_in(phase, side, turn):
        return face_in.at[phase, pl.ds(2 * h + q * (3 * side + turn), q)]

    def slot(ref, part_of, group):
        return ref.at[pl.ds(pl.multiple_of(q * (ng * part_of + group), q), q)]

    def drain(count, sem):
        source = face_in.at[0] if count <= face_in.shape[1] else root_in
        ref = source.at[pl.ds(0, count)]
        pltpu.make_async_copy(ref, ref, sem).wait()

    def drain_phases(start, count, sem):
        ref = face_in.at[pl.ds(start, count)]
        pltpu.make_async_copy(ref, ref, sem).wait()

    def send(src, dst, send_to, recv_to, target):
        return pltpu.make_async_remote_copy(
            src_ref=src, dst_ref=dst, send_sem=send_to, recv_sem=recv_to,
            device_id=target, device_id_type=MESH,
        )

    weights = weights_of(rows)
    cut = [slice(LANES * b, LANES * b + LANES) for b in range(4)]

    def pack(phase, blocks):
        for side in range(2):
            j_out(phase, side)[...] = pack_j_face(blocks, ez, side)
            i_out(phase, side)[...] = pack_i_face(blocks[3 * side], side)

    def give_j(phase, side, step, sem):
        for turn, a in ((0, -1), (2, 1), (1, 0)):
            send(j_out(phase, side), j_in(phase, side, turn), send_sem.at[phase], sem, at(a, step)).start()

    def give_i(phase, sems):
        for side, step in ((0, -1), (1, 1)):
            send(i_out(phase, side), i_in(phase, side), send_sem.at[phase], sems[side], at(step, 0)).start()

    def give(phase):
        give_j(phase, 0, -1, recv_sem.at[phase])
        give_j(phase, 1, 1, recv_sem.at[phase])
        give_i(phase, [recv_sem.at[phase]] * 2)

    def turns(phase, side):
        return [j_in(phase, side, turn)[...] for turn in (1, 2, 0)]

    def assembled(phase, blocks):
        blocks = add_i_face(add_i_face(blocks, i_in(phase, 1)[...], 0), i_in(phase, 0)[...], 1)
        return add_j_face(add_j_face(blocks, ez, *turns(phase, 1), 0), ez, *turns(phase, 0), 1)

    d = derivative_table().astype(np.float32)
    loads[0].wait()
    weighted = assemble_inside([weights[b] * dir_v[:, cut[b]] for b in range(4)], ez)
    pack(0, weighted)
    pl.semaphore_wait(barrier, jnp.where(at_hub, len(others), len(partners)))
    give(0)

    @pl.when(at_hub)
    def _():
        for a, b in others:
            pl.semaphore_signal(go, inc=1, device_id=at(a, b), device_id_type=MESH)

    for load in loads[1:5]:
        load.wait()
    geo_rows = stack([jnp.concatenate([geo_v[1, :, c], geo_v[2, :, c]], axis=1) for c in cut])
    squared = dot(geo_rows, tab_v[:, 768:1024])
    squared = squared[:, :LANES] + squared[:, LANES:]
    geo = [[geo_v[c, :, cut[b]].astype(jnp.float32) for b in range(4)] for c in range(3)]
    mass = [mass_v[:, c].astype(jnp.float32) for c in cut]
    diag = along_i((d * d).T, geo[0])
    diag = [diag[b] + squared[rows * b : rows * b + rows] + mass[b] for b in range(4)]
    diag = assemble_inside(diag, ez)
    pack(1, diag)
    give(1)
    residual = [res_v[:, c] for c in cut]
    spread_res = [weights[b] * residual[b] for b in range(4)]
    mixed = assemble_inside(spread_res, ez)
    pack(2, mixed)
    give(2)
    loads[5].wait()
    owned = owner_weights(rows, ez, is_last, owns_next)

    @pl.when(jnp.logical_not(at_hub))
    def _():
        pl.semaphore_wait(go, 1)

    drain_phases(0, 1, recv_sem.at[0])
    smooth = assembled(0, weighted)

    high, low = halves(stack(smooth))
    grads = dot(jnp.concatenate([high, low], axis=1), tab_v[:, :512])
    grads = grads[:, :256] + grads[:, 256:]
    grad_i = along_i(d, smooth)
    flux_i = [geo[0][b] * grad_i[b] for b in range(4)]
    flux = jnp.concatenate(
        [stack(geo[1]) * grads[:, :LANES], stack(geo[2]) * grads[:, LANES:]], axis=1
    )
    high, low = halves(flux)
    back = dot(jnp.concatenate([high, low], axis=0), tab_v[:, 512:768])
    back = back[: 4 * rows] + back[4 * rows :]
    back = back[:, :LANES] + back[:, LANES:]
    local = along_i(d.T, flux_i)
    local = [local[b] + back[rows * b : rows * b + rows] + mass[b] * smooth[b] for b in range(4)]

    inside = assemble_inside(local, ez)
    pack(3, inside)

    @pl.when(is_last)
    def _():
        for g in range(ng):
            send(j_out(3, 1), slot(wrap_in, 0, me_g), root_send, root_recv.at[0], (g, 0)).start()

    give_i(3, [last_recv.at[0], last_recv.at[1]])
    give_j(3, 0, -1, last_recv.at[2])

    @pl.when(jnp.logical_not(is_last))
    def _():
        give_j(3, 1, 1, last_recv.at[3])

    @pl.when(is_first)
    def _():
        for a in range(1, ng):
            send(j_out(3, 0), slot(root_in, 0, me_g), root_send, root_recv.at[1], at(a, 0)).start()

    drain_phases(1, 1, recv_sem.at[1])
    inverse = [1.0 / x for x in assembled(1, diag)]

    @pl.when(is_first)
    def _():
        lane = lane_of((q, LANES))
        ends = ((lane & 7) == 0) | ((lane & 7) == 7)
        share = jnp.where((lane < 64) & ((lane & 31) < 8), 0.0, jnp.where(ends, 0.5, 1.0))
        face_out[1, pl.ds(2 * h + 2 * q, q)] = share * pack_j_face(inverse, ez, 0)
        mine = face_out.at[1, pl.ds(2 * h + 2 * q, q)]
        for a in range(1, ng):
            send(mine, slot(root_in, 1, me_g), root_send, root_recv.at[1], at(a, 0)).start()

    drain_phases(2, 1, recv_sem.at[2])
    dual = assembled(2, mixed)
    norm_now = total_of([spread_res[b] * residual[b] * inverse[b] for b in range(4)])
    curvature = total_of([smooth[b] * local[b] for b in range(4)])
    cross = total_of([local[b] * dual[b] * inverse[b] for b in range(4)])
    share = [owned[b] * inverse[b] for b in range(4)]

    def hold(ref, side):
        for n, value in enumerate(turns(3, side)):
            ref[pl.ds(q * n, q)] = value

    def held(ref):
        return [ref[pl.ds(q * n, q)] for n in range(3)]

    drain(h, last_recv.at[0])
    closed = add_i_face(inside, i_in(3, 0)[...], 1)

    @pl.when(owns_next)
    def _():
        drain(3 * q, last_recv.at[2])
        hold(next_v, 0)

    @pl.when(jnp.logical_not(owns_next))
    def _():
        next_v[...] = jnp.zeros_like(next_v)

    @pl.when(is_last)
    def _():
        drain(3 * q, last_recv.at[3])
        hold(prev_v, 1)

    @pl.when(jnp.logical_not(is_last))
    def _():
        prev_v[...] = jnp.zeros_like(prev_v)

    mostly = add_j_face(add_j_face(closed, ez, *held(prev_v), 0), ez, *held(next_v), 1)
    quad = total_of([share[b] * mostly[b] * mostly[b] for b in range(4)])

    lane = lane_of((1, LANES))
    mine = jnp.where(
        lane < 32, norm_now, jnp.where(lane < 64, curvature, jnp.where(lane < 96, cross, quad))
    )
    part[0] = mine
    order = sorted(range(len(others)), key=lambda n: (others[n][1] != 0, others[n][1] != 1))
    for n in order:
        a, b = others[n]
        send(part.at[0], parts.at[n], part_send, part_recv, at(a, b)).start()

    @pl.when(is_first)
    def _():
        slot(root_in, 0, me_g)[...] = j_out(3, 0)[...]
        slot(root_in, 1, me_g)[...] = face_out[1, pl.ds(2 * h + 2 * q, q)]
        drain(2 * (ng - 1) * q, root_recv.at[1])
        drain(ng * q, root_recv.at[0])
        spot = lane_of((q, LANES))
        seam = (spot >= 64) & ((spot & 31) >= 24)
        faces = [wrap_in[pl.ds(q * g, q)] + root_in[pl.ds(q * g, q)] for g in range(ng)]
        total = None
        for g in range(ng):
            face = faces[g] + jnp.where(seam, roll(faces[(g + 1) % ng], 88), 0.0)
            term = face * face * root_in[pl.ds(q * (ng + g), q)]
            total = term if total is None else total + term
        total = jnp.sum(jnp.sum(total, axis=0, keepdims=True), axis=1, keepdims=True)
        late[0] = jnp.broadcast_to(total, (1, LANES))
        late_out[0] = jnp.broadcast_to(total, (1, LANES))
        for n, shift in enumerate((0, ng - 1, 1)):
            prev_v[pl.ds(q * n, q)] = slot(wrap_in, 0, lax.rem(me_g + shift, ng))[...]

    speaks = is_first & ((me_g & 1) == 1)

    @pl.when(speaks)
    def _():
        for b in range(1, nd):
            for a in (0, -1):
                send(late_out.at[0], late.at[0], late_send, root_recv.at[2], at(a, b)).start()

    drain(h, last_recv.at[1])

    @pl.when(jnp.logical_not(owns_next))
    def _():
        drain(3 * q, last_recv.at[2])
        hold(next_v, 0)

    @pl.when(jnp.logical_not(is_last | is_first))
    def _():
        drain(3 * q, last_recv.at[3])
        hold(prev_v, 1)

    applied = add_i_face(closed, i_in(3, 1)[...], 0)
    applied = add_j_face(add_j_face(applied, ez, *held(prev_v), 0), ez, *held(next_v), 1)

    @pl.when(jnp.logical_not(is_first))
    def _():
        pltpu.make_async_copy(late, late, root_recv.at[2]).wait()

    pltpu.make_async_copy(parts, parts, part_recv).wait()
    everyone = mine + jnp.sum(parts[...], axis=0)
    norm_now, curvature, cross, quad = (everyone[:, 32 * n : 32 * n + 1] for n in range(4))
    quad = quad + late[0][:, :1]
    step = norm_now / curvature
    norm_next = norm_now - 2.0 * step * cross + step * step * quad
    ratio = norm_next / norm_now
    for b, c in enumerate(cut):
        outs[0, :, c] = sol_v[:, c] + step * smooth[b]
        out = residual[b] - step * applied[b]
        outs[1, :, c] = out
        outs[2, :, c] = out * inverse[b] + ratio * smooth[b]
    for phase in range(3):
        drain_phases(phase, 1, send_sem.at[phase])

    @pl.when(jnp.logical_not(is_last))
    def _():
        drain(2 * h + 6 * q, send_sem.at[3])

    @pl.when(is_last)
    def _():
        drain(2 * h + 3 * q, send_sem.at[3])
        drain(ng * q, root_send)

    @pl.when(is_first)
    def _():
        drain(2 * (ng - 1) * q, root_send)

    @pl.when(speaks)
    def _():
        ref = parts.at[pl.ds(0, 2 * (nd - 1))]
        pltpu.make_async_copy(ref, ref, late_send).wait()

    pltpu.make_async_copy(parts, parts, part_send).wait()


def deliver(stacked, *refs):
    for n in range(3):
        pltpu.make_async_copy(stacked.at[n], refs[n], refs[3]).start()
    pltpu.make_async_copy(stacked, stacked, refs[3]).wait()


def on_device(solution, residual, direction, geometry, mass):
    dims = solution.shape
    ng, nd = lax.axis_size("group"), lax.axis_size("dev")
    ez, points = dims[2], dims[3]
    rows = dims[0] * dims[1] * ez
    flat = (rows, points)
    f32, bf16 = jnp.float32, jnp.bfloat16
    table = jnp.asarray(tables())
    h, q = rows // 2, ez // 2
    stacked = pl.pallas_call(
        functools.partial(kernel, ng, nd, ez),
        out_shape=pltpu.VMEM((3,) + flat, f32),
        in_specs=[pl.BlockSpec(memory_space=pltpu.HBM)] * 6,
        out_specs=pl.BlockSpec(memory_space=pltpu.VMEM),
        scratch_shapes=[
            pltpu.VMEM(flat, f32),
            pltpu.VMEM(flat, f32),
            pltpu.VMEM(flat, f32),
            pltpu.VMEM((3,) + flat, bf16),
            pltpu.VMEM(flat, bf16),
            pltpu.VMEM(table.shape, bf16),
            pltpu.VMEM((4, 2 * h + 3 * q, LANES), f32),
            pltpu.VMEM((4, 2 * h + 3 * ez, LANES), f32),
            pltpu.VMEM((ng * q, LANES), f32),
            pltpu.VMEM((2 * ng * q, LANES), f32),
            pltpu.VMEM((3 * q, LANES), f32),
            pltpu.VMEM((3 * q, LANES), f32),
            pltpu.VMEM((1, 1, LANES), f32),
            pltpu.VMEM((ng * nd - 1, 1, LANES), f32),
            pltpu.VMEM((1, 1, LANES), f32),
            pltpu.VMEM((1, 1, LANES), f32),
            pltpu.SemaphoreType.DMA((6,)),
            pltpu.SemaphoreType.DMA((4,)),
            pltpu.SemaphoreType.DMA((3,)),
            pltpu.SemaphoreType.DMA((4,)),
            pltpu.SemaphoreType.DMA,
            pltpu.SemaphoreType.DMA((3,)),
            pltpu.SemaphoreType.DMA,
            pltpu.SemaphoreType.DMA,
            pltpu.SemaphoreType.DMA,
            pltpu.SemaphoreType.REGULAR,
        ],
        compiler_params=pltpu.CompilerParams(collective_id=0, has_side_effects=True, vmem_limit_bytes=8 << 20),
    )(
        pltpu.with_memory_space_constraint(solution.reshape(flat), pltpu.HBM),
        pltpu.with_memory_space_constraint(residual.reshape(flat), pltpu.HBM),
        pltpu.with_memory_space_constraint(direction.reshape(flat), pltpu.HBM),
        pltpu.with_memory_space_constraint(geometry.reshape((3,) + flat), pltpu.HBM),
        pltpu.with_memory_space_constraint(mass.reshape(flat), pltpu.HBM),
        pltpu.with_memory_space_constraint(table, pltpu.HBM),
    )
    outs = pl.pallas_call(
        deliver,
        out_shape=[jax.ShapeDtypeStruct(flat, f32)] * 3,
        in_specs=[pl.BlockSpec(memory_space=pl.ANY)],
        out_specs=[pl.BlockSpec(memory_space=pltpu.HBM)] * 3,
        scratch_shapes=[pltpu.SemaphoreType.DMA],
        compiler_params=pltpu.CompilerParams(vmem_limit_bytes=8 << 20),
    )(stacked)
    return tuple(x.reshape(dims) for x in outs)


def solution(mesh):
    spec = P("group", "dev", None, None)
    return jax.shard_map(
        on_device,
        mesh=mesh,
        in_specs=(spec, spec, spec, P(None, "group", "dev", None, None), spec),
        out_specs=(spec, spec, spec),
        check_vma=False,
    )
```

```python
import functools

import jax
import jax.numpy as jnp
import numpy as np
from jax import lax
from jax.experimental import pallas as pl
from jax.experimental.pallas import tpu as pltpu
from jax.sharding import PartitionSpec as P

NP = 8
LANES = 128
MESH = pl.DeviceIdType.MESH

lobatto_nodes = [
    -1.0,
    -0.8717401485096066,
    -0.5917001814331423,
    -0.2092992179024789,
    0.2092992179024789,
    0.5917001814331423,
    0.8717401485096066,
    1.0,
]


def derivative_table():
    nodes = np.array(lobatto_nodes)
    identity = np.eye(NP)
    offset = nodes[:, None] - nodes[None, :] + identity
    barycentric = 1.0 / np.prod(offset, axis=1)
    derivative = barycentric[None, :] / barycentric[:, None] / offset * (1.0 - identity)
    return derivative - identity * np.sum(derivative, axis=1)[:, None]


def split_table(table):
    table = np.asarray(table, np.float32)
    high = table.astype(jnp.bfloat16)
    low = (table - high.astype(np.float32)).astype(jnp.bfloat16)
    return high, low


def tables():
    d = derivative_table().astype(np.float32)
    along_j = np.kron(np.kron(np.eye(2), d), np.eye(NP))
    along_k = np.kron(np.eye(16), d)
    high, low = split_table(np.concatenate([along_j.T, along_k.T], axis=1))
    forward = np.concatenate([np.concatenate([high, high], 0), np.concatenate([low, low], 0)], 1)
    high, low = split_table(np.concatenate([along_j, along_k], axis=0))
    backward = np.concatenate([high, low], axis=1)
    high, low = split_table(np.concatenate([along_j * along_j, along_k * along_k], axis=0))
    squares = np.concatenate([high, low], axis=1)
    return np.concatenate([forward, backward, squares], axis=1)


def roll(x, shift):
    shift %= LANES
    return x if shift == 0 else pltpu.roll(x, shift, 1)


def lane_of(shape):
    return lax.broadcasted_iota(jnp.int32, shape, 1)


def along_i(table, blocks):
    low = lane_of(blocks[0].shape) < 64
    swapped = [roll(x, 64) for x in blocks]
    outs = []
    for b in range(4):
        total = None
        for c in range(4):
            same = jnp.where(low, float(table[2 * b, 2 * c]), float(table[2 * b + 1, 2 * c + 1]))
            other = jnp.where(low, float(table[2 * b, 2 * c + 1]), float(table[2 * b + 1, 2 * c]))
            term = same * blocks[c] + other * swapped[c]
            total = term if total is None else total + term
        outs.append(total)
    return outs


def weights_of(rows):
    lane = lane_of((rows, LANES))
    k, j = lane & 7, (lane >> 3) & 7
    half = lambda cond: jnp.where(cond, 0.5, 1.0)
    base = half((k == 0) | (k == 7)) * half((j == 0) | (j == 7))
    return [base * half(lane < 64), base, base, base * half(lane >= 64)]


def pack_i_face(x, side):
    h = x.shape[0] // 2
    top, bottom = x[:h], x[h:]
    low = lane_of(top.shape) < 64
    if side == 0:
        return jnp.where(low, top, roll(bottom, 64))
    return jnp.where(low, roll(top, 64), bottom)


def unpack_i_face(m, side):
    other = roll(m, 64)
    return jnp.concatenate([m, other] if side == 0 else [other, m], axis=0)


def pack_j_face(blocks, ez, side):
    half = ez // 2
    lane = lane_of((half, LANES))
    slot = (lane & 63) >> 3
    out = jnp.zeros((half, LANES), jnp.float32)
    for b in range(4):
        rows = blocks[b][:ez] if side == 0 else blocks[b][-ez:]
        for n in range(2):
            moved = roll(rows[n * half : (n + 1) * half], 8 * b + 32 * n - (0 if side == 0 else 56))
            out = jnp.where(slot == b + 4 * n, moved, out)
    return out


def assemble_inside(blocks, ez):
    rows = blocks[0].shape[0]
    lane = lane_of((rows, LANES))
    j, k = (lane >> 3) & 7, lane & 7
    outs = []
    for x in blocks:
        if rows > ez:
            edge = jnp.zeros((ez, LANES), jnp.float32)
            after = jnp.concatenate([roll(x[ez:], 56), edge], axis=0)
            before = jnp.concatenate([edge, roll(x[:-ez], -56)], axis=0)
            x = x + jnp.where(j == 7, after, jnp.where(j == 0, before, 0.0))
        up, down = roll(x, 7), roll(x, -7)
        after = [pltpu.roll(up[e : e + ez], ez - 1, 0) for e in range(0, rows, ez)]
        before = [pltpu.roll(down[e : e + ez], 1, 0) for e in range(0, rows, ez)]
        after, before = jnp.concatenate(after, 0), jnp.concatenate(before, 0)
        outs.append(x + jnp.where(k == 7, after, jnp.where(k == 0, before, 0.0)))
    return outs


def add_i_face(blocks, message, side):
    blocks = list(blocks)
    low = lane_of(blocks[0].shape) < 64
    face = unpack_i_face(message, side)
    blocks[3 * side] = blocks[3 * side] + jnp.where(low if side == 0 else ~low, face, 0.0)
    return blocks


def add_j_face(blocks, ez, same, before, after, side):
    lane = lane_of((ez, LANES))
    here = ((lane >> 3) & 7) == 7 * side

    def spread(message, shift):
        return jnp.concatenate([roll(message, shift), roll(message, shift - 32)], axis=0)

    outs = []
    for b, x in enumerate(blocks):
        shift = 56 * side - 8 * b
        face = jnp.where(here, spread(same, shift), 0.0)
        if b == 0:
            face = face + jnp.where(here & (lane < 64), spread(before, shift + 40), 0.0)
        if b == 3:
            face = face + jnp.where(here & (lane >= 64), spread(after, shift + 88), 0.0)
        if x.shape[0] == ez:
            outs.append(x + face)
        elif side == 0:
            outs.append(jnp.concatenate([x[:ez] + face, x[ez:]], axis=0))
        else:
            outs.append(jnp.concatenate([x[:-ez], x[-ez:] + face], axis=0))
    return outs


def halves(x):
    high = x.astype(jnp.bfloat16)
    return high, (x - high.astype(jnp.float32)).astype(jnp.bfloat16)


def dot(left, right):
    return jnp.dot(left, right, preferred_element_type=jnp.float32)


def stack(blocks):
    return jnp.concatenate(blocks, axis=0)


def total_of(blocks):
    x = blocks[0] + blocks[1] + (blocks[2] + blocks[3])
    return jnp.sum(jnp.sum(x, axis=0, keepdims=True), axis=1, keepdims=True)


def owner_weights(rows, ez, first_owned, last_owned, high_owned):
    lane = lane_of((rows, LANES))
    row = lax.broadcasted_iota(jnp.int32, (rows, LANES), 0)
    k, j = lane & 7, (lane >> 3) & 7
    base = jnp.where((k == 0) | (k == 7), 0.5, 1.0)
    first = jnp.where(row < ez, jnp.where(first_owned, 1.0, 0.0), 0.5)
    last = jnp.where(row >= rows - ez, jnp.where(last_owned, 1.0, 0.0), 0.5)
    base = base * jnp.where(j == 0, first, jnp.where(j == 7, last, 1.0))
    high = jnp.where(high_owned, 1.0, 0.0)
    return [jnp.where(lane < 64, 0.0, base), base, base, jnp.where(lane < 64, base, high * base)]


def kernel(
    ng, nd, ez,
    sol_h, res_h, dir_h, geo_h, mass_h, tab_h,
    outs,
    pair_v, dir_v, geo_v, tab_v,
    face_out, face_in, wrap_in, root_in, side_in, side_out, prev_v, next_v, high_v, part, parts, late_out, late,
    load_sem, send_sem, recv_sem, side_recv, last_recv, root_recv, part_recv, go,
):
    me_g, me_d = lax.axis_index("group"), lax.axis_index("dev")

    def at(a, b):
        return (lax.rem(me_g + (a + ng), ng), lax.rem(me_d + (b + nd), nd))

    others = [(a, b) for a in range(ng) for b in range(nd) if (a, b) != (0, 0)]
    others.sort(key=lambda t: (min(t[1], nd - t[1]) != 1, min(t[0], ng - t[0]) > 1))

    pairs = (
        (dir_h, dir_v, 0), (geo_h, geo_v.at[pl.ds(0, 3)], 1), (mass_h, geo_v.at[3], 1),
        (tab_h, tab_v, 2), (res_h, pair_v.at[0], 3), (sol_h, pair_v.at[1], 3),
    )
    loads = [pltpu.make_async_copy(h, v, load_sem.at[n]) for h, v, n in pairs]
    loads[0].start()
    barrier = pltpu.get_barrier_semaphore()
    partners = [t for t in others if min(t[0], ng - t[0]) < 2 and min(t[1], nd - t[1]) < 2]
    hub = (1 % ng, nd // 2)
    hub_a, hub_b = lax.rem(me_g - hub[0] + ng, ng), lax.rem(me_d - hub[1] + nd, nd)
    at_hub = (hub_a == 0) & (hub_b == 0)
    near_hub = ((hub_a < 2) | (hub_a == ng - 1)) & ((hub_b < 2) | (hub_b == nd - 1))
    for a, b in partners:
        pl.semaphore_signal(barrier, inc=1, device_id=at(a, b), device_id_type=MESH)

    @pl.when(jnp.logical_not(near_hub))
    def _():
        pl.semaphore_signal(barrier, inc=1, device_id=hub, device_id_type=MESH)

    for load in loads[1:]:
        load.start()

    rows = dir_v.shape[0]
    h, q = rows // 2, ez // 2
    u, span = h + q, 2 * h + 6 * q
    is_first, is_last, is_near = me_d == 0, me_d == nd - 1, me_d == nd - 2
    odd = (me_g & 1) == 1
    owns_next = me_d < nd - 2
    owns_high = jnp.logical_not(is_last & odd)

    def i_out(phase, side):
        return face_out.at[phase, pl.ds(u * side, h)]

    def i_in(phase, side):
        return face_in.at[pl.ds(span * phase + h * side, h)]

    def j_out(phase, side):
        return face_out.at[phase, pl.ds(2 * h + q if side == 0 else h, q)]

    def j_in(phase, side, turn):
        return face_in.at[pl.ds(span * phase + 2 * h + q * (3 * side + turn), q)]

    def slot(ref, part_of, group):
        return ref.at[pl.ds(pl.multiple_of(q * (ng * part_of + group), q), q)]

    def drain(count, sem):
        ref = face_in.at[pl.ds(0, count)]
        pltpu.make_async_copy(ref, ref, sem).wait()

    def send(src, dst, recv_to, target):
        return pltpu.make_async_remote_copy(
            src_ref=src, dst_ref=dst, send_sem=send_sem, recv_sem=recv_to,
            device_id=target, device_id_type=MESH,
        )

    weights = weights_of(rows)
    cut = [slice(LANES * b, LANES * b + LANES) for b in range(4)]

    def pack(phase, blocks):
        for side in range(2):
            j_out(phase, side)[...] = pack_j_face(blocks, ez, side)
            i_out(phase, side)[...] = pack_i_face(blocks[3 * side], side)

    def give_j(phase, side, step, sem):
        for turn, a in ((0, -1), (2, 1), (1, 0)):
            send(j_out(phase, side), j_in(phase, side, turn), sem, at(a, step)).start()

    def give_i(phase, sems):
        for side, step in ((0, -1), (1, 1)):
            send(i_out(phase, side), i_in(phase, side), sems[side], at(step, 0)).start()

    def give(phase, sems):
        give_j(phase, 0, -1, sems[2])
        give_j(phase, 1, 1, sems[3])
        give_i(phase, sems[:2])

    def turns(phase, side):
        return [j_in(phase, side, turn)[...] for turn in (1, 2, 0)]

    def assembled(phase, blocks):
        blocks = add_i_face(add_i_face(blocks, i_in(phase, 1)[...], 0), i_in(phase, 0)[...], 1)
        return add_j_face(add_j_face(blocks, ez, *turns(phase, 1), 0), ez, *turns(phase, 0), 1)

    d = derivative_table().astype(np.float32)
    loads[0].wait()
    weighted = assemble_inside([weights[b] * dir_v[:, cut[b]] for b in range(4)], ez)
    pack(0, weighted)
    pl.semaphore_wait(barrier, jnp.where(at_hub, len(others), len(partners)))
    give(0, [recv_sem.at[0]] * 4)

    @pl.when(at_hub)
    def _():
        for a, b in others:
            pl.semaphore_signal(go, inc=1, device_id=at(a, b), device_id_type=MESH)

    pltpu.make_async_copy(geo_v, geo_v, load_sem.at[1]).wait()
    loads[3].wait()
    geo_rows = stack([jnp.concatenate([geo_v[1, :, c], geo_v[2, :, c]], axis=1) for c in cut])
    squared = dot(geo_rows, tab_v[:, 768:1024])
    squared = squared[:, :LANES] + squared[:, LANES:]
    geo = [[geo_v[c, :, cut[b]].astype(jnp.float32) for b in range(4)] for c in range(3)]
    mass = [geo_v[3, :, c].astype(jnp.float32) for c in cut]
    diag = along_i((d * d).T, geo[0])
    diag = [diag[b] + squared[rows * b : rows * b + rows] + mass[b] for b in range(4)]
    diag = assemble_inside(diag, ez)
    pack(1, diag)
    give(1, [side_recv.at[0], side_recv.at[0], side_recv.at[1], side_recv.at[0]])
    pltpu.make_async_copy(pair_v, pair_v, load_sem.at[3]).wait()
    residual = [pair_v[0, :, c] for c in cut]
    spread_res = [weights[b] * residual[b] for b in range(4)]
    mixed = assemble_inside(spread_res, ez)
    pack(2, mixed)
    give(2, [recv_sem.at[1]] * 4)
    owned = owner_weights(rows, ez, is_last, owns_next, owns_high)

    @pl.when(jnp.logical_not(at_hub))
    def _():
        pl.semaphore_wait(go, 1)

    @pl.when(is_last)
    def _():
        drain(2 * h + 3 * q, side_recv.at[0])

    @pl.when(is_last & odd)
    def _():
        side = add_i_face(add_i_face(diag, i_in(1, 1)[...], 0), i_in(1, 0)[...], 1)
        side = [1.0 / x for x in add_j_face(side, ez, *turns(1, 1), 0)]
        lane = lane_of((h, LANES))
        row = lax.broadcasted_iota(jnp.int32, (h, LANES), 0) + jnp.where(lane < 64, 0, h)
        j, k = (lane >> 3) & 7, lane & 7
        fit = jnp.where(j == 0, jnp.where(row < ez, 1.0, 0.5), 1.0)
        fit = jnp.where(j == 7, jnp.where(row < rows - ez, 0.5, 0.0), fit)
        fit = fit * jnp.where((k == 0) | (k == 7), 0.5, 1.0)
        side_out[...] = fit * pack_i_face(side[3], 1)
        for g in range(ng):
            dst = side_in.at[pl.ds(pl.multiple_of((me_g >> 1) * h, q), h)]
            send(side_out, dst, root_recv.at[1], (g, 0)).start()

    drain(span, recv_sem.at[0])
    smooth = assembled(0, weighted)

    high, low = halves(stack(smooth))
    grads = dot(jnp.concatenate([high, low], axis=1), tab_v[:, :512])
    grads = grads[:, :256] + grads[:, 256:]
    grad_i = along_i(d, smooth)
    flux_i = [geo[0][b] * grad_i[b] for b in range(4)]
    flux = jnp.concatenate(
        [stack(geo[1]) * grads[:, :LANES], stack(geo[2]) * grads[:, LANES:]], axis=1
    )
    high, low = halves(flux)
    back = dot(jnp.concatenate([high, low], axis=0), tab_v[:, 512:768])
    back = back[: 4 * rows] + back[4 * rows :]
    back = back[:, :LANES] + back[:, LANES:]
    local = along_i(d.T, flux_i)
    local = [local[b] + back[rows * b : rows * b + rows] + mass[b] * smooth[b] for b in range(4)]

    inside = assemble_inside(local, ez)
    pack(3, inside)

    @pl.when(is_last)
    def _():
        for g in range(ng):
            start = pl.multiple_of((me_g & 1) * h, q)
            dst = wrap_in.at[pl.ds(pl.multiple_of(me_g * u, q), u)]
            send(face_out.at[3, pl.ds(start, u)], dst, root_recv.at[0], (g, 0)).start()

    @pl.when(is_near)
    def _():
        for g in range(ng):
            send(j_out(3, 1), slot(root_in, 2, me_g), root_recv.at[1], (g, 0)).start()

    give_i(3, [last_recv.at[0], last_recv.at[1]])
    give_j(3, 0, -1, last_recv.at[2])

    @pl.when(jnp.logical_not(is_last))
    def _():
        give_j(3, 1, 1, last_recv.at[3])

    @pl.when(is_first)
    def _():
        for a in range(1, ng):
            send(j_out(3, 0), slot(root_in, 0, me_g), root_recv.at[1], at(a, 0)).start()

    @pl.when(jnp.logical_not(is_last))
    def _():
        drain(2 * h + 3 * q, side_recv.at[0])

    drain(3 * q, side_recv.at[1])
    inverse = [1.0 / x for x in assembled(1, diag)]

    @pl.when(is_first)
    def _():
        lane = lane_of((q, LANES))
        ends = ((lane & 7) == 0) | ((lane & 7) == 7)
        share = jnp.where((lane < 64) & ((lane & 31) < 8), 0.0, jnp.where(ends, 0.5, 1.0))
        side_out[pl.ds(0, q)] = share * pack_j_face(inverse, ez, 0)
        for a in range(1, ng):
            send(side_out.at[pl.ds(0, q)], slot(root_in, 1, me_g), root_recv.at[1], at(a, 0)).start()

    drain(span, recv_sem.at[1])
    dual = assembled(2, mixed)
    norm_now = total_of([spread_res[b] * residual[b] * inverse[b] for b in range(4)])
    curvature = total_of([smooth[b] * local[b] for b in range(4)])
    cross = total_of([local[b] * dual[b] * inverse[b] for b in range(4)])
    share = [owned[b] * inverse[b] for b in range(4)]

    def hold(ref, side):
        for n, value in enumerate(turns(3, side)):
            ref[pl.ds(q * n, q)] = value

    def held(ref):
        return [ref[pl.ds(q * n, q)] for n in range(3)]

    @pl.when(owns_high)
    def _():
        drain(h, last_recv.at[0])
        high_v[...] = i_in(3, 0)[...]

    @pl.when(jnp.logical_not(owns_high))
    def _():
        high_v[...] = jnp.zeros_like(high_v)

    @pl.when(owns_next)
    def _():
        drain(3 * q, last_recv.at[2])
        hold(next_v, 0)

    @pl.when(jnp.logical_not(owns_next))
    def _():
        next_v[...] = jnp.zeros_like(next_v)

    @pl.when(is_last)
    def _():
        drain(3 * q, last_recv.at[3])
        hold(prev_v, 1)

    @pl.when(jnp.logical_not(is_last))
    def _():
        prev_v[...] = jnp.zeros_like(prev_v)

    mostly = add_i_face(inside, high_v[...], 1)
    mostly = add_j_face(add_j_face(mostly, ez, *held(prev_v), 0), ez, *held(next_v), 1)
    quad = total_of([share[b] * mostly[b] * mostly[b] for b in range(4)])

    lane = lane_of((1, LANES))
    mine = jnp.where(
        lane < 32, norm_now, jnp.where(lane < 64, curvature, jnp.where(lane < 96, cross, quad))
    )
    part[0] = mine
    order = sorted(range(len(others)), key=lambda n: (others[n][1] != 0, others[n][1] != 1))
    for n in order:
        a, b = others[n]
        send(part.at[0], parts.at[n], part_recv, at(a, b)).start()

    @pl.when(is_first)
    def _():
        slot(root_in, 0, me_g)[...] = j_out(3, 0)[...]
        slot(root_in, 1, me_g)[...] = side_out[pl.ds(0, q)]
        drain((3 * ng - 2) * q + ng // 2 * h, root_recv.at[1])
        drain(ng * u, root_recv.at[0])

        def far(g):
            return wrap_in[pl.ds(u * g + (0 if g & 1 else h), q)]

        def across(g):
            return wrap_in[pl.ds(u * g + (q if g & 1 else 0), h)]

        def near(g):
            return root_in[pl.ds(q * (2 * ng + g), q)]

        spot = lane_of((q, LANES))
        seam = (spot >= 64) & ((spot & 31) >= 24)
        faces = [far(g) + root_in[pl.ds(q * g, q)] for g in range(ng)]
        total = None
        for g in range(ng):
            face = faces[g] + jnp.where(seam, roll(faces[(g + 1) % ng], 88), 0.0)
            term = face * face * root_in[pl.ds(q * (ng + g), q)]
            total = term if total is None else total + term
        spot = lane_of((ez, LANES))
        for g in range(1, ng, 2):
            one, two = near(g), near((g + 1) % ng)
            line = jnp.concatenate([roll(one, -88) + two, roll(one, -120) + roll(two, -32)], axis=0)
            line = jnp.where(spot < 8, line, 0.0)
            if h > ez:
                line = jnp.concatenate([line, jnp.zeros((h - ez, LANES), jnp.float32)], axis=0)
            face = across(g) + across((g + 1) % ng) + line
            term = face * face * side_in[pl.ds(h * (g // 2), h)]
            for n in range(0, h, q):
                total = total + term[n : n + q]
        total = jnp.sum(jnp.sum(total, axis=0, keepdims=True), axis=1, keepdims=True)
        late[0] = jnp.broadcast_to(total, (1, LANES))
        late_out[0] = jnp.broadcast_to(total, (1, LANES))
        for n, shift in enumerate((0, ng - 1, 1)):
            g = lax.rem(me_g + shift, ng)
            prev_v[pl.ds(q * n, q)] = wrap_in[pl.ds(pl.multiple_of(u * g + h * (1 - (g & 1)), q), q)]

    speaks = is_first & odd

    @pl.when(speaks)
    def _():
        for b in range(1, nd):
            for a in (0, -1):
                send(late_out.at[0], late.at[0], root_recv.at[2], at(a, b)).start()

    drain(h, last_recv.at[1])

    @pl.when(jnp.logical_not(owns_high))
    def _():
        drain(h, last_recv.at[0])
        high_v[...] = i_in(3, 0)[...]

    @pl.when(jnp.logical_not(owns_next))
    def _():
        drain(3 * q, last_recv.at[2])
        hold(next_v, 0)

    @pl.when(jnp.logical_not(is_last | is_first))
    def _():
        drain(3 * q, last_recv.at[3])
        hold(prev_v, 1)

    applied = add_i_face(add_i_face(inside, high_v[...], 1), i_in(3, 1)[...], 0)
    applied = add_j_face(add_j_face(applied, ez, *held(prev_v), 0), ez, *held(next_v), 1)

    @pl.when(jnp.logical_not(is_first))
    def _():
        pltpu.make_async_copy(late, late, root_recv.at[2]).wait()

    pltpu.make_async_copy(parts, parts, part_recv).wait()
    everyone = mine + jnp.sum(parts[...], axis=0)
    norm_now, curvature, cross, quad = (everyone[:, 32 * n : 32 * n + 1] for n in range(4))
    quad = quad + late[0][:, :1]
    step = norm_now / curvature
    norm_next = norm_now - 2.0 * step * cross + step * step * quad
    ratio = norm_next / norm_now
    for b, c in enumerate(cut):
        outs[0, :, c] = pair_v[1, :, c] + step * smooth[b]
        out = residual[b] - step * applied[b]
        outs[1, :, c] = out
        outs[2, :, c] = out * inverse[b] + ratio * smooth[b]
    common = 4 * span + len(others)
    roles = [
        (is_first & odd, 2 * (ng - 1) * q + 2 * (nd - 1)),
        (is_first & jnp.logical_not(odd), 2 * (ng - 1) * q),
        (is_last & odd, ng * (u + h) - 3 * q),
        (is_last & jnp.logical_not(odd), ng * u - 3 * q),
        (is_near, ng * q),
        (jnp.logical_not(is_first | is_last | is_near), 0),
    ]
    for role, extra in roles:

        @pl.when(role)
        def _():
            drain(common + extra, send_sem)


def deliver(stacked, *refs):
    for n in range(3):
        pltpu.make_async_copy(stacked.at[n], refs[n], refs[3]).start()
    pltpu.make_async_copy(stacked, stacked, refs[3]).wait()


def on_device(solution, residual, direction, geometry, mass):
    dims = solution.shape
    ng, nd = lax.axis_size("group"), lax.axis_size("dev")
    ez, points = dims[2], dims[3]
    rows = dims[0] * dims[1] * ez
    flat = (rows, points)
    f32, bf16 = jnp.float32, jnp.bfloat16
    table = jnp.asarray(tables())
    h, q = rows // 2, ez // 2
    u, q8 = h + q, 8
    spare = 4 * (2 * h + 6 * q) + ng * nd + 2 * nd + ng * (u + h)
    spare = -(-spare // q8) * q8
    stacked = pl.pallas_call(
        functools.partial(kernel, ng, nd, ez),
        out_shape=pltpu.VMEM((3,) + flat, f32),
        in_specs=[pl.BlockSpec(memory_space=pltpu.HBM)] * 6,
        out_specs=pl.BlockSpec(memory_space=pltpu.VMEM),
        scratch_shapes=[
            pltpu.VMEM((2,) + flat, f32),
            pltpu.VMEM(flat, f32),
            pltpu.VMEM((4,) + flat, bf16),
            pltpu.VMEM(table.shape, bf16),
            pltpu.VMEM((4, 2 * u, LANES), f32),
            pltpu.VMEM((spare, LANES), f32),
            pltpu.VMEM((ng * u, LANES), f32),
            pltpu.VMEM((3 * ng * q, LANES), f32),
            pltpu.VMEM((ng // 2 * h, LANES), f32),
            pltpu.VMEM((h, LANES), f32),
            pltpu.VMEM((3 * q, LANES), f32),
            pltpu.VMEM((3 * q, LANES), f32),
            pltpu.VMEM((h, LANES), f32),
            pltpu.VMEM((1, 1, LANES), f32),
            pltpu.VMEM((ng * nd - 1, 1, LANES), f32),
            pltpu.VMEM((1, 1, LANES), f32),
            pltpu.VMEM((1, 1, LANES), f32),
            pltpu.SemaphoreType.DMA((4,)),
            pltpu.SemaphoreType.DMA,
            pltpu.SemaphoreType.DMA((2,)),
            pltpu.SemaphoreType.DMA((2,)),
            pltpu.SemaphoreType.DMA((4,)),
            pltpu.SemaphoreType.DMA((3,)),
            pltpu.SemaphoreType.DMA,
            pltpu.SemaphoreType.REGULAR,
        ],
        compiler_params=pltpu.CompilerParams(collective_id=0, has_side_effects=True, vmem_limit_bytes=8 << 20),
    )(
        pltpu.with_memory_space_constraint(solution.reshape(flat), pltpu.HBM),
        pltpu.with_memory_space_constraint(residual.reshape(flat), pltpu.HBM),
        pltpu.with_memory_space_constraint(direction.reshape(flat), pltpu.HBM),
        pltpu.with_memory_space_constraint(geometry.reshape((3,) + flat), pltpu.HBM),
        pltpu.with_memory_space_constraint(mass.reshape(flat), pltpu.HBM),
        pltpu.with_memory_space_constraint(table, pltpu.HBM),
    )
    outs = pl.pallas_call(
        deliver,
        out_shape=[jax.ShapeDtypeStruct(flat, f32)] * 3,
        in_specs=[pl.BlockSpec(memory_space=pl.ANY)],
        out_specs=[pl.BlockSpec(memory_space=pltpu.HBM)] * 3,
        scratch_shapes=[pltpu.SemaphoreType.DMA],
        compiler_params=pltpu.CompilerParams(vmem_limit_bytes=8 << 20),
    )(stacked)
    return tuple(x.reshape(dims) for x in outs)


def solution(mesh):
    spec = P("group", "dev", None, None)
    return jax.shard_map(
        on_device,
        mesh=mesh,
        in_specs=(spec, spec, spec, P(None, "group", "dev", None, None), spec),
        out_specs=(spec, spec, spec),
        check_vma=False,
    )
```

```python
import functools

import jax
import jax.numpy as jnp
import numpy as np
from jax import lax
from jax.experimental import pallas as pl
from jax.experimental.pallas import tpu as pltpu
from jax.sharding import PartitionSpec as P

NP = 8
LANES = 128
MESH = pl.DeviceIdType.MESH

lobatto_nodes = [
    -1.0,
    -0.8717401485096066,
    -0.5917001814331423,
    -0.2092992179024789,
    0.2092992179024789,
    0.5917001814331423,
    0.8717401485096066,
    1.0,
]


def derivative_table():
    nodes = np.array(lobatto_nodes)
    identity = np.eye(NP)
    offset = nodes[:, None] - nodes[None, :] + identity
    barycentric = 1.0 / np.prod(offset, axis=1)
    derivative = barycentric[None, :] / barycentric[:, None] / offset * (1.0 - identity)
    return derivative - identity * np.sum(derivative, axis=1)[:, None]


def split_table(table):
    table = np.asarray(table, np.float32)
    high = table.astype(jnp.bfloat16)
    low = (table - high.astype(np.float32)).astype(jnp.bfloat16)
    return high, low


def tables():
    d = derivative_table().astype(np.float32)
    along_j = np.kron(np.kron(np.eye(2), d), np.eye(NP))
    along_k = np.kron(np.eye(16), d)
    high, low = split_table(np.concatenate([along_j.T, along_k.T], axis=1))
    forward = np.concatenate([np.concatenate([high, high], 0), np.concatenate([low, low], 0)], 1)
    high, low = split_table(np.concatenate([along_j, along_k], axis=0))
    backward = np.concatenate([high, low], axis=1)
    high, low = split_table(np.concatenate([along_j * along_j, along_k * along_k], axis=0))
    squares = np.concatenate([high, low], axis=1)
    return np.concatenate([forward, backward, squares], axis=1)


def roll(x, shift):
    shift %= LANES
    return x if shift == 0 else pltpu.roll(x, shift, 1)


def lane_of(shape):
    return lax.broadcasted_iota(jnp.int32, shape, 1)


def along_i(table, blocks):
    low = lane_of(blocks[0].shape) < 64
    swapped = [roll(x, 64) for x in blocks]
    outs = []
    for b in range(4):
        total = None
        for c in range(4):
            same = jnp.where(low, float(table[2 * b, 2 * c]), float(table[2 * b + 1, 2 * c + 1]))
            other = jnp.where(low, float(table[2 * b, 2 * c + 1]), float(table[2 * b + 1, 2 * c]))
            term = same * blocks[c] + other * swapped[c]
            total = term if total is None else total + term
        outs.append(total)
    return outs


def weights_of(rows):
    lane = lane_of((rows, LANES))
    k, j = lane & 7, (lane >> 3) & 7
    half = lambda cond: jnp.where(cond, 0.5, 1.0)
    base = half((k == 0) | (k == 7)) * half((j == 0) | (j == 7))
    return [base * half(lane < 64), base, base, base * half(lane >= 64)]


def pack_i_face(x, side):
    h = x.shape[0] // 2
    top, bottom = x[:h], x[h:]
    low = lane_of(top.shape) < 64
    if side == 0:
        return jnp.where(low, top, roll(bottom, 64))
    return jnp.where(low, roll(top, 64), bottom)


def unpack_i_face(m, side):
    other = roll(m, 64)
    return jnp.concatenate([m, other] if side == 0 else [other, m], axis=0)


def pack_j_face(blocks, ez, side):
    half = ez // 2
    lane = lane_of((half, LANES))
    slot = (lane & 63) >> 3
    out = jnp.zeros((half, LANES), jnp.float32)
    for b in range(4):
        rows = blocks[b][:ez] if side == 0 else blocks[b][-ez:]
        for n in range(2):
            moved = roll(rows[n * half : (n + 1) * half], 8 * b + 32 * n - (0 if side == 0 else 56))
            out = jnp.where(slot == b + 4 * n, moved, out)
    return out


def assemble_inside(blocks, ez):
    rows = blocks[0].shape[0]
    lane = lane_of((rows, LANES))
    j, k = (lane >> 3) & 7, lane & 7
    outs = []
    for x in blocks:
        if rows > ez:
            edge = jnp.zeros((ez, LANES), jnp.float32)
            after = jnp.concatenate([roll(x[ez:], 56), edge], axis=0)
            before = jnp.concatenate([edge, roll(x[:-ez], -56)], axis=0)
            x = x + jnp.where(j == 7, after, jnp.where(j == 0, before, 0.0))
        up, down = roll(x, 7), roll(x, -7)
        after = [pltpu.roll(up[e : e + ez], ez - 1, 0) for e in range(0, rows, ez)]
        before = [pltpu.roll(down[e : e + ez], 1, 0) for e in range(0, rows, ez)]
        after, before = jnp.concatenate(after, 0), jnp.concatenate(before, 0)
        outs.append(x + jnp.where(k == 7, after, jnp.where(k == 0, before, 0.0)))
    return outs


def turn_column(x, ez, shift):
    parts = [pltpu.roll(x[e : e + ez], shift % ez, 0) for e in range(0, x.shape[0], ez)]
    return parts[0] if len(parts) == 1 else jnp.concatenate(parts, axis=0)


def summed_j_face(blocks, ez, side):
    half = ez // 2
    lane = lane_of((half, LANES))
    slot, k = (lane & 63) >> 3, lane & 7
    kept = [jnp.zeros((half, LANES), jnp.float32)] * 3
    for b in range(4):
        column = blocks[b][:ez] if side == 0 else blocks[b][-ez:]
        kinds = ((column, 0), (turn_column(column, ez, -1), 7), (turn_column(column, ez, 1), -7))
        for n in range(2):
            shift = 8 * b + 32 * n - 56 * side
            for m, (rows, extra) in enumerate(kinds):
                moved = roll(rows[n * half : (n + 1) * half], shift + extra)
                kept[m] = jnp.where(slot == b + 4 * n, moved, kept[m])
    return kept[0] + jnp.where(k == 7, kept[1], jnp.where(k == 0, kept[2], 0.0))


def summed_i_face(x, ez, side):
    rows = x.shape[0]
    h = rows // 2
    lane = lane_of((h, LANES))
    j, k = (lane >> 3) & 7, lane & 7
    edge = jnp.zeros((ez, LANES), jnp.float32)

    def gather(bottom):
        cut = slice(h, rows) if bottom else slice(0, h)
        base = 64 if bottom != (side == 1) else 0
        total = None
        for column, shift, where in ((0, 0, None), (1, 56, j == 7), (-1, -56, j == 0)):
            if column and (rows == ez or (rows == 2 * ez and bottom == (column == 1))):
                continue
            found = None
            for turn, extra, only in ((0, 0, None), (-1, 7, k == 7), (1, -7, k == 0)):
                y = turn_column(x, ez, turn) if turn else x
                if column == 1:
                    y = jnp.concatenate([y[ez:], edge], axis=0)
                elif column == -1:
                    y = jnp.concatenate([edge, y[:-ez]], axis=0)
                y = roll(y[cut], base + shift + extra)
                y = y if only is None else jnp.where(only, y, 0.0)
                found = y if found is None else found + y
            found = found if where is None else jnp.where(where, found, 0.0)
            total = found if total is None else total + found
        return total

    return jnp.where(lane < 64, gather(False), gather(True))


def add_i_face(blocks, message, side):
    blocks = list(blocks)
    low = lane_of(blocks[0].shape) < 64
    face = unpack_i_face(message, side)
    blocks[3 * side] = blocks[3 * side] + jnp.where(low if side == 0 else ~low, face, 0.0)
    return blocks


def add_j_face(blocks, ez, same, before, after, side):
    lane = lane_of((ez, LANES))
    here = ((lane >> 3) & 7) == 7 * side

    def spread(message, shift):
        return jnp.concatenate([roll(message, shift), roll(message, shift - 32)], axis=0)

    outs = []
    for b, x in enumerate(blocks):
        shift = 56 * side - 8 * b
        face = jnp.where(here, spread(same, shift), 0.0)
        if b == 0:
            face = face + jnp.where(here & (lane < 64), spread(before, shift + 40), 0.0)
        if b == 3:
            face = face + jnp.where(here & (lane >= 64), spread(after, shift + 88), 0.0)
        if x.shape[0] == ez:
            outs.append(x + face)
        elif side == 0:
            outs.append(jnp.concatenate([x[:ez] + face, x[ez:]], axis=0))
        else:
            outs.append(jnp.concatenate([x[:-ez], x[-ez:] + face], axis=0))
    return outs


def halves(x):
    high = x.astype(jnp.bfloat16)
    return high, (x - high.astype(jnp.float32)).astype(jnp.bfloat16)


def dot(left, right):
    return jnp.dot(left, right, preferred_element_type=jnp.float32)


def stack(blocks):
    return jnp.concatenate(blocks, axis=0)


def total_of(blocks):
    x = blocks[0] + blocks[1] + (blocks[2] + blocks[3])
    return jnp.sum(jnp.sum(x, axis=0, keepdims=True), axis=1, keepdims=True)


def owner_weights(rows, ez, first_owned, last_owned, high_owned):
    lane = lane_of((rows, LANES))
    row = lax.broadcasted_iota(jnp.int32, (rows, LANES), 0)
    k, j = lane & 7, (lane >> 3) & 7
    base = jnp.where((k == 0) | (k == 7), 0.5, 1.0)
    first = jnp.where(row < ez, jnp.where(first_owned, 1.0, 0.0), 0.5)
    last = jnp.where(row >= rows - ez, jnp.where(last_owned, 1.0, 0.0), 0.5)
    base = base * jnp.where(j == 0, first, jnp.where(j == 7, last, 1.0))
    high = jnp.where(high_owned, 1.0, 0.0)
    outer = [jnp.where(lane < 64, 0.0, base), base, base, jnp.where(lane < 64, base, high * base)]
    return outer, base


def kernel(
    ng, nd, ez,
    sol_h, res_h, dir_h, geo_h, mass_h, tab_h,
    outs,
    pair_v, dir_v, geo_v, tab_v, early_v,
    face_out, face_in, wrap_in, root_in, side_in, side_out, prev_v, next_v, low_v, high_v, part, sums, parts, late_out,
    bulk, load_sem, send_sem, recv_sem, side_recv, last_recv, root_recv, sum_recv, part_recv, go,
):
    me_g, me_d = lax.axis_index("group"), lax.axis_index("dev")

    def at(a, b):
        return (lax.rem(me_g + (a + ng), ng), lax.rem(me_d + (b + nd), nd))

    others = [(a, b) for a in range(ng) for b in range(nd) if (a, b) != (0, 0)]
    others.sort(key=lambda t: (min(t[1], nd - t[1]) != 1, min(t[0], ng - t[0]) > 1))

    pairs = (
        (dir_h, dir_v, 0), (geo_h, geo_v.at[pl.ds(0, 3)], 1), (mass_h, geo_v.at[3], 1),
        (tab_h, tab_v, 1), (res_h, pair_v.at[0], 1), (sol_h, pair_v.at[1], 1),
    )
    loads = [pltpu.make_async_copy(h, v, load_sem.at[n]) for h, v, n in pairs]
    loads[0].start()
    barrier = pltpu.get_barrier_semaphore()
    partners = [t for t in others if min(t[0], ng - t[0]) < 2 and min(t[1], nd - t[1]) < 2]
    hub = (1 % ng, nd // 2)
    hub_a, hub_b = lax.rem(me_g - hub[0] + ng, ng), lax.rem(me_d - hub[1] + nd, nd)
    at_hub = (hub_a == 0) & (hub_b == 0)
    near_hub = ((hub_a < 2) | (hub_a == ng - 1)) & ((hub_b < 2) | (hub_b == nd - 1))
    for a, b in partners:
        pl.semaphore_signal(barrier, inc=1, device_id=at(a, b), device_id_type=MESH)

    @pl.when(jnp.logical_not(near_hub))
    def _():
        pl.semaphore_signal(barrier, inc=1, device_id=hub, device_id_type=MESH)

    for load in loads[1:]:
        load.start()

    rows = dir_v.shape[0]
    h, q = rows // 2, ez // 2
    u, span = h + q, 2 * h + 6 * q
    is_first, is_last, is_near = me_d == 0, me_d == nd - 1, me_d == nd - 2
    root = min(1, ng - 1)
    is_root = is_first & (me_g == root)
    odd = (me_g & 1) == 1
    owns_next = me_d < nd - 2
    owns_high, owns_low = jnp.logical_not(is_last), is_last & odd

    def i_out(phase, side):
        return face_out.at[phase, pl.ds(u * side, h)]

    def i_in(phase, side):
        return face_in.at[pl.ds(span * phase + h * side, h)]

    def j_out(phase, side):
        return face_out.at[phase, pl.ds(2 * h + q if side == 0 else h, q)]

    def j_in(phase, side, turn):
        return face_in.at[pl.ds(span * phase + 2 * h + q * (3 * side + turn), q)]

    def slot(ref, part_of, group):
        return ref.at[pl.ds(pl.multiple_of(q * (ng * part_of + group), q), q)]

    def drain(count, sem):
        ref = face_in.at[pl.ds(0, count)]
        pltpu.make_async_copy(ref, ref, sem).wait()

    def send(src, dst, recv_to, target):
        return pltpu.make_async_remote_copy(
            src_ref=src, dst_ref=dst, send_sem=send_sem, recv_sem=recv_to,
            device_id=target, device_id_type=MESH,
        )

    weights = weights_of(rows)
    cut = [slice(LANES * b, LANES * b + LANES) for b in range(4)]

    def pack(phase, blocks):
        for side in range(2):
            j_out(phase, side)[...] = pack_j_face(blocks, ez, side)
            i_out(phase, side)[...] = pack_i_face(blocks[3 * side], side)

    def give_j(phase, side, step, sem):
        for turn, a in ((2, 1), (0, -1), (1, 0)):
            send(j_out(phase, side), j_in(phase, side, turn), sem, at(a, step)).start()

    def give_i(phase, sems):
        for side, step in ((0, -1), (1, 1)):
            send(i_out(phase, side), i_in(phase, side), sems[side], at(step, 0)).start()

    def give(phase, sems):
        give_j(phase, 0, -1, sems[2])
        give_j(phase, 1, 1, sems[3])
        give_i(phase, sems[:2])

    def turns(phase, side):
        return [j_in(phase, side, turn)[...] for turn in (1, 2, 0)]

    def assembled(phase, blocks):
        blocks = add_i_face(add_i_face(blocks, i_in(phase, 1)[...], 0), i_in(phase, 0)[...], 1)
        return add_j_face(add_j_face(blocks, ez, *turns(phase, 1), 0), ez, *turns(phase, 0), 1)

    d = derivative_table().astype(np.float32)
    loads[0].wait()
    weighted = assemble_inside([weights[b] * dir_v[:, cut[b]] for b in range(4)], ez)
    pack(0, weighted)
    pl.semaphore_wait(barrier, jnp.where(at_hub, len(others), len(partners)))
    give(0, [recv_sem] * 4)

    @pl.when(at_hub)
    def _():
        for a, b in others:
            pl.semaphore_signal(go, inc=1, device_id=at(a, b), device_id_type=MESH)

    pltpu.make_async_copy(bulk, bulk, load_sem.at[1]).wait()
    geo_rows = stack([jnp.concatenate([geo_v[1, :, c], geo_v[2, :, c]], axis=1) for c in cut])
    squared = dot(geo_rows, tab_v[:, 768:1024])
    squared = squared[:, :LANES] + squared[:, LANES:]
    geo = [[geo_v[c, :, cut[b]].astype(jnp.float32) for b in range(4)] for c in range(3)]
    mass = [geo_v[3, :, c].astype(jnp.float32) for c in cut]
    diag = along_i((d * d).T, geo[0])
    diag = [diag[b] + squared[rows * b : rows * b + rows] + mass[b] for b in range(4)]
    diag = assemble_inside(diag, ez)
    pack(1, diag)
    give(1, [side_recv.at[0], side_recv.at[0], side_recv.at[1], side_recv.at[0]])
    residual = [pair_v[0, :, c] for c in cut]
    spread_res = [weights[b] * residual[b] for b in range(4)]
    mixed = assemble_inside(spread_res, ez)
    pack(2, mixed)
    give(2, [side_recv.at[0], side_recv.at[0], side_recv.at[1], side_recv.at[0]])
    owned, face_owned = owner_weights(rows, ez, is_last, owns_next, owns_high)

    @pl.when(jnp.logical_not(at_hub))
    def _():
        pl.semaphore_wait(go, 1)

    def nearly(phase, blocks):
        blocks = add_i_face(add_i_face(blocks, i_in(phase, 1)[...], 0), i_in(phase, 0)[...], 1)
        return add_j_face(blocks, ez, *turns(phase, 1), 0)

    def gather_sides():
        drain(2 * (2 * h + 3 * q), side_recv.at[0])
        for b, x in enumerate(nearly(1, [early_v[0, :, c] for c in cut])):
            early_v[0, :, cut[b]] = x
            early_v[2, :, cut[b]] = 1.0 / x
        for b, x in enumerate(nearly(2, [early_v[1, :, c] for c in cut])):
            early_v[1, :, cut[b]] = x

    for b, c in enumerate(cut):
        early_v[0, :, c] = diag[b]
        early_v[1, :, c] = mixed[b]

    @pl.when(is_last)
    def _():
        gather_sides()

    @pl.when(is_last & odd)
    def _():
        lane = lane_of((h, LANES))
        row = lax.broadcasted_iota(jnp.int32, (h, LANES), 0) + jnp.where(lane < 64, 0, h)
        j, k = (lane >> 3) & 7, lane & 7
        fit = jnp.where(j == 0, jnp.where(row < ez, 1.0, 0.5), 1.0)
        fit = jnp.where(j == 7, jnp.where(row < rows - ez, 0.5, 0.0), fit)
        fit = fit * jnp.where((k == 0) | (k == 7), 0.5, 1.0)
        side_out[...] = fit * pack_i_face(early_v[2, :, cut[3]], 1)
        dst = side_in.at[pl.ds(pl.multiple_of((me_g >> 1) * h, q), h)]
        send(side_out, dst, root_recv, (root, 0)).start()

    drain(span, recv_sem)
    smooth = assembled(0, weighted)

    high, low = halves(stack(smooth))
    grads = dot(jnp.concatenate([high, low], axis=1), tab_v[:, :512])
    grads = grads[:, :256] + grads[:, 256:]
    grad_i = along_i(d, smooth)
    flux_i = [geo[0][b] * grad_i[b] for b in range(4)]
    flux = jnp.concatenate(
        [stack(geo[1]) * grads[:, :LANES], stack(geo[2]) * grads[:, LANES:]], axis=1
    )
    high, low = halves(flux)
    back = dot(jnp.concatenate([high, low], axis=0), tab_v[:, 512:768])
    back = back[: 4 * rows] + back[4 * rows :]
    back = back[:, :LANES] + back[:, LANES:]
    local = along_i(d.T, flux_i)
    local = [local[b] + back[rows * b : rows * b + rows] + mass[b] * smooth[b] for b in range(4)]

    for side in range(2):
        j_out(3, side)[...] = summed_j_face(local, ez, side)
        i_out(3, side)[...] = summed_i_face(local[3 * side], ez, side)

    @pl.when(is_last)
    def _():
        start = pl.multiple_of((me_g & 1) * h, q)
        dst = wrap_in.at[pl.ds(pl.multiple_of(me_g * u, q), u)]
        send(face_out.at[3, pl.ds(start, u)], dst, root_recv, (root, 0)).start()

    def wrap_target(a):
        return lax.rem(me_g + (a + ng), ng)

    def give_wrap(first):
        for turn, a in ((2, 1), (0, -1), (1, 0)):
            target = wrap_target(a)
            wanted = target == 0 if first else (target != 0) & (target != root)

            @pl.when(is_last & wanted)
            def _():
                send(j_out(3, 1), j_in(3, 1, turn), last_recv.at[3], (target, 0)).start()

    give_wrap(True)

    @pl.when(is_near)
    def _():
        send(j_out(3, 1), slot(root_in, 2, me_g), root_recv, (root, 0)).start()

    give_i(3, [last_recv.at[0], last_recv.at[1]])
    give_j(3, 0, -1, last_recv.at[2])

    @pl.when(jnp.logical_not(is_last))
    def _():
        give_j(3, 1, 1, last_recv.at[3])

    @pl.when(is_first & (me_g != root))
    def _():
        send(j_out(3, 0), slot(root_in, 0, me_g), root_recv, (root, 0)).start()

    inside = assemble_inside(local, ez)

    @pl.when(jnp.logical_not(is_last))
    def _():
        gather_sides()

    drain(6 * q, side_recv.at[1])
    inverse = add_j_face([early_v[0, rows - ez :, c] for c in cut], ez, *turns(1, 0), 1)
    inverse = [1.0 / x for x in inverse]
    if rows > ez:
        kept = slice(0, rows - ez)
        inverse = [jnp.concatenate([early_v[2, kept, cut[b]], inverse[b]], axis=0) for b in range(4)]
    mixed = [early_v[1, :, c] for c in cut]

    @pl.when(is_first)
    def _():
        lane = lane_of((q, LANES))
        ends = ((lane & 7) == 0) | ((lane & 7) == 7)
        share = jnp.where((lane < 64) & ((lane & 31) < 8), 0.0, jnp.where(ends, 0.5, 1.0))
        side_out[pl.ds(0, q)] = share * pack_j_face(inverse, ez, 0)

    @pl.when(is_first & (me_g != root))
    def _():
        send(side_out.at[pl.ds(0, q)], slot(root_in, 1, me_g), root_recv, (root, 0)).start()

    dual = add_j_face(mixed, ez, *turns(2, 0), 1)
    norm_now = total_of([spread_res[b] * residual[b] * inverse[b] for b in range(4)])
    curvature = total_of([smooth[b] * local[b] for b in range(4)])
    cross = total_of([local[b] * dual[b] * inverse[b] for b in range(4)])
    share = [owned[b] * inverse[b] for b in range(4)]
    order = sorted(range(len(others)), key=lambda n: (others[n][1] != 1, others[n][1] != 0))

    def tell(row, table, sem, which=None):
        for n in order:
            a, b = others[n]
            if which is not None and which != (b == 1):
                continue
            send(part.at[pl.ds(row, 1)], table.at[pl.ds(n, 1)], sem, at(a, b)).start()

    lane = lane_of((1, LANES))
    early = jnp.where(lane < 32, norm_now, jnp.where(lane < 64, curvature, cross))
    part[pl.ds(0, 1)] = early

    @pl.when(jnp.logical_not(is_last))
    def _():
        tell(0, sums, sum_recv)

    @pl.when(is_last)
    def _():
        tell(0, sums, sum_recv, True)


    def hold(ref, side):
        for n, value in enumerate(turns(3, side)):
            ref[pl.ds(q * n, q)] = value

    def held(ref):
        return [ref[pl.ds(q * n, q)] for n in range(3)]

    @pl.when(owns_high)
    def _():
        drain(h, last_recv.at[0])
        high_v[...] = i_in(3, 0)[...]

    @pl.when(is_last)
    def _():
        high_v[...] = jnp.zeros_like(high_v)

    @pl.when(owns_next)
    def _():
        drain(3 * q, last_recv.at[2])
        hold(next_v, 0)

    @pl.when(jnp.logical_not(owns_next))
    def _():
        next_v[...] = jnp.zeros_like(next_v)

    @pl.when(is_last)
    def _():
        drain(3 * q, last_recv.at[3])
        hold(prev_v, 1)

    @pl.when(jnp.logical_not(is_last))
    def _():
        prev_v[...] = jnp.zeros_like(prev_v)

    mostly = add_i_face(inside, high_v[...], 1)
    mostly = add_j_face(add_j_face(mostly, ez, *held(prev_v), 0), ez, *held(next_v), 1)
    quad = stack([share[b] * mostly[b] * mostly[b] for b in range(4)])
    quad = jnp.sum(quad, axis=0, keepdims=True)
    part[pl.ds(1, 1)] = quad

    @pl.when(owns_low)
    def _():
        face = pack_i_face(mostly[0], 0)
        fit = pack_i_face(face_owned * inverse[0], 0)
        drain(h, last_recv.at[1])
        met = i_in(3, 1)[...]
        low_v[...] = met
        face = face + met
        part[pl.ds(1, 1)] = quad + jnp.sum(face * face * fit, axis=0, keepdims=True)

    @pl.when(jnp.logical_not(is_last))
    def _():
        tell(1, parts, part_recv)

    @pl.when(is_last)
    def _():
        tell(1, parts, part_recv)
        tell(0, sums, sum_recv, False)

    give_wrap(False)

    @pl.when(is_root)
    def _():
        slot(root_in, 0, me_g)[...] = j_out(3, 0)[...]
        slot(root_in, 1, me_g)[...] = side_out[pl.ds(0, q)]
        drain((3 * ng - 2) * q + ng // 2 * h + ng * u, root_recv)

        def far(g):
            return wrap_in[pl.ds(u * g + (0 if g & 1 else h), q)]

        def across(g):
            return wrap_in[pl.ds(u * g + (q if g & 1 else 0), h)]

        def near(g):
            return root_in[pl.ds(q * (2 * ng + g), q)]

        spot = lane_of((q, LANES))
        seam = (spot >= 64) & ((spot & 31) >= 24)
        faces = [far(g) + root_in[pl.ds(q * g, q)] for g in range(ng)]
        total = None
        for g in range(ng):
            face = faces[g] + jnp.where(seam, roll(faces[(g + 1) % ng], 88), 0.0)
            term = face * face * root_in[pl.ds(q * (ng + g), q)]
            total = term if total is None else total + term
        spot = lane_of((ez, LANES))
        for g in range(1, ng, 2):
            one, two = near(g), near((g + 1) % ng)
            line = jnp.concatenate([roll(one, -88) + two, roll(one, -120) + roll(two, -32)], axis=0)
            line = jnp.where(spot < 8, line, 0.0)
            if h > ez:
                line = jnp.concatenate([line, jnp.zeros((h - ez, LANES), jnp.float32)], axis=0)
            face = across(g) + across((g + 1) % ng) + line
            term = face * face * side_in[pl.ds(h * (g // 2), h)]
            for n in range(0, h, q):
                total = total + term[n : n + q]
        total = jnp.sum(total, axis=0, keepdims=True)
        parts[pl.ds(len(others), 1)] = total
        late_out[...] = total
        for n, shift in enumerate((0, ng - 1, 1)):
            g = lax.rem(me_g + shift, ng)
            prev_v[pl.ds(q * n, q)] = wrap_in[pl.ds(pl.multiple_of(u * g + h * (1 - (g & 1)), q), q)]

    heard = [(g, b) for b in range(nd) for g in range(ng) if (g, b) != (root, 0)]

    @pl.when(is_root)
    def _():
        for target in heard:
            send(late_out, parts.at[pl.ds(len(others), 1)], part_recv, target).start()

    @pl.when(jnp.logical_not(owns_low))
    def _():
        drain(h, last_recv.at[1])
        low_v[...] = i_in(3, 1)[...]

    @pl.when(is_last)
    def _():
        drain(h, last_recv.at[0])
        high_v[...] = i_in(3, 0)[...]

    @pl.when(jnp.logical_not(owns_next))
    def _():
        drain(3 * q, last_recv.at[2])
        hold(next_v, 0)

    @pl.when(jnp.logical_not(is_last | is_root))
    def _():
        drain(3 * q, last_recv.at[3])
        hold(prev_v, 1)

    applied = add_i_face(add_i_face(inside, low_v[...], 0), high_v[...], 1)
    applied = add_j_face(add_j_face(applied, ez, *held(prev_v), 0), ez, *held(next_v), 1)

    drain(len(others), sum_recv)
    everyone = early + jnp.sum(sums[pl.ds(0, len(others))], axis=0, keepdims=True)
    norm_now, curvature, cross = (everyone[:, 32 * n : 32 * n + 1] for n in range(3))
    step = norm_now / curvature
    shrunk = norm_now - 2.0 * step * cross
    scale = step * step
    moved = []
    for b, c in enumerate(cut):
        outs[0, :, c] = pair_v[1, :, c] + step * smooth[b]
        out = residual[b] - step * applied[b]
        outs[1, :, c] = out
        moved.append(out * inverse[b])

    @pl.when(is_root)
    def _():
        drain(len(others), part_recv)

    @pl.when(jnp.logical_not(is_root))
    def _():
        drain(len(others) + 1, part_recv)

    quad = part[pl.ds(1, 1)] + jnp.sum(parts[...], axis=0, keepdims=True)
    quad = jnp.sum(quad, axis=1, keepdims=True)
    ratio = (shrunk + scale * quad) / norm_now
    for b, c in enumerate(cut):
        outs[2, :, c] = moved[b] + ratio * smooth[b]
    common = 4 * span + 2 * len(others)
    roles = [
        (is_root, len(heard)),
        (is_first & jnp.logical_not(is_root), 2 * q),
        (is_near, q),
        (jnp.logical_not(is_first | is_last | is_near), 0),
    ]
    skipped = sum(jnp.where(wrap_target(a) == root, 1, 0) for a in (-1, 0, 1))
    for n in range(4):
        roles.append((is_last & odd & (skipped == n), u + h - n * q))
        roles.append((is_last & jnp.logical_not(odd) & (skipped == n), u - n * q))

    for role, extra in roles:

        @pl.when(role)
        def _():
            drain(common + extra, send_sem)


def deliver(stacked, *refs):
    for n in range(3):
        pltpu.make_async_copy(stacked.at[n], refs[n], refs[3]).start()
    pltpu.make_async_copy(stacked, stacked, refs[3]).wait()


def on_device(solution, residual, direction, geometry, mass):
    dims = solution.shape
    ng, nd = lax.axis_size("group"), lax.axis_size("dev")
    ez, points = dims[2], dims[3]
    rows = dims[0] * dims[1] * ez
    flat = (rows, points)
    f32, bf16 = jnp.float32, jnp.bfloat16
    table = jnp.asarray(tables())
    h, q = rows // 2, ez // 2
    u, q8 = h + q, 8
    spare = 4 * (2 * h + 6 * q) + 2 * ng * nd + 3 * ng * (u + h)
    bulk = (2 * rows * points * 4 + 4 * rows * points * 2 + table.size * 2) // (4 * LANES)
    spare = -(-spare // q8) * q8
    stacked = pl.pallas_call(
        functools.partial(kernel, ng, nd, ez),
        out_shape=pltpu.VMEM((3,) + flat, f32),
        in_specs=[pl.BlockSpec(memory_space=pltpu.HBM)] * 6,
        out_specs=pl.BlockSpec(memory_space=pltpu.VMEM),
        scratch_shapes=[
            pltpu.VMEM((2,) + flat, f32),
            pltpu.VMEM(flat, f32),
            pltpu.VMEM((4,) + flat, bf16),
            pltpu.VMEM(table.shape, bf16),
            pltpu.VMEM((3,) + flat, f32),
            pltpu.VMEM((4, 2 * u, LANES), f32),
            pltpu.VMEM((spare, LANES), f32),
            pltpu.VMEM((ng * u, LANES), f32),
            pltpu.VMEM((3 * ng * q, LANES), f32),
            pltpu.VMEM((ng // 2 * h, LANES), f32),
            pltpu.VMEM((h, LANES), f32),
            pltpu.VMEM((3 * q, LANES), f32),
            pltpu.VMEM((3 * q, LANES), f32),
            pltpu.VMEM((h, LANES), f32),
            pltpu.VMEM((h, LANES), f32),
            pltpu.VMEM((2, LANES), f32),
            pltpu.VMEM((ng * nd, LANES), f32),
            pltpu.VMEM((ng * nd, LANES), f32),
            pltpu.VMEM((1, LANES), f32),
            pltpu.VMEM((bulk, LANES), f32),
            pltpu.SemaphoreType.DMA((2,)),
            pltpu.SemaphoreType.DMA,
            pltpu.SemaphoreType.DMA,
            pltpu.SemaphoreType.DMA((2,)),
            pltpu.SemaphoreType.DMA((4,)),
            pltpu.SemaphoreType.DMA,
            pltpu.SemaphoreType.DMA,
            pltpu.SemaphoreType.DMA,
            pltpu.SemaphoreType.REGULAR,
        ],
        compiler_params=pltpu.CompilerParams(collective_id=0, has_side_effects=True, vmem_limit_bytes=8 << 20),
    )(
        pltpu.with_memory_space_constraint(solution.reshape(flat), pltpu.HBM),
        pltpu.with_memory_space_constraint(residual.reshape(flat), pltpu.HBM),
        pltpu.with_memory_space_constraint(direction.reshape(flat), pltpu.HBM),
        pltpu.with_memory_space_constraint(geometry.reshape((3,) + flat), pltpu.HBM),
        pltpu.with_memory_space_constraint(mass.reshape(flat), pltpu.HBM),
        pltpu.with_memory_space_constraint(table, pltpu.HBM),
    )
    outs = pl.pallas_call(
        deliver,
        out_shape=[jax.ShapeDtypeStruct(flat, f32)] * 3,
        in_specs=[pl.BlockSpec(memory_space=pl.ANY)],
        out_specs=[pl.BlockSpec(memory_space=pltpu.HBM)] * 3,
        scratch_shapes=[pltpu.SemaphoreType.DMA],
        compiler_params=pltpu.CompilerParams(vmem_limit_bytes=8 << 20),
    )(stacked)
    return tuple(x.reshape(dims) for x in outs)


def solution(mesh):
    spec = P("group", "dev", None, None)
    return jax.shard_map(
        on_device,
        mesh=mesh,
        in_specs=(spec, spec, spec, P(None, "group", "dev", None, None), spec),
        out_specs=(spec, spec, spec),
        check_vma=False,
    )
```

```python
import functools

import jax
import jax.numpy as jnp
import numpy as np
from jax import lax
from jax.experimental import pallas as pl
from jax.experimental.pallas import tpu as pltpu
from jax.sharding import PartitionSpec as P

NP = 8
LANES = 128
MESH = pl.DeviceIdType.MESH

lobatto_nodes = [
    -1.0,
    -0.8717401485096066,
    -0.5917001814331423,
    -0.2092992179024789,
    0.2092992179024789,
    0.5917001814331423,
    0.8717401485096066,
    1.0,
]


def derivative_table():
    nodes = np.array(lobatto_nodes)
    identity = np.eye(NP)
    offset = nodes[:, None] - nodes[None, :] + identity
    barycentric = 1.0 / np.prod(offset, axis=1)
    derivative = barycentric[None, :] / barycentric[:, None] / offset * (1.0 - identity)
    return derivative - identity * np.sum(derivative, axis=1)[:, None]


def split_table(table):
    table = np.asarray(table, np.float32)
    high = table.astype(jnp.bfloat16)
    low = (table - high.astype(np.float32)).astype(jnp.bfloat16)
    return high, low


def tables():
    d = derivative_table().astype(np.float32)
    along_j = np.kron(np.kron(np.eye(2), d), np.eye(NP))
    along_k = np.kron(np.eye(16), d)
    high, low = split_table(np.concatenate([along_j.T, along_k.T], axis=1))
    forward = np.concatenate([np.concatenate([high, high], 0), np.concatenate([low, low], 0)], 1)
    high, low = split_table(np.concatenate([along_j, along_k], axis=0))
    backward = np.concatenate([high, low], axis=1)
    high, low = split_table(np.concatenate([along_j * along_j, along_k * along_k], axis=0))
    squares = np.concatenate([high, low], axis=1)
    return np.concatenate([forward, backward, squares], axis=1)


def roll(x, shift):
    shift %= LANES
    return x if shift == 0 else pltpu.roll(x, shift, 1)


def lane_of(shape):
    return lax.broadcasted_iota(jnp.int32, shape, 1)


def along_i(table, blocks):
    low = lane_of(blocks[0].shape) < 64
    swapped = [roll(x, 64) for x in blocks]
    outs = []
    for b in range(4):
        total = None
        for c in range(4):
            same = jnp.where(low, float(table[2 * b, 2 * c]), float(table[2 * b + 1, 2 * c + 1]))
            other = jnp.where(low, float(table[2 * b, 2 * c + 1]), float(table[2 * b + 1, 2 * c]))
            term = same * blocks[c] + other * swapped[c]
            total = term if total is None else total + term
        outs.append(total)
    return outs


def weights_of(rows):
    lane = lane_of((rows, LANES))
    k, j = lane & 7, (lane >> 3) & 7
    half = lambda cond: jnp.where(cond, 0.5, 1.0)
    base = half((k == 0) | (k == 7)) * half((j == 0) | (j == 7))
    return [base * half(lane < 64), base, base, base * half(lane >= 64)]


def pack_i_face(x, side):
    h = x.shape[0] // 2
    top, bottom = x[:h], x[h:]
    low = lane_of(top.shape) < 64
    if side == 0:
        return jnp.where(low, top, roll(bottom, 64))
    return jnp.where(low, roll(top, 64), bottom)


def unpack_i_face(m, side):
    other = roll(m, 64)
    return jnp.concatenate([m, other] if side == 0 else [other, m], axis=0)


def pack_j_face(blocks, ez, side):
    half = ez // 2
    lane = lane_of((half, LANES))
    slot = (lane & 63) >> 3
    out = jnp.zeros((half, LANES), jnp.float32)
    for b in range(4):
        rows = blocks[b][:ez] if side == 0 else blocks[b][-ez:]
        for n in range(2):
            moved = roll(rows[n * half : (n + 1) * half], 8 * b + 32 * n - (0 if side == 0 else 56))
            out = jnp.where(slot == b + 4 * n, moved, out)
    return out


def assemble_inside(blocks, ez):
    rows = blocks[0].shape[0]
    lane = lane_of((rows, LANES))
    j, k = (lane >> 3) & 7, lane & 7
    outs = []
    for x in blocks:
        if rows > ez:
            edge = jnp.zeros((ez, LANES), jnp.float32)
            after = jnp.concatenate([roll(x[ez:], 56), edge], axis=0)
            before = jnp.concatenate([edge, roll(x[:-ez], -56)], axis=0)
            x = x + jnp.where(j == 7, after, jnp.where(j == 0, before, 0.0))
        up, down = roll(x, 7), roll(x, -7)
        after = [pltpu.roll(up[e : e + ez], ez - 1, 0) for e in range(0, rows, ez)]
        before = [pltpu.roll(down[e : e + ez], 1, 0) for e in range(0, rows, ez)]
        after, before = jnp.concatenate(after, 0), jnp.concatenate(before, 0)
        outs.append(x + jnp.where(k == 7, after, jnp.where(k == 0, before, 0.0)))
    return outs


def turn_column(x, ez, shift):
    parts = [pltpu.roll(x[e : e + ez], shift % ez, 0) for e in range(0, x.shape[0], ez)]
    return parts[0] if len(parts) == 1 else jnp.concatenate(parts, axis=0)


def summed_j_face(blocks, ez, side):
    half = ez // 2
    lane = lane_of((half, LANES))
    slot, k = (lane & 63) >> 3, lane & 7
    kept = [jnp.zeros((half, LANES), jnp.float32)] * 3
    for b in range(4):
        column = blocks[b][:ez] if side == 0 else blocks[b][-ez:]
        kinds = ((column, 0), (turn_column(column, ez, -1), 7), (turn_column(column, ez, 1), -7))
        for n in range(2):
            shift = 8 * b + 32 * n - 56 * side
            for m, (rows, extra) in enumerate(kinds):
                moved = roll(rows[n * half : (n + 1) * half], shift + extra)
                kept[m] = jnp.where(slot == b + 4 * n, moved, kept[m])
    return kept[0] + jnp.where(k == 7, kept[1], jnp.where(k == 0, kept[2], 0.0))


def summed_i_face(x, ez, side):
    rows = x.shape[0]
    h = rows // 2
    lane = lane_of((h, LANES))
    j, k = (lane >> 3) & 7, lane & 7
    edge = jnp.zeros((ez, LANES), jnp.float32)

    def gather(bottom):
        cut = slice(h, rows) if bottom else slice(0, h)
        base = 64 if bottom != (side == 1) else 0
        total = None
        for column, shift, where in ((0, 0, None), (1, 56, j == 7), (-1, -56, j == 0)):
            if column and (rows == ez or (rows == 2 * ez and bottom == (column == 1))):
                continue
            found = None
            for turn, extra, only in ((0, 0, None), (-1, 7, k == 7), (1, -7, k == 0)):
                y = turn_column(x, ez, turn) if turn else x
                if column == 1:
                    y = jnp.concatenate([y[ez:], edge], axis=0)
                elif column == -1:
                    y = jnp.concatenate([edge, y[:-ez]], axis=0)
                y = roll(y[cut], base + shift + extra)
                y = y if only is None else jnp.where(only, y, 0.0)
                found = y if found is None else found + y
            found = found if where is None else jnp.where(where, found, 0.0)
            total = found if total is None else total + found
        return total

    return jnp.where(lane < 64, gather(False), gather(True))


def add_i_face(blocks, message, side):
    blocks = list(blocks)
    low = lane_of(blocks[0].shape) < 64
    face = unpack_i_face(message, side)
    blocks[3 * side] = blocks[3 * side] + jnp.where(low if side == 0 else ~low, face, 0.0)
    return blocks


def add_j_face(blocks, ez, same, before, after, side):
    lane = lane_of((ez, LANES))
    here = ((lane >> 3) & 7) == 7 * side

    def spread(message, shift):
        return jnp.concatenate([roll(message, shift), roll(message, shift - 32)], axis=0)

    outs = []
    for b, x in enumerate(blocks):
        shift = 56 * side - 8 * b
        face = jnp.where(here, spread(same, shift), 0.0)
        if b == 0:
            face = face + jnp.where(here & (lane < 64), spread(before, shift + 40), 0.0)
        if b == 3:
            face = face + jnp.where(here & (lane >= 64), spread(after, shift + 88), 0.0)
        if x.shape[0] == ez:
            outs.append(x + face)
        elif side == 0:
            outs.append(jnp.concatenate([x[:ez] + face, x[ez:]], axis=0))
        else:
            outs.append(jnp.concatenate([x[:-ez], x[-ez:] + face], axis=0))
    return outs


def halves(x):
    high = x.astype(jnp.bfloat16)
    return high, (x - high.astype(jnp.float32)).astype(jnp.bfloat16)


def dot(left, right):
    return jnp.dot(left, right, preferred_element_type=jnp.float32)


def stack(blocks):
    return jnp.concatenate(blocks, axis=0)


def total_of(blocks):
    x = blocks[0] + blocks[1] + (blocks[2] + blocks[3])
    return jnp.sum(jnp.sum(x, axis=0, keepdims=True), axis=1, keepdims=True)


def owner_weights(rows, ez, first_owned, last_owned, high_owned):
    lane = lane_of((rows, LANES))
    row = lax.broadcasted_iota(jnp.int32, (rows, LANES), 0)
    k, j = lane & 7, (lane >> 3) & 7
    base = jnp.where((k == 0) | (k == 7), 0.5, 1.0)
    first = jnp.where(row < ez, jnp.where(first_owned, 1.0, 0.0), 0.5)
    last = jnp.where(row >= rows - ez, jnp.where(last_owned, 1.0, 0.0), 0.5)
    base = base * jnp.where(j == 0, first, jnp.where(j == 7, last, 1.0))
    high = jnp.where(high_owned, 1.0, 0.0)
    outer = [jnp.where(lane < 64, 0.0, base), base, base, jnp.where(lane < 64, base, high * base)]
    return outer, base


def kernel(
    ng, nd, ez,
    sol_h, res_h, dir_h, geo_h, mass_h, tab_h,
    outs,
    pair_v, dir_v, geo_v, tab_v, early_v,
    face_out, face_in, wrap_in, root_in, relay_in, side_in, side_out, prev_v, next_v, low_v, high_v, part, sums, parts, late_out,
    bulk, load_sem, send_sem, recv_sem, side_recv, last_recv, root_recv, relay_recv, sum_recv, part_recv, go,
):
    me_g, me_d = lax.axis_index("group"), lax.axis_index("dev")

    def at(a, b):
        return (lax.rem(me_g + (a + ng), ng), lax.rem(me_d + (b + nd), nd))

    others = [(a, b) for a in range(ng) for b in range(nd) if (a, b) != (0, 0)]
    others.sort(key=lambda t: (min(t[1], nd - t[1]) != 1, min(t[0], ng - t[0]) > 1))

    pairs = (
        (dir_h, dir_v, 0), (geo_h, geo_v.at[pl.ds(0, 3)], 1), (mass_h, geo_v.at[3], 1),
        (tab_h, tab_v, 1), (res_h, pair_v.at[0], 1), (sol_h, pair_v.at[1], 1),
    )
    loads = [pltpu.make_async_copy(h, v, load_sem.at[n]) for h, v, n in pairs]
    loads[0].start()
    barrier = pltpu.get_barrier_semaphore()
    is_first, is_last, is_near = me_d == 0, me_d == nd - 1, me_d == nd - 2
    odd = (me_g & 1) == 1
    is_relay = (me_d == nd - 3) & odd
    own_relay = (me_g | 1, nd - 3)
    partners = [t for t in others if min(t[0], ng - t[0]) < 2 and min(t[1], nd - t[1]) < 2]
    hub = (1 % ng, nd // 2)
    hub_a, hub_b = lax.rem(me_g - hub[0] + ng, ng), lax.rem(me_d - hub[1] + nd, nd)
    at_hub = (hub_a == 0) & (hub_b == 0)
    near_hub = ((hub_a < 2) | (hub_a == ng - 1)) & ((hub_b < 2) | (hub_b == nd - 1))
    @pl.when(is_last)
    def _():
        beside = lax.rem(jnp.where(odd, me_g + 2, me_g + (ng - 1)), ng)
        for target in ((beside, nd - 3), own_relay):
            pl.semaphore_signal(barrier, inc=1, device_id=target, device_id_type=MESH)

    @pl.when(is_relay)
    def _():
        for target in ((me_g, 0), (me_g - 1, 0)):
            pl.semaphore_signal(barrier, inc=1, device_id=target, device_id_type=MESH)

    for a, b in partners:
        if b == 1:

            @pl.when(jnp.logical_not(is_last))
            def _():
                pl.semaphore_signal(barrier, inc=1, device_id=at(a, b), device_id_type=MESH)

        else:
            pl.semaphore_signal(barrier, inc=1, device_id=at(a, b), device_id_type=MESH)

    @pl.when(jnp.logical_not(near_hub))
    def _():
        pl.semaphore_signal(barrier, inc=1, device_id=hub, device_id_type=MESH)

    for load in loads[1:]:
        load.start()

    rows = dir_v.shape[0]
    h, q = rows // 2, ez // 2
    u, span = h + q, 2 * h + 6 * q
    root = min(1, ng - 1)
    is_root = is_first & (me_g == root)
    owns_next = me_d < nd - 3
    owns_high, owns_low = jnp.logical_not(is_last), is_last & odd

    def i_out(phase, side):
        return face_out.at[phase, pl.ds(u * side, h)]

    def i_in(phase, side):
        return face_in.at[pl.ds(span * phase + h * side, h)]

    def j_out(phase, side):
        return face_out.at[phase, pl.ds(2 * h + q if side == 0 else h, q)]

    def j_in(phase, side, turn):
        return face_in.at[pl.ds(span * phase + 2 * h + q * (3 * side + turn), q)]

    def slot(ref, part_of, group):
        return ref.at[pl.ds(pl.multiple_of(q * (ng * part_of + group), q), q)]

    def drain(count, sem):
        ref = face_in.at[pl.ds(0, count)]
        pltpu.make_async_copy(ref, ref, sem).wait()

    def send(src, dst, recv_to, target):
        return pltpu.make_async_remote_copy(
            src_ref=src, dst_ref=dst, send_sem=send_sem, recv_sem=recv_to,
            device_id=target, device_id_type=MESH,
        )

    weights = weights_of(rows)
    cut = [slice(LANES * b, LANES * b + LANES) for b in range(4)]

    def pack(phase, blocks):
        for side in range(2):
            j_out(phase, side)[...] = pack_j_face(blocks, ez, side)
            i_out(phase, side)[...] = pack_i_face(blocks[3 * side], side)

    def give_j(phase, side, step, sem):
        for turn, a in ((2, 1), (0, -1), (1, 0)):
            send(j_out(phase, side), j_in(phase, side, turn), sem, at(a, step)).start()

    def give_i(phase, sems):
        for side, step in ((0, -1), (1, 1)):
            send(i_out(phase, side), i_in(phase, side), sems[side], at(step, 0)).start()

    def give_rest(phase, sems):
        give_j(phase, 1, 1, sems[2])
        give_i(phase, sems[:2])

    def give_relay(phase, sem):
        dst = relay_in.at[pl.ds(pl.multiple_of(q * (2 * phase + (me_g & 1)), q), q)]
        send(j_out(phase, 0), dst, sem, own_relay).start()

    def turns(phase, side):
        return [j_in(phase, side, turn)[...] for turn in (1, 2, 0)]

    def assembled(phase, blocks):
        blocks = add_i_face(add_i_face(blocks, i_in(phase, 1)[...], 0), i_in(phase, 0)[...], 1)
        return add_j_face(add_j_face(blocks, ez, *turns(phase, 1), 0), ez, *turns(phase, 0), 1)

    d = derivative_table().astype(np.float32)
    loads[0].wait()
    weighted = assemble_inside([weights[b] * dir_v[:, cut[b]] for b in range(4)], ez)
    pack(0, weighted)
    count = jnp.where(at_hub, len(others), len(partners))
    count = jnp.where(is_relay, len(partners) + 4, count)

    @pl.when(jnp.logical_not(is_first))
    def _():
        pl.semaphore_wait(barrier, count)
        give_j(0, 0, -1, recv_sem)
        give_rest(0, [recv_sem] * 3)

    @pl.when(at_hub)
    def _():
        for a, b in others:
            pl.semaphore_signal(go, inc=1, device_id=at(a, b), device_id_type=MESH)

    pltpu.make_async_copy(bulk, bulk, load_sem.at[1]).wait()
    geo_rows = stack([jnp.concatenate([geo_v[1, :, c], geo_v[2, :, c]], axis=1) for c in cut])
    squared = dot(geo_rows, tab_v[:, 768:1024])
    squared = squared[:, :LANES] + squared[:, LANES:]
    geo = [[geo_v[c, :, cut[b]].astype(jnp.float32) for b in range(4)] for c in range(3)]
    mass = [geo_v[3, :, c].astype(jnp.float32) for c in cut]
    diag = along_i((d * d).T, geo[0])
    diag = [diag[b] + squared[rows * b : rows * b + rows] + mass[b] for b in range(4)]
    diag = assemble_inside(diag, ez)
    pack(1, diag)
    residual = [pair_v[0, :, c] for c in cut]
    spread_res = [weights[b] * residual[b] for b in range(4)]
    mixed = assemble_inside(spread_res, ez)
    pack(2, mixed)

    @pl.when(is_first)
    def _():
        pl.semaphore_wait(barrier, len(partners) - 2)
        give_relay(0, relay_recv.at[me_g & 1])
        give_relay(1, relay_recv.at[2])
        give_relay(2, relay_recv.at[2])
        give_rest(0, [recv_sem] * 3)

    @pl.when(jnp.logical_not(is_first))
    def _():
        give_j(1, 0, -1, side_recv.at[1])
        give_j(2, 0, -1, side_recv.at[1])

    give_rest(1, [side_recv.at[0]] * 3)
    give_rest(2, [side_recv.at[0]] * 3)
    owned, face_owned = owner_weights(rows, ez, False, owns_next, owns_high)

    def pass_on(phase, core, sem):
        for turn, a in ((2, 1), (0, -1), (1, 0)):
            target = lax.rem(me_g + (core - 1 + a + ng), ng)
            src = relay_in.at[pl.ds(q * (2 * phase + core), q)]
            send(src, j_in(phase, 0, turn), sem, (target, nd - 1)).start()

    @pl.when(is_relay)
    def _():
        for core in (1, 0):
            drain(q, relay_recv.at[core])
            pass_on(0, core, recv_sem)
        drain(4 * q, relay_recv.at[2])
        for phase in (1, 2):
            for core in (1, 0):
                pass_on(phase, core, side_recv.at[1])

    @pl.when(jnp.logical_not(at_hub))
    def _():
        pl.semaphore_wait(go, 1)

    def nearly(phase, blocks):
        blocks = add_i_face(add_i_face(blocks, i_in(phase, 1)[...], 0), i_in(phase, 0)[...], 1)
        return add_j_face(blocks, ez, *turns(phase, 1), 0)

    def gather_sides():
        drain(2 * (2 * h + 3 * q), side_recv.at[0])
        for b, x in enumerate(nearly(1, [early_v[0, :, c] for c in cut])):
            early_v[0, :, cut[b]] = x
            early_v[2, :, cut[b]] = 1.0 / x
        for b, x in enumerate(nearly(2, [early_v[1, :, c] for c in cut])):
            early_v[1, :, cut[b]] = x

    for b, c in enumerate(cut):
        early_v[0, :, c] = diag[b]
        early_v[1, :, c] = mixed[b]

    @pl.when(is_last)
    def _():
        gather_sides()

    @pl.when(is_last & odd)
    def _():
        lane = lane_of((h, LANES))
        row = lax.broadcasted_iota(jnp.int32, (h, LANES), 0) + jnp.where(lane < 64, 0, h)
        j, k = (lane >> 3) & 7, lane & 7
        fit = jnp.where(j == 0, jnp.where(row < ez, 0.0, 0.5), 1.0)
        fit = jnp.where(j == 7, jnp.where(row < rows - ez, 0.5, 0.0), fit)
        fit = fit * jnp.where((k == 0) | (k == 7), 0.5, 1.0)
        side_out[...] = fit * pack_i_face(early_v[2, :, cut[3]], 1)
        dst = side_in.at[pl.ds(pl.multiple_of((me_g >> 1) * h, q), h)]
        send(side_out, dst, root_recv, (root, 0)).start()

    drain(span, recv_sem)
    smooth = assembled(0, weighted)

    high, low = halves(stack(smooth))
    grads = dot(jnp.concatenate([high, low], axis=1), tab_v[:, :512])
    grads = grads[:, :256] + grads[:, 256:]
    grad_i = along_i(d, smooth)
    flux_i = [geo[0][b] * grad_i[b] for b in range(4)]
    flux = jnp.concatenate(
        [stack(geo[1]) * grads[:, :LANES], stack(geo[2]) * grads[:, LANES:]], axis=1
    )
    high, low = halves(flux)
    back = dot(jnp.concatenate([high, low], axis=0), tab_v[:, 512:768])
    back = back[: 4 * rows] + back[4 * rows :]
    back = back[:, :LANES] + back[:, LANES:]
    local = along_i(d.T, flux_i)
    local = [local[b] + back[rows * b : rows * b + rows] + mass[b] * smooth[b] for b in range(4)]

    for side in range(2):
        j_out(3, side)[...] = summed_j_face(local, ez, side)
        i_out(3, side)[...] = summed_i_face(local[3 * side], ez, side)

    @pl.when(is_last)
    def _():
        start = pl.multiple_of((me_g & 1) * h, q)
        dst = wrap_in.at[pl.ds(pl.multiple_of(me_g * u, q), u)]
        send(face_out.at[3, pl.ds(start, u)], dst, root_recv, (root, 0)).start()

    def wrap_target(a):
        return lax.rem(me_g + (a + ng), ng)

    def give_wrap(first):
        for turn, a in ((2, 1), (0, -1), (1, 0)):
            target = wrap_target(a)
            wanted = target == 0 if first else (target != 0) & (target != root)

            @pl.when(is_last & wanted)
            def _():
                send(j_out(3, 1), j_in(3, 1, turn), last_recv.at[3], (target, 0)).start()

    @pl.when(is_last)
    def _():
        send(j_out(3, 0), slot(root_in, 5, me_g), root_recv, (root, 0)).start()

    give_wrap(True)

    @pl.when(is_near)
    def _():
        send(j_out(3, 1), slot(root_in, 2, me_g), root_recv, (root, 0)).start()
        send(j_out(3, 0), slot(root_in, 3, me_g), root_recv, (root, 0)).start()

    @pl.when(me_d == nd - 3)
    def _():
        send(j_out(3, 1), slot(root_in, 4, me_g), root_recv, (root, 0)).start()

    give_i(3, [last_recv.at[0], last_recv.at[1]])
    give_j(3, 0, -1, last_recv.at[2])

    @pl.when(jnp.logical_not(is_last))
    def _():
        give_j(3, 1, 1, last_recv.at[3])

    @pl.when(is_first & (me_g != root))
    def _():
        send(j_out(3, 0), slot(root_in, 0, me_g), root_recv, (root, 0)).start()

    inside = assemble_inside(local, ez)

    @pl.when(jnp.logical_not(is_last))
    def _():
        gather_sides()

    drain(6 * q, side_recv.at[1])
    inverse = add_j_face([early_v[0, rows - ez :, c] for c in cut], ez, *turns(1, 0), 1)
    inverse = [1.0 / x for x in inverse]
    if rows > ez:
        kept = slice(0, rows - ez)
        inverse = [jnp.concatenate([early_v[2, kept, cut[b]], inverse[b]], axis=0) for b in range(4)]
    mixed = [early_v[1, :, c] for c in cut]

    def shared(side):
        lane = lane_of((q, LANES))
        ends = ((lane & 7) == 0) | ((lane & 7) == 7)
        share = jnp.where((lane < 64) & ((lane & 31) < 8), 0.0, jnp.where(ends, 0.5, 1.0))
        return share * pack_j_face(inverse, ez, side)

    @pl.when(is_first | is_near)
    def _():
        side_out[pl.ds(0, q)] = shared(0)

    @pl.when(is_first & (me_g != root))
    def _():
        send(side_out.at[pl.ds(0, q)], slot(root_in, 1, me_g), root_recv, (root, 0)).start()

    @pl.when(is_near)
    def _():
        side_out[pl.ds(q, q)] = shared(1)
        dst = root_in.at[pl.ds(pl.multiple_of(q * (6 * ng + 2 * me_g), q), 2 * q)]
        send(side_out.at[pl.ds(0, 2 * q)], dst, root_recv, (root, 0)).start()

    dual = add_j_face(mixed, ez, *turns(2, 0), 1)
    norm_now = total_of([spread_res[b] * residual[b] * inverse[b] for b in range(4)])
    curvature = total_of([smooth[b] * local[b] for b in range(4)])
    cross = total_of([local[b] * dual[b] * inverse[b] for b in range(4)])
    share = [owned[b] * inverse[b] for b in range(4)]
    order = sorted(range(len(others)), key=lambda n: (others[n][1] != 1, others[n][1] != 0))

    def tell(row, table, sem, which=None):
        for n in order:
            a, b = others[n]
            if which is not None and which != (b == 1):
                continue
            send(part.at[pl.ds(row, 1)], table.at[pl.ds(n, 1)], sem, at(a, b)).start()

    lane = lane_of((1, LANES))
    early = jnp.where(lane < 32, norm_now, jnp.where(lane < 64, curvature, cross))
    part[pl.ds(0, 1)] = early

    @pl.when(jnp.logical_not(is_last))
    def _():
        tell(0, sums, sum_recv)

    @pl.when(is_last)
    def _():
        tell(0, sums, sum_recv, True)


    def hold(ref, side):
        for n, value in enumerate(turns(3, side)):
            ref[pl.ds(q * n, q)] = value

    def held(ref):
        return [ref[pl.ds(q * n, q)] for n in range(3)]

    @pl.when(owns_high)
    def _():
        drain(h, last_recv.at[0])
        high_v[...] = i_in(3, 0)[...]

    @pl.when(is_last)
    def _():
        high_v[...] = jnp.zeros_like(high_v)

    @pl.when(owns_next)
    def _():
        drain(3 * q, last_recv.at[2])
        hold(next_v, 0)

    @pl.when(jnp.logical_not(owns_next))
    def _():
        next_v[...] = jnp.zeros_like(next_v)

    mostly = add_i_face(inside, high_v[...], 1)
    mostly = add_j_face(mostly, ez, *held(next_v), 1)
    quad = stack([share[b] * mostly[b] * mostly[b] for b in range(4)])
    quad = jnp.sum(quad, axis=0, keepdims=True)
    part[pl.ds(1, 1)] = quad

    @pl.when(owns_low)
    def _():
        face = pack_i_face(mostly[0], 0)
        fit = pack_i_face(face_owned * inverse[0], 0)
        drain(h, last_recv.at[1])
        met = i_in(3, 1)[...]
        low_v[...] = met
        face = face + met
        part[pl.ds(1, 1)] = quad + jnp.sum(face * face * fit, axis=0, keepdims=True)

    @pl.when(jnp.logical_not(is_last))
    def _():
        tell(1, parts, part_recv)

    @pl.when(is_last)
    def _():
        tell(1, parts, part_recv)
        tell(0, sums, sum_recv, False)

    give_wrap(False)

    @pl.when(is_root)
    def _():
        slot(root_in, 0, me_g)[...] = j_out(3, 0)[...]
        slot(root_in, 1, me_g)[...] = side_out[pl.ds(0, q)]
        drain((8 * ng - 2) * q + ng // 2 * h + ng * u, root_recv)

        def far(g):
            return wrap_in[pl.ds(u * g + (0 if g & 1 else h), q)]

        def across(g):
            return wrap_in[pl.ds(u * g + (q if g & 1 else 0), h)]

        def got(part_of, g):
            return root_in[pl.ds(q * (ng * part_of + g), q)]

        def paired(g, n):
            return root_in[pl.ds(q * (6 * ng + 2 * g + n), q)]

        spot = lane_of((q, LANES))
        seam = (spot >= 64) & ((spot & 31) >= 24)
        total = None
        groups = range(ng)
        seams = (
            ([got(3, g) + got(4, g) for g in groups], [paired(g, 0) for g in groups]),
            ([got(2, g) + got(5, g) for g in groups], [paired(g, 1) for g in groups]),
            ([got(0, g) + far(g) for g in groups], [got(1, g) for g in groups]),
        )
        for faces, fits in seams:
            for g in groups:
                face = faces[g] + jnp.where(seam, roll(faces[(g + 1) % ng], 88), 0.0)
                term = face * face * fits[g]
                total = term if total is None else total + term
        for g in range(1, ng, 2):
            face = across(g) + across((g + 1) % ng)
            term = face * face * side_in[pl.ds(h * (g // 2), h)]
            for n in range(0, h, q):
                total = total + term[n : n + q]
        total = jnp.sum(total, axis=0, keepdims=True)
        parts[pl.ds(len(others), 1)] = total
        late_out[...] = total
        for n, shift in enumerate((0, ng - 1, 1)):
            g = lax.rem(me_g + shift, ng)
            prev_v[pl.ds(q * n, q)] = wrap_in[pl.ds(pl.multiple_of(u * g + h * (1 - (g & 1)), q), q)]

    heard = [(g, b) for b in range(nd) for g in range(ng) if (g, b) != (root, 0)]

    @pl.when(is_root)
    def _():
        for target in heard:
            send(late_out, parts.at[pl.ds(len(others), 1)], part_recv, target).start()

    @pl.when(jnp.logical_not(owns_low))
    def _():
        drain(h, last_recv.at[1])
        low_v[...] = i_in(3, 1)[...]

    @pl.when(is_last)
    def _():
        drain(h, last_recv.at[0])
        high_v[...] = i_in(3, 0)[...]

    @pl.when(jnp.logical_not(owns_next))
    def _():
        drain(3 * q, last_recv.at[2])
        hold(next_v, 0)

    @pl.when(jnp.logical_not(is_root))
    def _():
        drain(3 * q, last_recv.at[3])
        hold(prev_v, 1)

    applied = add_i_face(add_i_face(inside, low_v[...], 0), high_v[...], 1)
    applied = add_j_face(add_j_face(applied, ez, *held(prev_v), 0), ez, *held(next_v), 1)

    drain(len(others), sum_recv)
    everyone = early + jnp.sum(sums[pl.ds(0, len(others))], axis=0, keepdims=True)
    norm_now, curvature, cross = (everyone[:, 32 * n : 32 * n + 1] for n in range(3))
    step = norm_now / curvature
    shrunk = norm_now - 2.0 * step * cross
    scale = step * step
    moved = []
    for b, c in enumerate(cut):
        outs[0, :, c] = pair_v[1, :, c] + step * smooth[b]
        out = residual[b] - step * applied[b]
        outs[1, :, c] = out
        moved.append(out * inverse[b])

    @pl.when(is_root)
    def _():
        drain(len(others), part_recv)

    @pl.when(jnp.logical_not(is_root))
    def _():
        drain(len(others) + 1, part_recv)

    quad = part[pl.ds(1, 1)] + jnp.sum(parts[...], axis=0, keepdims=True)
    quad = jnp.sum(quad, axis=1, keepdims=True)
    ratio = (shrunk + scale * quad) / norm_now
    for b, c in enumerate(cut):
        outs[2, :, c] = moved[b] + ratio * smooth[b]
    common = 4 * span + 2 * len(others)
    roles = [
        (is_root, len(heard) - 6 * q),
        (is_first & jnp.logical_not(is_root), 2 * q - 6 * q),
        (is_near, 4 * q),
        (is_relay, 19 * q),
        ((me_d == nd - 3) & jnp.logical_not(odd), q),
        (me_d * (nd - 4 - me_d) > 0, 0),
        (me_d == nd - 4, 0),
    ]
    skipped = sum(jnp.where(wrap_target(a) == root, 1, 0) for a in (-1, 0, 1))
    for n in range(4):
        roles.append((is_last & odd & (skipped == n), u + h + q - n * q))
        roles.append((is_last & jnp.logical_not(odd) & (skipped == n), u + q - n * q))

    for role, extra in roles:

        @pl.when(role)
        def _():
            drain(common + extra, send_sem)


def deliver(stacked, *refs):
    for n in range(3):
        pltpu.make_async_copy(stacked.at[n], refs[n], refs[3]).start()
    pltpu.make_async_copy(stacked, stacked, refs[3]).wait()


def on_device(solution, residual, direction, geometry, mass):
    dims = solution.shape
    ng, nd = lax.axis_size("group"), lax.axis_size("dev")
    ez, points = dims[2], dims[3]
    rows = dims[0] * dims[1] * ez
    flat = (rows, points)
    f32, bf16 = jnp.float32, jnp.bfloat16
    table = jnp.asarray(tables())
    h, q = rows // 2, ez // 2
    u, q8 = h + q, 8
    spare = 4 * (2 * h + 6 * q) + 3 * ng * nd + 8 * ng * (u + h)
    bulk = (2 * rows * points * 4 + 4 * rows * points * 2 + table.size * 2) // (4 * LANES)
    spare = -(-spare // q8) * q8
    stacked = pl.pallas_call(
        functools.partial(kernel, ng, nd, ez),
        out_shape=pltpu.VMEM((3,) + flat, f32),
        in_specs=[pl.BlockSpec(memory_space=pltpu.HBM)] * 6,
        out_specs=pl.BlockSpec(memory_space=pltpu.VMEM),
        scratch_shapes=[
            pltpu.VMEM((2,) + flat, f32),
            pltpu.VMEM(flat, f32),
            pltpu.VMEM((4,) + flat, bf16),
            pltpu.VMEM(table.shape, bf16),
            pltpu.VMEM((3,) + flat, f32),
            pltpu.VMEM((4, 2 * u, LANES), f32),
            pltpu.VMEM((spare, LANES), f32),
            pltpu.VMEM((ng * u, LANES), f32),
            pltpu.VMEM((8 * ng * q, LANES), f32),
            pltpu.VMEM((6 * q, LANES), f32),
            pltpu.VMEM((ng // 2 * h, LANES), f32),
            pltpu.VMEM((h, LANES), f32),
            pltpu.VMEM((3 * q, LANES), f32),
            pltpu.VMEM((3 * q, LANES), f32),
            pltpu.VMEM((h, LANES), f32),
            pltpu.VMEM((h, LANES), f32),
            pltpu.VMEM((2, LANES), f32),
            pltpu.VMEM((ng * nd, LANES), f32),
            pltpu.VMEM((ng * nd, LANES), f32),
            pltpu.VMEM((1, LANES), f32),
            pltpu.VMEM((bulk, LANES), f32),
            pltpu.SemaphoreType.DMA((2,)),
            pltpu.SemaphoreType.DMA,
            pltpu.SemaphoreType.DMA,
            pltpu.SemaphoreType.DMA((2,)),
            pltpu.SemaphoreType.DMA((4,)),
            pltpu.SemaphoreType.DMA,
            pltpu.SemaphoreType.DMA((3,)),
            pltpu.SemaphoreType.DMA,
            pltpu.SemaphoreType.DMA,
            pltpu.SemaphoreType.REGULAR,
        ],
        compiler_params=pltpu.CompilerParams(collective_id=0, has_side_effects=True, vmem_limit_bytes=8 << 20),
    )(
        pltpu.with_memory_space_constraint(solution.reshape(flat), pltpu.HBM),
        pltpu.with_memory_space_constraint(residual.reshape(flat), pltpu.HBM),
        pltpu.with_memory_space_constraint(direction.reshape(flat), pltpu.HBM),
        pltpu.with_memory_space_constraint(geometry.reshape((3,) + flat), pltpu.HBM),
        pltpu.with_memory_space_constraint(mass.reshape(flat), pltpu.HBM),
        pltpu.with_memory_space_constraint(table, pltpu.HBM),
    )
    outs = pl.pallas_call(
        deliver,
        out_shape=[jax.ShapeDtypeStruct(flat, f32)] * 3,
        in_specs=[pl.BlockSpec(memory_space=pl.ANY)],
        out_specs=[pl.BlockSpec(memory_space=pltpu.HBM)] * 3,
        scratch_shapes=[pltpu.SemaphoreType.DMA],
        compiler_params=pltpu.CompilerParams(vmem_limit_bytes=8 << 20),
    )(stacked)
    return tuple(x.reshape(dims) for x in outs)


def solution(mesh):
    spec = P("group", "dev", None, None)
    return jax.shard_map(
        on_device,
        mesh=mesh,
        in_specs=(spec, spec, spec, P(None, "group", "dev", None, None), spec),
        out_specs=(spec, spec, spec),
        check_vma=False,
    )
```

```python
import functools

import jax
import jax.numpy as jnp
import numpy as np
from jax import lax
from jax.experimental import pallas as pl
from jax.experimental.pallas import tpu as pltpu
from jax.sharding import PartitionSpec as P

NP = 8
LANES = 128
MESH = pl.DeviceIdType.MESH

lobatto_nodes = [
    -1.0,
    -0.8717401485096066,
    -0.5917001814331423,
    -0.2092992179024789,
    0.2092992179024789,
    0.5917001814331423,
    0.8717401485096066,
    1.0,
]


def derivative_table():
    nodes = np.array(lobatto_nodes)
    identity = np.eye(NP)
    offset = nodes[:, None] - nodes[None, :] + identity
    barycentric = 1.0 / np.prod(offset, axis=1)
    derivative = barycentric[None, :] / barycentric[:, None] / offset * (1.0 - identity)
    return derivative - identity * np.sum(derivative, axis=1)[:, None]


def split_table(table):
    table = np.asarray(table, np.float32)
    high = table.astype(jnp.bfloat16)
    low = (table - high.astype(np.float32)).astype(jnp.bfloat16)
    return high, low


def tables():
    d = derivative_table().astype(np.float32)
    along_j = np.kron(np.kron(np.eye(2), d), np.eye(NP))
    along_k = np.kron(np.eye(16), d)
    high, low = split_table(np.concatenate([along_j.T, along_k.T], axis=1))
    forward = np.concatenate([np.concatenate([high, high], 0), np.concatenate([low, low], 0)], 1)
    high, low = split_table(np.concatenate([along_j, along_k], axis=0))
    backward = np.concatenate([high, low], axis=1)
    high, low = split_table(np.concatenate([along_j * along_j, along_k * along_k], axis=0))
    squares = np.concatenate([high, low], axis=1)
    return np.concatenate([forward, backward, squares], axis=1)


def roll(x, shift):
    shift %= LANES
    return x if shift == 0 else pltpu.roll(x, shift, 1)


def lane_of(shape):
    return lax.broadcasted_iota(jnp.int32, shape, 1)


def along_i(table, blocks):
    low = lane_of(blocks[0].shape) < 64
    swapped = [roll(x, 64) for x in blocks]
    outs = []
    for b in range(4):
        total = None
        for c in range(4):
            same = jnp.where(low, float(table[2 * b, 2 * c]), float(table[2 * b + 1, 2 * c + 1]))
            other = jnp.where(low, float(table[2 * b, 2 * c + 1]), float(table[2 * b + 1, 2 * c]))
            term = same * blocks[c] + other * swapped[c]
            total = term if total is None else total + term
        outs.append(total)
    return outs


def weights_of(rows):
    lane = lane_of((rows, LANES))
    k, j = lane & 7, (lane >> 3) & 7
    half = lambda cond: jnp.where(cond, 0.5, 1.0)
    base = half((k == 0) | (k == 7)) * half((j == 0) | (j == 7))
    return [base * half(lane < 64), base, base, base * half(lane >= 64)]


def pack_i_face(x, side):
    h = x.shape[0] // 2
    top, bottom = x[:h], x[h:]
    low = lane_of(top.shape) < 64
    if side == 0:
        return jnp.where(low, top, roll(bottom, 64))
    return jnp.where(low, roll(top, 64), bottom)


def unpack_i_face(m, side):
    other = roll(m, 64)
    return jnp.concatenate([m, other] if side == 0 else [other, m], axis=0)


def pack_j_face(blocks, ez, side):
    half = ez // 2
    lane = lane_of((half, LANES))
    slot = (lane & 63) >> 3
    out = jnp.zeros((half, LANES), jnp.float32)
    for b in range(4):
        rows = blocks[b][:ez] if side == 0 else blocks[b][-ez:]
        for n in range(2):
            moved = roll(rows[n * half : (n + 1) * half], 8 * b + 32 * n - (0 if side == 0 else 56))
            out = jnp.where(slot == b + 4 * n, moved, out)
    return out


def assemble_inside(blocks, ez):
    rows = blocks[0].shape[0]
    lane = lane_of((rows, LANES))
    j, k = (lane >> 3) & 7, lane & 7
    outs = []
    for x in blocks:
        if rows > ez:
            edge = jnp.zeros((ez, LANES), jnp.float32)
            after = jnp.concatenate([roll(x[ez:], 56), edge], axis=0)
            before = jnp.concatenate([edge, roll(x[:-ez], -56)], axis=0)
            x = x + jnp.where(j == 7, after, jnp.where(j == 0, before, 0.0))
        up, down = roll(x, 7), roll(x, -7)
        after = [pltpu.roll(up[e : e + ez], ez - 1, 0) for e in range(0, rows, ez)]
        before = [pltpu.roll(down[e : e + ez], 1, 0) for e in range(0, rows, ez)]
        after, before = jnp.concatenate(after, 0), jnp.concatenate(before, 0)
        outs.append(x + jnp.where(k == 7, after, jnp.where(k == 0, before, 0.0)))
    return outs


def turn_column(x, ez, shift):
    parts = [pltpu.roll(x[e : e + ez], shift % ez, 0) for e in range(0, x.shape[0], ez)]
    return parts[0] if len(parts) == 1 else jnp.concatenate(parts, axis=0)


def summed_j_face(blocks, ez, side):
    half = ez // 2
    lane = lane_of((half, LANES))
    slot, k = (lane & 63) >> 3, lane & 7
    kept = [jnp.zeros((half, LANES), jnp.float32)] * 3
    for b in range(4):
        column = blocks[b][:ez] if side == 0 else blocks[b][-ez:]
        kinds = ((column, 0), (turn_column(column, ez, -1), 7), (turn_column(column, ez, 1), -7))
        for n in range(2):
            shift = 8 * b + 32 * n - 56 * side
            for m, (rows, extra) in enumerate(kinds):
                moved = roll(rows[n * half : (n + 1) * half], shift + extra)
                kept[m] = jnp.where(slot == b + 4 * n, moved, kept[m])
    return kept[0] + jnp.where(k == 7, kept[1], jnp.where(k == 0, kept[2], 0.0))


def summed_i_face(x, ez, side):
    rows = x.shape[0]
    h = rows // 2
    lane = lane_of((h, LANES))
    j, k = (lane >> 3) & 7, lane & 7
    edge = jnp.zeros((ez, LANES), jnp.float32)

    def gather(bottom):
        cut = slice(h, rows) if bottom else slice(0, h)
        base = 64 if bottom != (side == 1) else 0
        total = None
        for column, shift, where in ((0, 0, None), (1, 56, j == 7), (-1, -56, j == 0)):
            if column and (rows == ez or (rows == 2 * ez and bottom == (column == 1))):
                continue
            found = None
            for turn, extra, only in ((0, 0, None), (-1, 7, k == 7), (1, -7, k == 0)):
                y = turn_column(x, ez, turn) if turn else x
                if column == 1:
                    y = jnp.concatenate([y[ez:], edge], axis=0)
                elif column == -1:
                    y = jnp.concatenate([edge, y[:-ez]], axis=0)
                y = roll(y[cut], base + shift + extra)
                y = y if only is None else jnp.where(only, y, 0.0)
                found = y if found is None else found + y
            found = found if where is None else jnp.where(where, found, 0.0)
            total = found if total is None else total + found
        return total

    return jnp.where(lane < 64, gather(False), gather(True))


def add_i_face(blocks, message, side):
    blocks = list(blocks)
    low = lane_of(blocks[0].shape) < 64
    face = unpack_i_face(message, side)
    blocks[3 * side] = blocks[3 * side] + jnp.where(low if side == 0 else ~low, face, 0.0)
    return blocks


def add_j_face(blocks, ez, same, before, after, side):
    lane = lane_of((ez, LANES))
    here = ((lane >> 3) & 7) == 7 * side

    def spread(message, shift):
        return jnp.concatenate([roll(message, shift), roll(message, shift - 32)], axis=0)

    outs = []
    for b, x in enumerate(blocks):
        shift = 56 * side - 8 * b
        face = jnp.where(here, spread(same, shift), 0.0)
        if b == 0:
            face = face + jnp.where(here & (lane < 64), spread(before, shift + 40), 0.0)
        if b == 3:
            face = face + jnp.where(here & (lane >= 64), spread(after, shift + 88), 0.0)
        if x.shape[0] == ez:
            outs.append(x + face)
        elif side == 0:
            outs.append(jnp.concatenate([x[:ez] + face, x[ez:]], axis=0))
        else:
            outs.append(jnp.concatenate([x[:-ez], x[-ez:] + face], axis=0))
    return outs


def halves(x):
    high = x.astype(jnp.bfloat16)
    return high, (x - high.astype(jnp.float32)).astype(jnp.bfloat16)


def dot(left, right):
    return jnp.dot(left, right, preferred_element_type=jnp.float32)


def stack(blocks):
    return jnp.concatenate(blocks, axis=0)


def total_of(blocks):
    x = blocks[0] + blocks[1] + (blocks[2] + blocks[3])
    return jnp.sum(jnp.sum(x, axis=0, keepdims=True), axis=1, keepdims=True)


def owner_weights(rows, ez, first_owned, last_owned, high_owned):
    lane = lane_of((rows, LANES))
    row = lax.broadcasted_iota(jnp.int32, (rows, LANES), 0)
    k, j = lane & 7, (lane >> 3) & 7
    base = jnp.where((k == 0) | (k == 7), 0.5, 1.0)
    first = jnp.where(row < ez, jnp.where(first_owned, 1.0, 0.0), 0.5)
    last = jnp.where(row >= rows - ez, jnp.where(last_owned, 1.0, 0.0), 0.5)
    base = base * jnp.where(j == 0, first, jnp.where(j == 7, last, 1.0))
    high = jnp.where(high_owned, 1.0, 0.0)
    outer = [jnp.where(lane < 64, 0.0, base), base, base, jnp.where(lane < 64, base, high * base)]
    return outer, base


def kernel(
    ng, nd, ez,
    sol_h, res_h, dir_h, geo_h, mass_h, tab_h,
    outs,
    pair_v, dir_v, geo_v, tab_v, early_v,
    face_out, face_in, wrap_in, root_in, relay_in, side_in, side_out, prev_v, next_v, low_v, high_v, part, sums, parts, late_out,
    bulk, load_sem, send_sem, recv_sem, side_recv, last_recv, root_recv, relay_recv, sum_recv, part_recv, go,
):
    me_g, me_d = lax.axis_index("group"), lax.axis_index("dev")

    def at(a, b):
        return (lax.rem(me_g + (a + ng), ng), lax.rem(me_d + (b + nd), nd))

    others = [(a, b) for a in range(ng) for b in range(nd) if (a, b) != (0, 0)]
    others.sort(key=lambda t: (min(t[1], nd - t[1]) != 1, min(t[0], ng - t[0]) > 1))

    pairs = (
        (dir_h, dir_v, 0), (geo_h, geo_v.at[pl.ds(0, 3)], 1), (mass_h, geo_v.at[3], 1),
        (tab_h, tab_v, 1), (res_h, pair_v.at[0], 1), (sol_h, pair_v.at[1], 1),
    )
    loads = [pltpu.make_async_copy(h, v, load_sem.at[n]) for h, v, n in pairs]
    loads[0].start()
    barrier = pltpu.get_barrier_semaphore()
    is_first, is_last, is_near = me_d == 0, me_d == nd - 1, me_d == nd - 2
    odd = (me_g & 1) == 1
    middle = nd // 2 - 1
    is_relay = (me_d == middle) & odd
    own_relay = (me_g | 1, middle)
    partners = [t for t in others if min(t[0], ng - t[0]) < 2 and min(t[1], nd - t[1]) < 2]
    hub = (1 % ng, nd // 2)
    hub_a, hub_b = lax.rem(me_g - hub[0] + ng, ng), lax.rem(me_d - hub[1] + nd, nd)
    at_hub = (hub_a == 0) & (hub_b == 0)
    near_hub = ((hub_a < 2) | (hub_a == ng - 1)) & ((hub_b < 2) | (hub_b == nd - 1))
    @pl.when(is_last)
    def _():
        beside = lax.rem(jnp.where(odd, me_g + 2, me_g + (ng - 1)), ng)
        for target in ((beside, middle), own_relay):
            pl.semaphore_signal(barrier, inc=1, device_id=target, device_id_type=MESH)

    @pl.when(is_relay)
    def _():
        for target in ((me_g, 0), (me_g - 1, 0)):
            pl.semaphore_signal(barrier, inc=1, device_id=target, device_id_type=MESH)

    for a, b in partners:
        if b == 1:

            @pl.when(jnp.logical_not(is_last))
            def _():
                pl.semaphore_signal(barrier, inc=1, device_id=at(a, b), device_id_type=MESH)

        else:
            pl.semaphore_signal(barrier, inc=1, device_id=at(a, b), device_id_type=MESH)

    @pl.when(jnp.logical_not(near_hub))
    def _():
        pl.semaphore_signal(barrier, inc=1, device_id=hub, device_id_type=MESH)

    for load in loads[1:]:
        load.start()

    rows = dir_v.shape[0]
    h, q = rows // 2, ez // 2
    u, span = h + q, 2 * h + 6 * q
    root = min(1, ng - 1)
    is_root = is_first & (me_g == root)
    owns_next = me_d < nd - 5
    is_mid = (me_d == nd - 3) | (me_d == nd - 4)
    owns_high, owns_low = jnp.logical_not(is_last), is_last & odd

    def i_out(phase, side):
        return face_out.at[phase, pl.ds(u * side, h)]

    def i_in(phase, side):
        return face_in.at[pl.ds(span * phase + h * side, h)]

    def j_out(phase, side):
        return face_out.at[phase, pl.ds(2 * h + q if side == 0 else h, q)]

    def j_in(phase, side, turn):
        return face_in.at[pl.ds(span * phase + 2 * h + q * (3 * side + turn), q)]

    def slot(ref, part_of, group):
        return ref.at[pl.ds(pl.multiple_of(q * (ng * part_of + group), q), q)]

    def drain(count, sem):
        ref = face_in.at[pl.ds(0, count)]
        pltpu.make_async_copy(ref, ref, sem).wait()

    def send(src, dst, recv_to, target):
        return pltpu.make_async_remote_copy(
            src_ref=src, dst_ref=dst, send_sem=send_sem, recv_sem=recv_to,
            device_id=target, device_id_type=MESH,
        )

    weights = weights_of(rows)
    cut = [slice(LANES * b, LANES * b + LANES) for b in range(4)]

    def pack(phase, blocks):
        for side in range(2):
            j_out(phase, side)[...] = pack_j_face(blocks, ez, side)
            i_out(phase, side)[...] = pack_i_face(blocks[3 * side], side)

    def give_j(phase, side, step, sem):
        for turn, a in ((2, 1), (0, -1), (1, 0)):
            send(j_out(phase, side), j_in(phase, side, turn), sem, at(a, step)).start()

    def give_i(phase, sems):
        for side, step in ((0, -1), (1, 1)):
            send(i_out(phase, side), i_in(phase, side), sems[side], at(step, 0)).start()

    def give_rest(phase, sems):
        give_j(phase, 1, 1, sems[2])
        give_i(phase, sems[:2])

    def give_relay(phase, sem):
        dst = relay_in.at[pl.ds(pl.multiple_of(q * (2 * phase + (me_g & 1)), q), q)]
        send(j_out(phase, 0), dst, sem, own_relay).start()

    def turns(phase, side):
        return [j_in(phase, side, turn)[...] for turn in (1, 2, 0)]

    def assembled(phase, blocks):
        blocks = add_i_face(add_i_face(blocks, i_in(phase, 1)[...], 0), i_in(phase, 0)[...], 1)
        return add_j_face(add_j_face(blocks, ez, *turns(phase, 1), 0), ez, *turns(phase, 0), 1)

    d = derivative_table().astype(np.float32)
    loads[0].wait()
    weighted = assemble_inside([weights[b] * dir_v[:, cut[b]] for b in range(4)], ez)
    pack(0, weighted)
    count = jnp.where(at_hub, len(others), len(partners))
    count = jnp.where(is_relay, len(partners) + 4, count)

    @pl.when(jnp.logical_not(is_first))
    def _():
        pl.semaphore_wait(barrier, count)
        give_j(0, 0, -1, recv_sem)
        give_rest(0, [recv_sem] * 3)

    @pl.when(at_hub)
    def _():
        for a, b in others:
            pl.semaphore_signal(go, inc=1, device_id=at(a, b), device_id_type=MESH)

    pltpu.make_async_copy(bulk, bulk, load_sem.at[1]).wait()
    geo_rows = stack([jnp.concatenate([geo_v[1, :, c], geo_v[2, :, c]], axis=1) for c in cut])
    squared = dot(geo_rows, tab_v[:, 768:1024])
    squared = squared[:, :LANES] + squared[:, LANES:]
    geo = [[geo_v[c, :, cut[b]].astype(jnp.float32) for b in range(4)] for c in range(3)]
    mass = [geo_v[3, :, c].astype(jnp.float32) for c in cut]
    diag = along_i((d * d).T, geo[0])
    diag = [diag[b] + squared[rows * b : rows * b + rows] + mass[b] for b in range(4)]
    diag = assemble_inside(diag, ez)
    pack(1, diag)
    residual = [pair_v[0, :, c] for c in cut]
    spread_res = [weights[b] * residual[b] for b in range(4)]
    mixed = assemble_inside(spread_res, ez)
    pack(2, mixed)

    @pl.when(is_first)
    def _():
        pl.semaphore_wait(barrier, len(partners) - 2)
        give_relay(0, relay_recv.at[me_g & 1])
        give_relay(1, relay_recv.at[2])
        give_relay(2, relay_recv.at[2])
        give_rest(0, [recv_sem] * 3)

    @pl.when(jnp.logical_not(is_first))
    def _():
        give_j(1, 0, -1, side_recv.at[1])
        give_j(2, 0, -1, side_recv.at[1])

    give_rest(1, [side_recv.at[0]] * 3)
    give_rest(2, [side_recv.at[0]] * 3)
    owned, face_owned = owner_weights(rows, ez, False, owns_next, owns_high)

    def pass_on(phase, core, sem):
        for turn, a in ((2, 1), (0, -1), (1, 0)):
            target = lax.rem(me_g + (core - 1 + a + ng), ng)
            src = relay_in.at[pl.ds(q * (2 * phase + core), q)]
            send(src, j_in(phase, 0, turn), sem, (target, nd - 1)).start()

    @pl.when(is_relay)
    def _():
        for core in (1, 0):
            drain(q, relay_recv.at[core])
            pass_on(0, core, recv_sem)
        drain(4 * q, relay_recv.at[2])
        for phase in (1, 2):
            for core in (1, 0):
                pass_on(phase, core, side_recv.at[1])

    @pl.when(jnp.logical_not(at_hub))
    def _():
        pl.semaphore_wait(go, 1)

    def nearly(phase, blocks):
        blocks = add_i_face(add_i_face(blocks, i_in(phase, 1)[...], 0), i_in(phase, 0)[...], 1)
        return add_j_face(blocks, ez, *turns(phase, 1), 0)

    def gather_sides():
        drain(2 * (2 * h + 3 * q), side_recv.at[0])
        for b, x in enumerate(nearly(1, [early_v[0, :, c] for c in cut])):
            early_v[0, :, cut[b]] = x
            early_v[2, :, cut[b]] = 1.0 / x
        for b, x in enumerate(nearly(2, [early_v[1, :, c] for c in cut])):
            early_v[1, :, cut[b]] = x

    for b, c in enumerate(cut):
        early_v[0, :, c] = diag[b]
        early_v[1, :, c] = mixed[b]

    @pl.when(is_last)
    def _():
        gather_sides()

    @pl.when(is_last & odd)
    def _():
        lane = lane_of((h, LANES))
        row = lax.broadcasted_iota(jnp.int32, (h, LANES), 0) + jnp.where(lane < 64, 0, h)
        j, k = (lane >> 3) & 7, lane & 7
        fit = jnp.where(j == 0, jnp.where(row < ez, 0.0, 0.5), 1.0)
        fit = jnp.where(j == 7, jnp.where(row < rows - ez, 0.5, 0.0), fit)
        fit = fit * jnp.where((k == 0) | (k == 7), 0.5, 1.0)
        side_out[...] = fit * pack_i_face(early_v[2, :, cut[3]], 1)
        dst = side_in.at[pl.ds(pl.multiple_of((me_g >> 1) * h, q), h)]
        send(side_out, dst, root_recv, (root, 0)).start()

    drain(span, recv_sem)
    smooth = assembled(0, weighted)

    high, low = halves(stack(smooth))
    grads = dot(jnp.concatenate([high, low], axis=1), tab_v[:, :512])
    grads = grads[:, :256] + grads[:, 256:]
    grad_i = along_i(d, smooth)
    flux_i = [geo[0][b] * grad_i[b] for b in range(4)]
    flux = jnp.concatenate(
        [stack(geo[1]) * grads[:, :LANES], stack(geo[2]) * grads[:, LANES:]], axis=1
    )
    high, low = halves(flux)
    back = dot(jnp.concatenate([high, low], axis=0), tab_v[:, 512:768])
    back = back[: 4 * rows] + back[4 * rows :]
    back = back[:, :LANES] + back[:, LANES:]
    local = along_i(d.T, flux_i)
    local = [local[b] + back[rows * b : rows * b + rows] + mass[b] * smooth[b] for b in range(4)]

    for side in range(2):
        j_out(3, side)[...] = summed_j_face(local, ez, side)
        i_out(3, side)[...] = summed_i_face(local[3 * side], ez, side)

    @pl.when(is_last)
    def _():
        start = pl.multiple_of((me_g & 1) * h, q)
        dst = wrap_in.at[pl.ds(pl.multiple_of(me_g * u, q), u)]
        send(face_out.at[3, pl.ds(start, u)], dst, root_recv, (root, 0)).start()

    def wrap_target(a):
        return lax.rem(me_g + (a + ng), ng)

    def give_wrap(first):
        for turn, a in ((2, 1), (0, -1), (1, 0)):
            target = wrap_target(a)
            wanted = target == 0 if first else (target != 0) & (target != root)

            @pl.when(is_last & wanted)
            def _():
                send(j_out(3, 1), j_in(3, 1, turn), last_recv.at[3], (target, 0)).start()

    @pl.when(is_last)
    def _():
        send(j_out(3, 0), slot(root_in, 5, me_g), root_recv, (root, 0)).start()

    give_wrap(True)

    @pl.when(is_near)
    def _():
        send(j_out(3, 1), slot(root_in, 2, me_g), root_recv, (root, 0)).start()
        send(j_out(3, 0), slot(root_in, 3, me_g), root_recv, (root, 0)).start()

    @pl.when(is_mid | (me_d == nd - 5))
    def _():
        where = jnp.where(me_d == nd - 3, 4, jnp.where(me_d == nd - 4, 8, 11))
        send(j_out(3, 1), slot(root_in, where, me_g), root_recv, (root, 0)).start()

    @pl.when(is_mid)
    def _():
        where = jnp.where(me_d == nd - 3, 9, 12)
        send(j_out(3, 0), slot(root_in, where, me_g), root_recv, (root, 0)).start()

    give_i(3, [last_recv.at[0], last_recv.at[1]])
    give_j(3, 0, -1, last_recv.at[2])

    @pl.when(jnp.logical_not(is_last))
    def _():
        give_j(3, 1, 1, last_recv.at[3])

    @pl.when(is_first & (me_g != root))
    def _():
        send(j_out(3, 0), slot(root_in, 0, me_g), root_recv, (root, 0)).start()

    inside = assemble_inside(local, ez)

    @pl.when(jnp.logical_not(is_last))
    def _():
        gather_sides()

    drain(6 * q, side_recv.at[1])
    inverse = add_j_face([early_v[0, rows - ez :, c] for c in cut], ez, *turns(1, 0), 1)
    inverse = [1.0 / x for x in inverse]
    if rows > ez:
        kept = slice(0, rows - ez)
        inverse = [jnp.concatenate([early_v[2, kept, cut[b]], inverse[b]], axis=0) for b in range(4)]
    mixed = [early_v[1, :, c] for c in cut]

    def shared(side):
        lane = lane_of((q, LANES))
        ends = ((lane & 7) == 0) | ((lane & 7) == 7)
        share = jnp.where((lane < 64) & ((lane & 31) < 8), 0.0, jnp.where(ends, 0.5, 1.0))
        return share * pack_j_face(inverse, ez, side)

    @pl.when(is_first | is_near | is_mid)
    def _():
        side_out[pl.ds(0, q)] = shared(0)

    @pl.when(is_mid)
    def _():
        where = jnp.where(me_d == nd - 3, 10, 13)
        send(side_out.at[pl.ds(0, q)], slot(root_in, where, me_g), root_recv, (root, 0)).start()

    @pl.when(is_first & (me_g != root))
    def _():
        send(side_out.at[pl.ds(0, q)], slot(root_in, 1, me_g), root_recv, (root, 0)).start()

    @pl.when(is_near)
    def _():
        side_out[pl.ds(q, q)] = shared(1)
        dst = root_in.at[pl.ds(pl.multiple_of(q * (6 * ng + 2 * me_g), q), 2 * q)]
        send(side_out.at[pl.ds(0, 2 * q)], dst, root_recv, (root, 0)).start()

    dual = add_j_face(mixed, ez, *turns(2, 0), 1)
    norm_now = total_of([spread_res[b] * residual[b] * inverse[b] for b in range(4)])
    curvature = total_of([smooth[b] * local[b] for b in range(4)])
    cross = total_of([local[b] * dual[b] * inverse[b] for b in range(4)])
    share = [owned[b] * inverse[b] for b in range(4)]
    order = sorted(range(len(others)), key=lambda n: (others[n][1] != 1, others[n][1] != 0))

    def tell(row, table, sem, which=None):
        for n in order:
            a, b = others[n]
            if which is not None and which != (b == 1):
                continue
            send(part.at[pl.ds(row, 1)], table.at[pl.ds(n, 1)], sem, at(a, b)).start()

    lane = lane_of((1, LANES))
    early = jnp.where(lane < 32, norm_now, jnp.where(lane < 64, curvature, cross))
    part[pl.ds(0, 1)] = early

    @pl.when(jnp.logical_not(is_last))
    def _():
        tell(0, sums, sum_recv)

    @pl.when(is_last)
    def _():
        tell(0, sums, sum_recv, True)


    def hold(ref, side):
        for n, value in enumerate(turns(3, side)):
            ref[pl.ds(q * n, q)] = value

    def held(ref):
        return [ref[pl.ds(q * n, q)] for n in range(3)]

    @pl.when(owns_high)
    def _():
        drain(h, last_recv.at[0])
        high_v[...] = i_in(3, 0)[...]

    @pl.when(is_last)
    def _():
        high_v[...] = jnp.zeros_like(high_v)

    @pl.when(owns_next)
    def _():
        drain(3 * q, last_recv.at[2])
        hold(next_v, 0)

    @pl.when(jnp.logical_not(owns_next))
    def _():
        next_v[...] = jnp.zeros_like(next_v)

    mostly = add_i_face(inside, high_v[...], 1)
    mostly = add_j_face(mostly, ez, *held(next_v), 1)
    quad = stack([share[b] * mostly[b] * mostly[b] for b in range(4)])
    quad = jnp.sum(quad, axis=0, keepdims=True)
    part[pl.ds(1, 1)] = quad

    @pl.when(owns_low)
    def _():
        face = pack_i_face(mostly[0], 0)
        fit = pack_i_face(face_owned * inverse[0], 0)
        drain(h, last_recv.at[1])
        met = i_in(3, 1)[...]
        low_v[...] = met
        face = face + met
        part[pl.ds(1, 1)] = quad + jnp.sum(face * face * fit, axis=0, keepdims=True)

    @pl.when(jnp.logical_not(is_last))
    def _():
        tell(1, parts, part_recv)

    @pl.when(is_last)
    def _():
        tell(1, parts, part_recv)
        tell(0, sums, sum_recv, False)

    give_wrap(False)

    @pl.when(is_root)
    def _():
        slot(root_in, 0, me_g)[...] = j_out(3, 0)[...]
        slot(root_in, 1, me_g)[...] = side_out[pl.ds(0, q)]
        drain((14 * ng - 2) * q + ng // 2 * h + ng * u, root_recv)

        def far(g):
            return wrap_in[pl.ds(u * g + (0 if g & 1 else h), q)]

        def across(g):
            return wrap_in[pl.ds(u * g + (q if g & 1 else 0), h)]

        def got(part_of, g):
            return root_in[pl.ds(q * (ng * part_of + g), q)]

        def paired(g, n):
            return root_in[pl.ds(q * (6 * ng + 2 * g + n), q)]

        spot = lane_of((q, LANES))
        seam = (spot >= 64) & ((spot & 31) >= 24)
        total = None
        groups = range(ng)
        seams = (
            ([got(3, g) + got(4, g) for g in groups], [paired(g, 0) for g in groups]),
            ([got(2, g) + got(5, g) for g in groups], [paired(g, 1) for g in groups]),
            ([got(8, g) + got(9, g) for g in groups], [got(10, g) for g in groups]),
            ([got(11, g) + got(12, g) for g in groups], [got(13, g) for g in groups]),
            ([got(0, g) + far(g) for g in groups], [got(1, g) for g in groups]),
        )
        for faces, fits in seams:
            for g in groups:
                face = faces[g] + jnp.where(seam, roll(faces[(g + 1) % ng], 88), 0.0)
                term = face * face * fits[g]
                total = term if total is None else total + term
        for g in range(1, ng, 2):
            face = across(g) + across((g + 1) % ng)
            term = face * face * side_in[pl.ds(h * (g // 2), h)]
            for n in range(0, h, q):
                total = total + term[n : n + q]
        total = jnp.sum(total, axis=0, keepdims=True)
        parts[pl.ds(len(others), 1)] = total
        late_out[...] = total
        for n, shift in enumerate((0, ng - 1, 1)):
            g = lax.rem(me_g + shift, ng)
            prev_v[pl.ds(q * n, q)] = wrap_in[pl.ds(pl.multiple_of(u * g + h * (1 - (g & 1)), q), q)]

    heard = [(g, b) for b in range(nd) for g in range(ng) if (g, b) != (root, 0)]

    @pl.when(is_root)
    def _():
        for target in heard:
            send(late_out, parts.at[pl.ds(len(others), 1)], part_recv, target).start()

    @pl.when(jnp.logical_not(owns_low))
    def _():
        drain(h, last_recv.at[1])
        low_v[...] = i_in(3, 1)[...]

    @pl.when(is_last)
    def _():
        drain(h, last_recv.at[0])
        high_v[...] = i_in(3, 0)[...]

    @pl.when(jnp.logical_not(owns_next))
    def _():
        drain(3 * q, last_recv.at[2])
        hold(next_v, 0)

    @pl.when(jnp.logical_not(is_root))
    def _():
        drain(3 * q, last_recv.at[3])
        hold(prev_v, 1)

    applied = add_i_face(add_i_face(inside, low_v[...], 0), high_v[...], 1)
    applied = add_j_face(add_j_face(applied, ez, *held(prev_v), 0), ez, *held(next_v), 1)

    drain(len(others), sum_recv)
    everyone = early + jnp.sum(sums[pl.ds(0, len(others))], axis=0, keepdims=True)
    norm_now, curvature, cross = (everyone[:, 32 * n : 32 * n + 1] for n in range(3))
    step = norm_now / curvature
    shrunk = norm_now - 2.0 * step * cross
    scale = step * step
    moved = []
    for b, c in enumerate(cut):
        outs[0, :, c] = pair_v[1, :, c] + step * smooth[b]
        out = residual[b] - step * applied[b]
        outs[1, :, c] = out
        moved.append(out * inverse[b])

    @pl.when(is_root)
    def _():
        drain(len(others), part_recv)

    @pl.when(jnp.logical_not(is_root))
    def _():
        drain(len(others) + 1, part_recv)

    quad = part[pl.ds(1, 1)] + jnp.sum(parts[...], axis=0, keepdims=True)
    quad = jnp.sum(quad, axis=1, keepdims=True)
    ratio = (shrunk + scale * quad) / norm_now
    for b, c in enumerate(cut):
        outs[2, :, c] = moved[b] + ratio * smooth[b]
    common = 4 * span + 2 * len(others)
    roles = [
        (is_root, len(heard) - 6 * q),
        (is_first & jnp.logical_not(is_root), 2 * q - 6 * q),
        (is_near, 4 * q),
        (is_mid, 3 * q),
        ((me_d == nd - 5) & is_relay, 19 * q),
        ((me_d == nd - 5) & jnp.logical_not(is_relay), q),
        ((me_d > 0) & (me_d < nd - 5) & is_relay, 18 * q),
        ((me_d > 0) & (me_d < nd - 5) & jnp.logical_not(is_relay), 0),
    ]
    skipped = sum(jnp.where(wrap_target(a) == root, 1, 0) for a in (-1, 0, 1))
    for n in range(4):
        roles.append((is_last & odd & (skipped == n), u + h + q - n * q))
        roles.append((is_last & jnp.logical_not(odd) & (skipped == n), u + q - n * q))

    for role, extra in roles:

        @pl.when(role)
        def _():
            drain(common + extra, send_sem)


def deliver(stacked, *refs):
    for n in range(3):
        pltpu.make_async_copy(stacked.at[n], refs[n], refs[3]).start()
    pltpu.make_async_copy(stacked, stacked, refs[3]).wait()


def on_device(solution, residual, direction, geometry, mass):
    dims = solution.shape
    ng, nd = lax.axis_size("group"), lax.axis_size("dev")
    ez, points = dims[2], dims[3]
    rows = dims[0] * dims[1] * ez
    flat = (rows, points)
    f32, bf16 = jnp.float32, jnp.bfloat16
    table = jnp.asarray(tables())
    h, q = rows // 2, ez // 2
    u, q8 = h + q, 8
    spare = max(14 * ng * q + ng * (u + h), 4 * (2 * h + 6 * q) + 3 * ng * nd + 32 * q)
    bulk = (2 * rows * points * 4 + 4 * rows * points * 2 + table.size * 2) // (4 * LANES)
    spare = -(-spare // q8) * q8
    stacked = pl.pallas_call(
        functools.partial(kernel, ng, nd, ez),
        out_shape=pltpu.VMEM((3,) + flat, f32),
        in_specs=[pl.BlockSpec(memory_space=pltpu.HBM)] * 6,
        out_specs=pl.BlockSpec(memory_space=pltpu.VMEM),
        scratch_shapes=[
            pltpu.VMEM((2,) + flat, f32),
            pltpu.VMEM(flat, f32),
            pltpu.VMEM((4,) + flat, bf16),
            pltpu.VMEM(table.shape, bf16),
            pltpu.VMEM((3,) + flat, f32),
            pltpu.VMEM((4, 2 * u, LANES), f32),
            pltpu.VMEM((spare, LANES), f32),
            pltpu.VMEM((ng * u, LANES), f32),
            pltpu.VMEM((14 * ng * q, LANES), f32),
            pltpu.VMEM((6 * q, LANES), f32),
            pltpu.VMEM((ng // 2 * h, LANES), f32),
            pltpu.VMEM((h, LANES), f32),
            pltpu.VMEM((3 * q, LANES), f32),
            pltpu.VMEM((3 * q, LANES), f32),
            pltpu.VMEM((h, LANES), f32),
            pltpu.VMEM((h, LANES), f32),
            pltpu.VMEM((2, LANES), f32),
            pltpu.VMEM((ng * nd, LANES), f32),
            pltpu.VMEM((ng * nd, LANES), f32),
            pltpu.VMEM((1, LANES), f32),
            pltpu.VMEM((bulk, LANES), f32),
            pltpu.SemaphoreType.DMA((2,)),
            pltpu.SemaphoreType.DMA,
            pltpu.SemaphoreType.DMA,
            pltpu.SemaphoreType.DMA((2,)),
            pltpu.SemaphoreType.DMA((4,)),
            pltpu.SemaphoreType.DMA,
            pltpu.SemaphoreType.DMA((3,)),
            pltpu.SemaphoreType.DMA,
            pltpu.SemaphoreType.DMA,
            pltpu.SemaphoreType.REGULAR,
        ],
        compiler_params=pltpu.CompilerParams(collective_id=0, has_side_effects=True, vmem_limit_bytes=8 << 20),
    )(
        pltpu.with_memory_space_constraint(solution.reshape(flat), pltpu.HBM),
        pltpu.with_memory_space_constraint(residual.reshape(flat), pltpu.HBM),
        pltpu.with_memory_space_constraint(direction.reshape(flat), pltpu.HBM),
        pltpu.with_memory_space_constraint(geometry.reshape((3,) + flat), pltpu.HBM),
        pltpu.with_memory_space_constraint(mass.reshape(flat), pltpu.HBM),
        pltpu.with_memory_space_constraint(table, pltpu.HBM),
    )
    outs = pl.pallas_call(
        deliver,
        out_shape=[jax.ShapeDtypeStruct(flat, f32)] * 3,
        in_specs=[pl.BlockSpec(memory_space=pl.ANY)],
        out_specs=[pl.BlockSpec(memory_space=pltpu.HBM)] * 3,
        scratch_shapes=[pltpu.SemaphoreType.DMA],
        compiler_params=pltpu.CompilerParams(vmem_limit_bytes=8 << 20),
    )(stacked)
    return tuple(x.reshape(dims) for x in outs)


def solution(mesh):
    spec = P("group", "dev", None, None)
    return jax.shard_map(
        on_device,
        mesh=mesh,
        in_specs=(spec, spec, spec, P(None, "group", "dev", None, None), spec),
        out_specs=(spec, spec, spec),
        check_vma=False,
    )
```

```python
import functools

import jax
import jax.numpy as jnp
import numpy as np
from jax import lax
from jax.experimental import pallas as pl
from jax.experimental.pallas import tpu as pltpu
from jax.sharding import PartitionSpec as P

NP = 8
LANES = 128
MESH = pl.DeviceIdType.MESH

lobatto_nodes = [
    -1.0,
    -0.8717401485096066,
    -0.5917001814331423,
    -0.2092992179024789,
    0.2092992179024789,
    0.5917001814331423,
    0.8717401485096066,
    1.0,
]


def derivative_table():
    nodes = np.array(lobatto_nodes)
    identity = np.eye(NP)
    offset = nodes[:, None] - nodes[None, :] + identity
    barycentric = 1.0 / np.prod(offset, axis=1)
    derivative = barycentric[None, :] / barycentric[:, None] / offset * (1.0 - identity)
    return derivative - identity * np.sum(derivative, axis=1)[:, None]


def split_table(table):
    table = np.asarray(table, np.float32)
    high = table.astype(jnp.bfloat16)
    low = (table - high.astype(np.float32)).astype(jnp.bfloat16)
    return high, low


def tables():
    d = derivative_table().astype(np.float32)
    along_j = np.kron(np.kron(np.eye(2), d), np.eye(NP))
    along_k = np.kron(np.eye(16), d)
    high, low = split_table(np.concatenate([along_j.T, along_k.T], axis=1))
    forward = np.concatenate([np.concatenate([high, high], 0), np.concatenate([low, low], 0)], 1)
    high, low = split_table(np.concatenate([along_j, along_k], axis=0))
    backward = np.concatenate([high, low], axis=1)
    high, low = split_table(np.concatenate([along_j * along_j, along_k * along_k], axis=0))
    squares = np.concatenate([high, low], axis=1)
    return np.concatenate([forward, backward, squares], axis=1)


def roll(x, shift):
    shift %= LANES
    return x if shift == 0 else pltpu.roll(x, shift, 1)


def lane_of(shape):
    return lax.broadcasted_iota(jnp.int32, shape, 1)


def along_i(table, blocks):
    low = lane_of(blocks[0].shape) < 64
    swapped = [roll(x, 64) for x in blocks]
    outs = []
    for b in range(4):
        total = None
        for c in range(4):
            same = jnp.where(low, float(table[2 * b, 2 * c]), float(table[2 * b + 1, 2 * c + 1]))
            other = jnp.where(low, float(table[2 * b, 2 * c + 1]), float(table[2 * b + 1, 2 * c]))
            term = same * blocks[c] + other * swapped[c]
            total = term if total is None else total + term
        outs.append(total)
    return outs


def weights_of(rows):
    lane = lane_of((rows, LANES))
    k, j = lane & 7, (lane >> 3) & 7
    half = lambda cond: jnp.where(cond, 0.5, 1.0)
    base = half((k == 0) | (k == 7)) * half((j == 0) | (j == 7))
    return [base * half(lane < 64), base, base, base * half(lane >= 64)]


def pack_i_face(x, side):
    h = x.shape[0] // 2
    top, bottom = x[:h], x[h:]
    low = lane_of(top.shape) < 64
    if side == 0:
        return jnp.where(low, top, roll(bottom, 64))
    return jnp.where(low, roll(top, 64), bottom)


def unpack_i_face(m, side):
    other = roll(m, 64)
    return jnp.concatenate([m, other] if side == 0 else [other, m], axis=0)


def pack_j_face(blocks, ez, side):
    half = ez // 2
    lane = lane_of((half, LANES))
    slot = (lane & 63) >> 3
    out = jnp.zeros((half, LANES), jnp.float32)
    for b in range(4):
        rows = blocks[b][:ez] if side == 0 else blocks[b][-ez:]
        for n in range(2):
            moved = roll(rows[n * half : (n + 1) * half], 8 * b + 32 * n - (0 if side == 0 else 56))
            out = jnp.where(slot == b + 4 * n, moved, out)
    return out


def assemble_inside(blocks, ez):
    rows = blocks[0].shape[0]
    lane = lane_of((rows, LANES))
    j, k = (lane >> 3) & 7, lane & 7
    outs = []
    for x in blocks:
        if rows > ez:
            edge = jnp.zeros((ez, LANES), jnp.float32)
            after = jnp.concatenate([roll(x[ez:], 56), edge], axis=0)
            before = jnp.concatenate([edge, roll(x[:-ez], -56)], axis=0)
            x = x + jnp.where(j == 7, after, jnp.where(j == 0, before, 0.0))
        up, down = roll(x, 7), roll(x, -7)
        after = [pltpu.roll(up[e : e + ez], ez - 1, 0) for e in range(0, rows, ez)]
        before = [pltpu.roll(down[e : e + ez], 1, 0) for e in range(0, rows, ez)]
        after, before = jnp.concatenate(after, 0), jnp.concatenate(before, 0)
        outs.append(x + jnp.where(k == 7, after, jnp.where(k == 0, before, 0.0)))
    return outs


def turn_column(x, ez, shift):
    parts = [pltpu.roll(x[e : e + ez], shift % ez, 0) for e in range(0, x.shape[0], ez)]
    return parts[0] if len(parts) == 1 else jnp.concatenate(parts, axis=0)


def summed_j_face(blocks, ez, side):
    half = ez // 2
    lane = lane_of((half, LANES))
    slot, k = (lane & 63) >> 3, lane & 7
    kept = [jnp.zeros((half, LANES), jnp.float32)] * 3
    for b in range(4):
        column = blocks[b][:ez] if side == 0 else blocks[b][-ez:]
        kinds = ((column, 0), (turn_column(column, ez, -1), 7), (turn_column(column, ez, 1), -7))
        for n in range(2):
            shift = 8 * b + 32 * n - 56 * side
            for m, (rows, extra) in enumerate(kinds):
                moved = roll(rows[n * half : (n + 1) * half], shift + extra)
                kept[m] = jnp.where(slot == b + 4 * n, moved, kept[m])
    return kept[0] + jnp.where(k == 7, kept[1], jnp.where(k == 0, kept[2], 0.0))


def summed_i_face(x, ez, side):
    rows = x.shape[0]
    h = rows // 2
    lane = lane_of((h, LANES))
    j, k = (lane >> 3) & 7, lane & 7
    edge = jnp.zeros((ez, LANES), jnp.float32)

    def gather(bottom):
        cut = slice(h, rows) if bottom else slice(0, h)
        base = 64 if bottom != (side == 1) else 0
        total = None
        for column, shift, where in ((0, 0, None), (1, 56, j == 7), (-1, -56, j == 0)):
            if column and (rows == ez or (rows == 2 * ez and bottom == (column == 1))):
                continue
            found = None
            for turn, extra, only in ((0, 0, None), (-1, 7, k == 7), (1, -7, k == 0)):
                y = turn_column(x, ez, turn) if turn else x
                if column == 1:
                    y = jnp.concatenate([y[ez:], edge], axis=0)
                elif column == -1:
                    y = jnp.concatenate([edge, y[:-ez]], axis=0)
                y = roll(y[cut], base + shift + extra)
                y = y if only is None else jnp.where(only, y, 0.0)
                found = y if found is None else found + y
            found = found if where is None else jnp.where(where, found, 0.0)
            total = found if total is None else total + found
        return total

    return jnp.where(lane < 64, gather(False), gather(True))


def add_i_face(blocks, message, side):
    blocks = list(blocks)
    low = lane_of(blocks[0].shape) < 64
    face = unpack_i_face(message, side)
    blocks[3 * side] = blocks[3 * side] + jnp.where(low if side == 0 else ~low, face, 0.0)
    return blocks


def add_j_face(blocks, ez, same, before, after, side):
    lane = lane_of((ez, LANES))
    here = ((lane >> 3) & 7) == 7 * side

    def spread(message, shift):
        return jnp.concatenate([roll(message, shift), roll(message, shift - 32)], axis=0)

    outs = []
    for b, x in enumerate(blocks):
        shift = 56 * side - 8 * b
        face = jnp.where(here, spread(same, shift), 0.0)
        if b == 0:
            face = face + jnp.where(here & (lane < 64), spread(before, shift + 40), 0.0)
        if b == 3:
            face = face + jnp.where(here & (lane >= 64), spread(after, shift + 88), 0.0)
        if x.shape[0] == ez:
            outs.append(x + face)
        elif side == 0:
            outs.append(jnp.concatenate([x[:ez] + face, x[ez:]], axis=0))
        else:
            outs.append(jnp.concatenate([x[:-ez], x[-ez:] + face], axis=0))
    return outs


def halves(x):
    high = x.astype(jnp.bfloat16)
    return high, (x - high.astype(jnp.float32)).astype(jnp.bfloat16)


def dot(left, right):
    return jnp.dot(left, right, preferred_element_type=jnp.float32)


def stack(blocks):
    return jnp.concatenate(blocks, axis=0)


def total_of(blocks):
    x = blocks[0] + blocks[1] + (blocks[2] + blocks[3])
    return jnp.sum(jnp.sum(x, axis=0, keepdims=True), axis=1, keepdims=True)


def owner_weights(rows, ez, first_owned, last_owned, high_owned):
    lane = lane_of((rows, LANES))
    row = lax.broadcasted_iota(jnp.int32, (rows, LANES), 0)
    k, j = lane & 7, (lane >> 3) & 7
    base = jnp.where((k == 0) | (k == 7), 0.5, 1.0)
    first = jnp.where(row < ez, jnp.where(first_owned, 1.0, 0.0), 0.5)
    last = jnp.where(row >= rows - ez, jnp.where(last_owned, 1.0, 0.0), 0.5)
    base = base * jnp.where(j == 0, first, jnp.where(j == 7, last, 1.0))
    high = jnp.where(high_owned, 1.0, 0.0)
    outer = [jnp.where(lane < 64, 0.0, base), base, base, jnp.where(lane < 64, base, high * base)]
    return outer, base


def kernel(
    ng, nd, ez,
    sol_h, res_h, dir_h, geo_h, mass_h, tab_h,
    outs,
    pair_v, dir_v, geo_v, tab_v, early_v,
    face_out, face_in, wrap_in, root_in, relay_in, side_in, side_out, prev_v, next_v, low_v, high_v, part, sums, parts, late_out,
    bulk, load_sem, send_sem, recv_sem, side_recv, last_recv, root_recv, relay_recv, sum_recv, part_recv, go,
):
    me_g, me_d = lax.axis_index("group"), lax.axis_index("dev")

    def at(a, b):
        return (lax.rem(me_g + (a + ng), ng), lax.rem(me_d + (b + nd), nd))

    others = [(a, b) for a in range(ng) for b in range(nd) if (a, b) != (0, 0)]
    others.sort(key=lambda t: (min(t[1], nd - t[1]) != 1, min(t[0], ng - t[0]) > 1))

    pairs = (
        (dir_h, dir_v, 0), (geo_h, geo_v.at[pl.ds(0, 3)], 1), (mass_h, geo_v.at[3], 1),
        (tab_h, tab_v, 1), (res_h, pair_v.at[0], 1), (sol_h, pair_v.at[1], 1),
    )
    loads = [pltpu.make_async_copy(h, v, load_sem.at[n]) for h, v, n in pairs]
    loads[0].start()
    barrier = pltpu.get_barrier_semaphore()
    is_first, is_last, is_near = me_d == 0, me_d == nd - 1, me_d == nd - 2
    odd = (me_g & 1) == 1
    middle = nd // 2 - 1
    is_relay = (me_d == middle) & odd
    own_relay = (me_g | 1, middle)
    partners = [t for t in others if min(t[0], ng - t[0]) < 2 and min(t[1], nd - t[1]) < 2]
    hub = (1 % ng, nd // 2)
    hub_a, hub_b = lax.rem(me_g - hub[0] + ng, ng), lax.rem(me_d - hub[1] + nd, nd)
    at_hub = (hub_a == 0) & (hub_b == 0)
    near_hub = ((hub_a < 2) | (hub_a == ng - 1)) & ((hub_b < 2) | (hub_b == nd - 1))
    @pl.when(is_last)
    def _():
        beside = lax.rem(jnp.where(odd, me_g + 2, me_g + (ng - 1)), ng)
        for target in ((beside, middle), own_relay):
            pl.semaphore_signal(barrier, inc=1, device_id=target, device_id_type=MESH)

    @pl.when(is_relay)
    def _():
        for target in ((me_g, 0), (me_g - 1, 0)):
            pl.semaphore_signal(barrier, inc=1, device_id=target, device_id_type=MESH)

    for a, b in partners:
        if b == 1:

            @pl.when(jnp.logical_not(is_last))
            def _():
                pl.semaphore_signal(barrier, inc=1, device_id=at(a, b), device_id_type=MESH)

        else:
            pl.semaphore_signal(barrier, inc=1, device_id=at(a, b), device_id_type=MESH)

    @pl.when(jnp.logical_not(near_hub))
    def _():
        pl.semaphore_signal(barrier, inc=1, device_id=hub, device_id_type=MESH)

    for load in loads[1:]:
        load.start()

    rows = dir_v.shape[0]
    h, q = rows // 2, ez // 2
    u, span = h + q, 2 * h + 6 * q
    root = min(1, ng - 1)
    is_root = is_first & (me_g == root)
    owns_next = me_d < nd - 7
    is_mid = (me_d >= nd - 6) & (me_d <= nd - 3)
    place = 3 * (nd - 3 - me_d)
    owns_high, owns_low = jnp.logical_not(is_last), is_last & odd

    def i_out(phase, side):
        return face_out.at[phase, pl.ds(u * side, h)]

    def i_in(phase, side):
        return face_in.at[pl.ds(span * phase + h * side, h)]

    def j_out(phase, side):
        return face_out.at[phase, pl.ds(2 * h + q if side == 0 else h, q)]

    def j_in(phase, side, turn):
        return face_in.at[pl.ds(span * phase + 2 * h + q * (3 * side + turn), q)]

    def slot(ref, part_of, group):
        return ref.at[pl.ds(pl.multiple_of(q * (ng * part_of + group), q), q)]

    def drain(count, sem):
        ref = face_in.at[pl.ds(0, count)]
        pltpu.make_async_copy(ref, ref, sem).wait()

    def send(src, dst, recv_to, target):
        return pltpu.make_async_remote_copy(
            src_ref=src, dst_ref=dst, send_sem=send_sem, recv_sem=recv_to,
            device_id=target, device_id_type=MESH,
        )

    weights = weights_of(rows)
    cut = [slice(LANES * b, LANES * b + LANES) for b in range(4)]

    def pack(phase, blocks):
        for side in range(2):
            j_out(phase, side)[...] = pack_j_face(blocks, ez, side)
            i_out(phase, side)[...] = pack_i_face(blocks[3 * side], side)

    def give_j(phase, side, step, sem):
        for turn, a in ((2, 1), (0, -1), (1, 0)):
            send(j_out(phase, side), j_in(phase, side, turn), sem, at(a, step)).start()

    def give_i(phase, sems):
        for side, step in ((0, -1), (1, 1)):
            send(i_out(phase, side), i_in(phase, side), sems[side], at(step, 0)).start()

    def give_rest(phase, sems):
        give_j(phase, 1, 1, sems[2])
        give_i(phase, sems[:2])

    def give_relay(phase, sem):
        dst = relay_in.at[pl.ds(pl.multiple_of(q * (2 * phase + (me_g & 1)), q), q)]
        send(j_out(phase, 0), dst, sem, own_relay).start()

    def turns(phase, side):
        return [j_in(phase, side, turn)[...] for turn in (1, 2, 0)]

    def assembled(phase, blocks):
        blocks = add_i_face(add_i_face(blocks, i_in(phase, 1)[...], 0), i_in(phase, 0)[...], 1)
        return add_j_face(add_j_face(blocks, ez, *turns(phase, 1), 0), ez, *turns(phase, 0), 1)

    d = derivative_table().astype(np.float32)
    loads[0].wait()
    weighted = assemble_inside([weights[b] * dir_v[:, cut[b]] for b in range(4)], ez)
    pack(0, weighted)
    count = jnp.where(at_hub, len(others), len(partners))
    count = jnp.where(is_relay, len(partners) + 4, count)

    @pl.when(jnp.logical_not(is_first))
    def _():
        pl.semaphore_wait(barrier, count)
        give_j(0, 0, -1, recv_sem)
        give_rest(0, [recv_sem] * 3)

    @pl.when(at_hub)
    def _():
        for a, b in others:
            pl.semaphore_signal(go, inc=1, device_id=at(a, b), device_id_type=MESH)

    pltpu.make_async_copy(bulk, bulk, load_sem.at[1]).wait()
    geo_rows = stack([jnp.concatenate([geo_v[1, :, c], geo_v[2, :, c]], axis=1) for c in cut])
    squared = dot(geo_rows, tab_v[:, 768:1024])
    squared = squared[:, :LANES] + squared[:, LANES:]
    geo = [[geo_v[c, :, cut[b]].astype(jnp.float32) for b in range(4)] for c in range(3)]
    mass = [geo_v[3, :, c].astype(jnp.float32) for c in cut]
    diag = along_i((d * d).T, geo[0])
    diag = [diag[b] + squared[rows * b : rows * b + rows] + mass[b] for b in range(4)]
    diag = assemble_inside(diag, ez)
    pack(1, diag)
    residual = [pair_v[0, :, c] for c in cut]
    spread_res = [weights[b] * residual[b] for b in range(4)]
    mixed = assemble_inside(spread_res, ez)
    pack(2, mixed)

    @pl.when(is_first)
    def _():
        pl.semaphore_wait(barrier, len(partners) - 2)
        give_relay(0, relay_recv.at[me_g & 1])
        give_relay(1, relay_recv.at[2])
        give_relay(2, relay_recv.at[2])
        give_rest(0, [recv_sem] * 3)

    @pl.when(jnp.logical_not(is_first))
    def _():
        give_j(1, 0, -1, side_recv.at[1])
        give_j(2, 0, -1, side_recv.at[1])

    give_rest(1, [side_recv.at[0]] * 3)
    give_rest(2, [side_recv.at[0]] * 3)
    owned, face_owned = owner_weights(rows, ez, False, owns_next, owns_high)

    def pass_on(phase, core, sem):
        for turn, a in ((2, 1), (0, -1), (1, 0)):
            target = lax.rem(me_g + (core - 1 + a + ng), ng)
            src = relay_in.at[pl.ds(q * (2 * phase + core), q)]
            send(src, j_in(phase, 0, turn), sem, (target, nd - 1)).start()

    @pl.when(is_relay)
    def _():
        for core in (1, 0):
            drain(q, relay_recv.at[core])
            pass_on(0, core, recv_sem)
        drain(4 * q, relay_recv.at[2])
        for phase in (1, 2):
            for core in (1, 0):
                pass_on(phase, core, side_recv.at[1])

    @pl.when(jnp.logical_not(at_hub))
    def _():
        pl.semaphore_wait(go, 1)

    def nearly(phase, blocks):
        blocks = add_i_face(add_i_face(blocks, i_in(phase, 1)[...], 0), i_in(phase, 0)[...], 1)
        return add_j_face(blocks, ez, *turns(phase, 1), 0)

    def gather_sides():
        drain(2 * (2 * h + 3 * q), side_recv.at[0])
        for b, x in enumerate(nearly(1, [early_v[0, :, c] for c in cut])):
            early_v[0, :, cut[b]] = x
            early_v[2, :, cut[b]] = 1.0 / x
        for b, x in enumerate(nearly(2, [early_v[1, :, c] for c in cut])):
            early_v[1, :, cut[b]] = x

    for b, c in enumerate(cut):
        early_v[0, :, c] = diag[b]
        early_v[1, :, c] = mixed[b]

    @pl.when(is_last)
    def _():
        gather_sides()

    @pl.when(is_last & odd)
    def _():
        lane = lane_of((h, LANES))
        row = lax.broadcasted_iota(jnp.int32, (h, LANES), 0) + jnp.where(lane < 64, 0, h)
        j, k = (lane >> 3) & 7, lane & 7
        fit = jnp.where(j == 0, jnp.where(row < ez, 0.0, 0.5), 1.0)
        fit = jnp.where(j == 7, jnp.where(row < rows - ez, 0.5, 0.0), fit)
        fit = fit * jnp.where((k == 0) | (k == 7), 0.5, 1.0)
        side_out[...] = fit * pack_i_face(early_v[2, :, cut[3]], 1)
        dst = side_in.at[pl.ds(pl.multiple_of((me_g >> 1) * h, q), h)]
        send(side_out, dst, root_recv, (root, 0)).start()

    drain(span, recv_sem)
    smooth = assembled(0, weighted)

    high, low = halves(stack(smooth))
    grads = dot(jnp.concatenate([high, low], axis=1), tab_v[:, :512])
    grads = grads[:, :256] + grads[:, 256:]
    grad_i = along_i(d, smooth)
    flux_i = [geo[0][b] * grad_i[b] for b in range(4)]
    flux = jnp.concatenate(
        [stack(geo[1]) * grads[:, :LANES], stack(geo[2]) * grads[:, LANES:]], axis=1
    )
    high, low = halves(flux)
    back = dot(jnp.concatenate([high, low], axis=0), tab_v[:, 512:768])
    back = back[: 4 * rows] + back[4 * rows :]
    back = back[:, :LANES] + back[:, LANES:]
    local = along_i(d.T, flux_i)
    local = [local[b] + back[rows * b : rows * b + rows] + mass[b] * smooth[b] for b in range(4)]

    for side in range(2):
        j_out(3, side)[...] = summed_j_face(local, ez, side)
        i_out(3, side)[...] = summed_i_face(local[3 * side], ez, side)

    @pl.when(is_last)
    def _():
        start = pl.multiple_of((me_g & 1) * h, q)
        dst = wrap_in.at[pl.ds(pl.multiple_of(me_g * u, q), u)]
        send(face_out.at[3, pl.ds(start, u)], dst, root_recv, (root, 0)).start()

    def wrap_target(a):
        return lax.rem(me_g + (a + ng), ng)

    def give_wrap(first):
        for turn, a in ((2, 1), (0, -1), (1, 0)):
            target = wrap_target(a)
            wanted = target == 0 if first else (target != 0) & (target != root)

            @pl.when(is_last & wanted)
            def _():
                send(j_out(3, 1), j_in(3, 1, turn), last_recv.at[3], (target, 0)).start()

    @pl.when(is_last)
    def _():
        send(j_out(3, 0), slot(root_in, 5, me_g), root_recv, (root, 0)).start()

    give_wrap(True)

    @pl.when(is_near)
    def _():
        send(j_out(3, 1), slot(root_in, 2, me_g), root_recv, (root, 0)).start()
        send(j_out(3, 0), slot(root_in, 3, me_g), root_recv, (root, 0)).start()

    @pl.when(is_mid | (me_d == nd - 7))
    def _():
        where = jnp.where(me_d == nd - 3, 4, 5 + place)
        send(j_out(3, 1), slot(root_in, where, me_g), root_recv, (root, 0)).start()

    @pl.when(is_mid)
    def _():
        send(j_out(3, 0), slot(root_in, 9 + place, me_g), root_recv, (root, 0)).start()

    give_i(3, [last_recv.at[0], last_recv.at[1]])
    give_j(3, 0, -1, last_recv.at[2])

    @pl.when(jnp.logical_not(is_last))
    def _():
        give_j(3, 1, 1, last_recv.at[3])

    @pl.when(is_first & (me_g != root))
    def _():
        send(j_out(3, 0), slot(root_in, 0, me_g), root_recv, (root, 0)).start()

    inside = assemble_inside(local, ez)

    @pl.when(jnp.logical_not(is_last))
    def _():
        gather_sides()

    drain(6 * q, side_recv.at[1])
    inverse = add_j_face([early_v[0, rows - ez :, c] for c in cut], ez, *turns(1, 0), 1)
    inverse = [1.0 / x for x in inverse]
    if rows > ez:
        kept = slice(0, rows - ez)
        inverse = [jnp.concatenate([early_v[2, kept, cut[b]], inverse[b]], axis=0) for b in range(4)]
    mixed = [early_v[1, :, c] for c in cut]

    def shared(side):
        lane = lane_of((q, LANES))
        ends = ((lane & 7) == 0) | ((lane & 7) == 7)
        share = jnp.where((lane < 64) & ((lane & 31) < 8), 0.0, jnp.where(ends, 0.5, 1.0))
        return share * pack_j_face(inverse, ez, side)

    @pl.when(is_first | is_near | is_mid)
    def _():
        side_out[pl.ds(0, q)] = shared(0)

    @pl.when(is_mid)
    def _():
        send(side_out.at[pl.ds(0, q)], slot(root_in, 10 + place, me_g), root_recv, (root, 0)).start()

    @pl.when(is_first & (me_g != root))
    def _():
        send(side_out.at[pl.ds(0, q)], slot(root_in, 1, me_g), root_recv, (root, 0)).start()

    @pl.when(is_near)
    def _():
        side_out[pl.ds(q, q)] = shared(1)
        dst = root_in.at[pl.ds(pl.multiple_of(q * (6 * ng + 2 * me_g), q), 2 * q)]
        send(side_out.at[pl.ds(0, 2 * q)], dst, root_recv, (root, 0)).start()

    dual = add_j_face(mixed, ez, *turns(2, 0), 1)
    norm_now = total_of([spread_res[b] * residual[b] * inverse[b] for b in range(4)])
    curvature = total_of([smooth[b] * local[b] for b in range(4)])
    cross = total_of([local[b] * dual[b] * inverse[b] for b in range(4)])
    share = [owned[b] * inverse[b] for b in range(4)]
    order = sorted(range(len(others)), key=lambda n: (others[n][1] != 1, others[n][1] != 0))

    def tell(row, table, sem, which=None):
        for n in order:
            a, b = others[n]
            if which is not None and which != (b == 1):
                continue
            send(part.at[pl.ds(row, 1)], table.at[pl.ds(n, 1)], sem, at(a, b)).start()

    lane = lane_of((1, LANES))
    early = jnp.where(lane < 32, norm_now, jnp.where(lane < 64, curvature, cross))
    part[pl.ds(0, 1)] = early

    @pl.when(jnp.logical_not(is_last))
    def _():
        tell(0, sums, sum_recv)

    @pl.when(is_last)
    def _():
        tell(0, sums, sum_recv, True)


    def hold(ref, side):
        for n, value in enumerate(turns(3, side)):
            ref[pl.ds(q * n, q)] = value

    def held(ref):
        return [ref[pl.ds(q * n, q)] for n in range(3)]

    @pl.when(owns_high)
    def _():
        drain(h, last_recv.at[0])
        high_v[...] = i_in(3, 0)[...]

    @pl.when(is_last)
    def _():
        high_v[...] = jnp.zeros_like(high_v)

    @pl.when(owns_next)
    def _():
        drain(3 * q, last_recv.at[2])
        hold(next_v, 0)

    @pl.when(jnp.logical_not(owns_next))
    def _():
        next_v[...] = jnp.zeros_like(next_v)

    mostly = add_i_face(inside, high_v[...], 1)
    mostly = add_j_face(mostly, ez, *held(next_v), 1)
    quad = stack([share[b] * mostly[b] * mostly[b] for b in range(4)])
    quad = jnp.sum(quad, axis=0, keepdims=True)
    part[pl.ds(1, 1)] = quad

    @pl.when(owns_low)
    def _():
        face = pack_i_face(mostly[0], 0)
        fit = pack_i_face(face_owned * inverse[0], 0)
        drain(h, last_recv.at[1])
        met = i_in(3, 1)[...]
        low_v[...] = met
        face = face + met
        part[pl.ds(1, 1)] = quad + jnp.sum(face * face * fit, axis=0, keepdims=True)

    @pl.when(jnp.logical_not(is_last))
    def _():
        tell(1, parts, part_recv)

    @pl.when(is_last)
    def _():
        tell(1, parts, part_recv)
        tell(0, sums, sum_recv, False)

    give_wrap(False)

    @pl.when(is_root)
    def _():
        slot(root_in, 0, me_g)[...] = j_out(3, 0)[...]
        slot(root_in, 1, me_g)[...] = side_out[pl.ds(0, q)]
        drain((20 * ng - 2) * q + ng // 2 * h + ng * u, root_recv)

        def far(g):
            return wrap_in[pl.ds(u * g + (0 if g & 1 else h), q)]

        def across(g):
            return wrap_in[pl.ds(u * g + (q if g & 1 else 0), h)]

        def got(part_of, g):
            return root_in[pl.ds(q * (ng * part_of + g), q)]

        def paired(g, n):
            return root_in[pl.ds(q * (6 * ng + 2 * g + n), q)]

        spot = lane_of((q, LANES))
        seam = (spot >= 64) & ((spot & 31) >= 24)
        total = None
        groups = range(ng)
        seams = (
            ([got(3, g) + got(4, g) for g in groups], [paired(g, 0) for g in groups]),
            ([got(2, g) + got(5, g) for g in groups], [paired(g, 1) for g in groups]),
            ([got(8, g) + got(9, g) for g in groups], [got(10, g) for g in groups]),
            ([got(11, g) + got(12, g) for g in groups], [got(13, g) for g in groups]),
            ([got(14, g) + got(15, g) for g in groups], [got(16, g) for g in groups]),
            ([got(17, g) + got(18, g) for g in groups], [got(19, g) for g in groups]),
            ([got(0, g) + far(g) for g in groups], [got(1, g) for g in groups]),
        )
        for faces, fits in seams:
            for g in groups:
                face = faces[g] + jnp.where(seam, roll(faces[(g + 1) % ng], 88), 0.0)
                term = face * face * fits[g]
                total = term if total is None else total + term
        for g in range(1, ng, 2):
            face = across(g) + across((g + 1) % ng)
            term = face * face * side_in[pl.ds(h * (g // 2), h)]
            for n in range(0, h, q):
                total = total + term[n : n + q]
        total = jnp.sum(total, axis=0, keepdims=True)
        parts[pl.ds(len(others), 1)] = total
        late_out[...] = total
        for n, shift in enumerate((0, ng - 1, 1)):
            g = lax.rem(me_g + shift, ng)
            prev_v[pl.ds(q * n, q)] = wrap_in[pl.ds(pl.multiple_of(u * g + h * (1 - (g & 1)), q), q)]

    heard = [(g, b) for b in range(nd) for g in range(ng) if (g, b) != (root, 0)]

    @pl.when(is_root)
    def _():
        for target in heard:
            send(late_out, parts.at[pl.ds(len(others), 1)], part_recv, target).start()

    @pl.when(jnp.logical_not(owns_low))
    def _():
        drain(h, last_recv.at[1])
        low_v[...] = i_in(3, 1)[...]

    @pl.when(is_last)
    def _():
        drain(h, last_recv.at[0])
        high_v[...] = i_in(3, 0)[...]

    @pl.when(jnp.logical_not(owns_next))
    def _():
        drain(3 * q, last_recv.at[2])
        hold(next_v, 0)

    @pl.when(jnp.logical_not(is_root))
    def _():
        drain(3 * q, last_recv.at[3])
        hold(prev_v, 1)

    applied = add_i_face(add_i_face(inside, low_v[...], 0), high_v[...], 1)
    applied = add_j_face(add_j_face(applied, ez, *held(prev_v), 0), ez, *held(next_v), 1)

    drain(len(others), sum_recv)
    everyone = early + jnp.sum(sums[pl.ds(0, len(others))], axis=0, keepdims=True)
    norm_now, curvature, cross = (everyone[:, 32 * n : 32 * n + 1] for n in range(3))
    step = norm_now / curvature
    shrunk = norm_now - 2.0 * step * cross
    scale = step * step
    moved = []
    for b, c in enumerate(cut):
        outs[0, :, c] = pair_v[1, :, c] + step * smooth[b]
        out = residual[b] - step * applied[b]
        outs[1, :, c] = out
        moved.append(out * inverse[b])

    @pl.when(is_root)
    def _():
        drain(len(others), part_recv)

    @pl.when(jnp.logical_not(is_root))
    def _():
        drain(len(others) + 1, part_recv)

    quad = part[pl.ds(1, 1)] + jnp.sum(parts[...], axis=0, keepdims=True)
    quad = jnp.sum(quad, axis=1, keepdims=True)
    ratio = (shrunk + scale * quad) / norm_now
    for b, c in enumerate(cut):
        outs[2, :, c] = moved[b] + ratio * smooth[b]
    common = 4 * span + 2 * len(others)
    roles = [
        (is_root, len(heard) - 6 * q),
        (is_first & jnp.logical_not(is_root), 2 * q - 6 * q),
        (is_near, 4 * q),
        (is_mid & is_relay, 21 * q),
        (is_mid & jnp.logical_not(is_relay), 3 * q),
        ((me_d == nd - 7) & is_relay, 19 * q),
        ((me_d == nd - 7) & jnp.logical_not(is_relay), q),
        ((me_d > 0) & (me_d < nd - 7) & is_relay, 18 * q),
        ((me_d > 0) & (me_d < nd - 7) & jnp.logical_not(is_relay), 0),
    ]
    skipped = sum(jnp.where(wrap_target(a) == root, 1, 0) for a in (-1, 0, 1))
    for n in range(4):
        roles.append((is_last & odd & (skipped == n), u + h + q - n * q))
        roles.append((is_last & jnp.logical_not(odd) & (skipped == n), u + q - n * q))

    for role, extra in roles:

        @pl.when(role)
        def _():
            drain(common + extra, send_sem)


def deliver(stacked, *refs):
    for n in range(3):
        pltpu.make_async_copy(stacked.at[n], refs[n], refs[3]).start()
    pltpu.make_async_copy(stacked, stacked, refs[3]).wait()


def on_device(solution, residual, direction, geometry, mass):
    dims = solution.shape
    ng, nd = lax.axis_size("group"), lax.axis_size("dev")
    ez, points = dims[2], dims[3]
    rows = dims[0] * dims[1] * ez
    flat = (rows, points)
    f32, bf16 = jnp.float32, jnp.bfloat16
    table = jnp.asarray(tables())
    h, q = rows // 2, ez // 2
    u, q8 = h + q, 8
    spare = max(20 * ng * q + ng * (u + h), 4 * (2 * h + 6 * q) + 3 * ng * nd + 32 * q)
    bulk = (2 * rows * points * 4 + 4 * rows * points * 2 + table.size * 2) // (4 * LANES)
    spare = -(-spare // q8) * q8
    stacked = pl.pallas_call(
        functools.partial(kernel, ng, nd, ez),
        out_shape=pltpu.VMEM((3,) + flat, f32),
        in_specs=[pl.BlockSpec(memory_space=pltpu.HBM)] * 6,
        out_specs=pl.BlockSpec(memory_space=pltpu.VMEM),
        scratch_shapes=[
            pltpu.VMEM((2,) + flat, f32),
            pltpu.VMEM(flat, f32),
            pltpu.VMEM((4,) + flat, bf16),
            pltpu.VMEM(table.shape, bf16),
            pltpu.VMEM((3,) + flat, f32),
            pltpu.VMEM((4, 2 * u, LANES), f32),
            pltpu.VMEM((spare, LANES), f32),
            pltpu.VMEM((ng * u, LANES), f32),
            pltpu.VMEM((20 * ng * q, LANES), f32),
            pltpu.VMEM((6 * q, LANES), f32),
            pltpu.VMEM((ng // 2 * h, LANES), f32),
            pltpu.VMEM((h, LANES), f32),
            pltpu.VMEM((3 * q, LANES), f32),
            pltpu.VMEM((3 * q, LANES), f32),
            pltpu.VMEM((h, LANES), f32),
            pltpu.VMEM((h, LANES), f32),
            pltpu.VMEM((2, LANES), f32),
            pltpu.VMEM((ng * nd, LANES), f32),
            pltpu.VMEM((ng * nd, LANES), f32),
            pltpu.VMEM((1, LANES), f32),
            pltpu.VMEM((bulk, LANES), f32),
            pltpu.SemaphoreType.DMA((2,)),
            pltpu.SemaphoreType.DMA,
            pltpu.SemaphoreType.DMA,
            pltpu.SemaphoreType.DMA((2,)),
            pltpu.SemaphoreType.DMA((4,)),
            pltpu.SemaphoreType.DMA,
            pltpu.SemaphoreType.DMA((3,)),
            pltpu.SemaphoreType.DMA,
            pltpu.SemaphoreType.DMA,
            pltpu.SemaphoreType.REGULAR,
        ],
        compiler_params=pltpu.CompilerParams(collective_id=0, has_side_effects=True, vmem_limit_bytes=8 << 20),
    )(
        pltpu.with_memory_space_constraint(solution.reshape(flat), pltpu.HBM),
        pltpu.with_memory_space_constraint(residual.reshape(flat), pltpu.HBM),
        pltpu.with_memory_space_constraint(direction.reshape(flat), pltpu.HBM),
        pltpu.with_memory_space_constraint(geometry.reshape((3,) + flat), pltpu.HBM),
        pltpu.with_memory_space_constraint(mass.reshape(flat), pltpu.HBM),
        pltpu.with_memory_space_constraint(table, pltpu.HBM),
    )
    outs = pl.pallas_call(
        deliver,
        out_shape=[jax.ShapeDtypeStruct(flat, f32)] * 3,
        in_specs=[pl.BlockSpec(memory_space=pl.ANY)],
        out_specs=[pl.BlockSpec(memory_space=pltpu.HBM)] * 3,
        scratch_shapes=[pltpu.SemaphoreType.DMA],
        compiler_params=pltpu.CompilerParams(vmem_limit_bytes=8 << 20),
    )(stacked)
    return tuple(x.reshape(dims) for x in outs)


def solution(mesh):
    spec = P("group", "dev", None, None)
    return jax.shard_map(
        on_device,
        mesh=mesh,
        in_specs=(spec, spec, spec, P(None, "group", "dev", None, None), spec),
        out_specs=(spec, spec, spec),
        check_vma=False,
    )
```

```python
import functools

import jax
import jax.numpy as jnp
import numpy as np
from jax import lax
from jax.experimental import pallas as pl
from jax.experimental.pallas import tpu as pltpu
from jax.sharding import PartitionSpec as P

NP = 8
LANES = 128
MESH = pl.DeviceIdType.MESH

lobatto_nodes = [
    -1.0,
    -0.8717401485096066,
    -0.5917001814331423,
    -0.2092992179024789,
    0.2092992179024789,
    0.5917001814331423,
    0.8717401485096066,
    1.0,
]


def derivative_table():
    nodes = np.array(lobatto_nodes)
    identity = np.eye(NP)
    offset = nodes[:, None] - nodes[None, :] + identity
    barycentric = 1.0 / np.prod(offset, axis=1)
    derivative = barycentric[None, :] / barycentric[:, None] / offset * (1.0 - identity)
    return derivative - identity * np.sum(derivative, axis=1)[:, None]


def split_table(table):
    table = np.asarray(table, np.float32)
    high = table.astype(jnp.bfloat16)
    low = (table - high.astype(np.float32)).astype(jnp.bfloat16)
    return high, low


def tables():
    d = derivative_table().astype(np.float32)
    along_j = np.kron(np.kron(np.eye(2), d), np.eye(NP))
    along_k = np.kron(np.eye(16), d)
    high, low = split_table(np.concatenate([along_j.T, along_k.T], axis=1))
    forward = np.concatenate([np.concatenate([high, high], 0), np.concatenate([low, low], 0)], 1)
    high, low = split_table(np.concatenate([along_j, along_k], axis=0))
    backward = np.concatenate([high, low], axis=1)
    high, low = split_table(np.concatenate([along_j * along_j, along_k * along_k], axis=0))
    squares = np.concatenate([high, low], axis=1)
    return np.concatenate([forward, backward, squares], axis=1)


def roll(x, shift):
    shift %= LANES
    return x if shift == 0 else pltpu.roll(x, shift, 1)


def lane_of(shape):
    return lax.broadcasted_iota(jnp.int32, shape, 1)


def along_i(table, blocks):
    low = lane_of(blocks[0].shape) < 64
    swapped = [roll(x, 64) for x in blocks]
    outs = []
    for b in range(4):
        total = None
        for c in range(4):
            same = jnp.where(low, float(table[2 * b, 2 * c]), float(table[2 * b + 1, 2 * c + 1]))
            other = jnp.where(low, float(table[2 * b, 2 * c + 1]), float(table[2 * b + 1, 2 * c]))
            term = same * blocks[c] + other * swapped[c]
            total = term if total is None else total + term
        outs.append(total)
    return outs


def weights_of(rows):
    lane = lane_of((rows, LANES))
    k, j = lane & 7, (lane >> 3) & 7
    half = lambda cond: jnp.where(cond, 0.5, 1.0)
    base = half((k == 0) | (k == 7)) * half((j == 0) | (j == 7))
    return [base * half(lane < 64), base, base, base * half(lane >= 64)]


def pack_i_face(x, side):
    h = x.shape[0] // 2
    top, bottom = x[:h], x[h:]
    low = lane_of(top.shape) < 64
    if side == 0:
        return jnp.where(low, top, roll(bottom, 64))
    return jnp.where(low, roll(top, 64), bottom)


def unpack_i_face(m, side):
    other = roll(m, 64)
    return jnp.concatenate([m, other] if side == 0 else [other, m], axis=0)


def pack_j_face(blocks, ez, side):
    half = ez // 2
    lane = lane_of((half, LANES))
    slot = (lane & 63) >> 3
    out = jnp.zeros((half, LANES), jnp.float32)
    for b in range(4):
        rows = blocks[b][:ez] if side == 0 else blocks[b][-ez:]
        for n in range(2):
            moved = roll(rows[n * half : (n + 1) * half], 8 * b + 32 * n - (0 if side == 0 else 56))
            out = jnp.where(slot == b + 4 * n, moved, out)
    return out


def assemble_inside(blocks, ez):
    rows = blocks[0].shape[0]
    lane = lane_of((rows, LANES))
    j, k = (lane >> 3) & 7, lane & 7
    outs = []
    for x in blocks:
        if rows > ez:
            edge = jnp.zeros((ez, LANES), jnp.float32)
            after = jnp.concatenate([roll(x[ez:], 56), edge], axis=0)
            before = jnp.concatenate([edge, roll(x[:-ez], -56)], axis=0)
            x = x + jnp.where(j == 7, after, jnp.where(j == 0, before, 0.0))
        up, down = roll(x, 7), roll(x, -7)
        after = [pltpu.roll(up[e : e + ez], ez - 1, 0) for e in range(0, rows, ez)]
        before = [pltpu.roll(down[e : e + ez], 1, 0) for e in range(0, rows, ez)]
        after, before = jnp.concatenate(after, 0), jnp.concatenate(before, 0)
        outs.append(x + jnp.where(k == 7, after, jnp.where(k == 0, before, 0.0)))
    return outs


def turn_column(x, ez, shift):
    parts = [pltpu.roll(x[e : e + ez], shift % ez, 0) for e in range(0, x.shape[0], ez)]
    return parts[0] if len(parts) == 1 else jnp.concatenate(parts, axis=0)


def summed_j_face(blocks, ez, side):
    half = ez // 2
    lane = lane_of((half, LANES))
    slot, k = (lane & 63) >> 3, lane & 7
    kept = [jnp.zeros((half, LANES), jnp.float32)] * 3
    for b in range(4):
        column = blocks[b][:ez] if side == 0 else blocks[b][-ez:]
        kinds = ((column, 0), (turn_column(column, ez, -1), 7), (turn_column(column, ez, 1), -7))
        for n in range(2):
            shift = 8 * b + 32 * n - 56 * side
            for m, (rows, extra) in enumerate(kinds):
                moved = roll(rows[n * half : (n + 1) * half], shift + extra)
                kept[m] = jnp.where(slot == b + 4 * n, moved, kept[m])
    return kept[0] + jnp.where(k == 7, kept[1], jnp.where(k == 0, kept[2], 0.0))


def summed_i_face(x, ez, side):
    rows = x.shape[0]
    h = rows // 2
    lane = lane_of((h, LANES))
    j, k = (lane >> 3) & 7, lane & 7
    edge = jnp.zeros((ez, LANES), jnp.float32)

    def gather(bottom):
        cut = slice(h, rows) if bottom else slice(0, h)
        base = 64 if bottom != (side == 1) else 0
        total = None
        for column, shift, where in ((0, 0, None), (1, 56, j == 7), (-1, -56, j == 0)):
            if column and (rows == ez or (rows == 2 * ez and bottom == (column == 1))):
                continue
            found = None
            for turn, extra, only in ((0, 0, None), (-1, 7, k == 7), (1, -7, k == 0)):
                y = turn_column(x, ez, turn) if turn else x
                if column == 1:
                    y = jnp.concatenate([y[ez:], edge], axis=0)
                elif column == -1:
                    y = jnp.concatenate([edge, y[:-ez]], axis=0)
                y = roll(y[cut], base + shift + extra)
                y = y if only is None else jnp.where(only, y, 0.0)
                found = y if found is None else found + y
            found = found if where is None else jnp.where(where, found, 0.0)
            total = found if total is None else total + found
        return total

    return jnp.where(lane < 64, gather(False), gather(True))


def add_i_face(blocks, message, side):
    blocks = list(blocks)
    low = lane_of(blocks[0].shape) < 64
    face = unpack_i_face(message, side)
    blocks[3 * side] = blocks[3 * side] + jnp.where(low if side == 0 else ~low, face, 0.0)
    return blocks


def add_j_face(blocks, ez, same, before, after, side):
    lane = lane_of((ez, LANES))
    here = ((lane >> 3) & 7) == 7 * side

    def spread(message, shift):
        return jnp.concatenate([roll(message, shift), roll(message, shift - 32)], axis=0)

    outs = []
    for b, x in enumerate(blocks):
        shift = 56 * side - 8 * b
        face = jnp.where(here, spread(same, shift), 0.0)
        if b == 0:
            face = face + jnp.where(here & (lane < 64), spread(before, shift + 40), 0.0)
        if b == 3:
            face = face + jnp.where(here & (lane >= 64), spread(after, shift + 88), 0.0)
        if x.shape[0] == ez:
            outs.append(x + face)
        elif side == 0:
            outs.append(jnp.concatenate([x[:ez] + face, x[ez:]], axis=0))
        else:
            outs.append(jnp.concatenate([x[:-ez], x[-ez:] + face], axis=0))
    return outs


def halves(x):
    high = x.astype(jnp.bfloat16)
    return high, (x - high.astype(jnp.float32)).astype(jnp.bfloat16)


def dot(left, right):
    return jnp.dot(left, right, preferred_element_type=jnp.float32)


def stack(blocks):
    return jnp.concatenate(blocks, axis=0)


def total_of(blocks):
    x = blocks[0] + blocks[1] + (blocks[2] + blocks[3])
    return jnp.sum(jnp.sum(x, axis=0, keepdims=True), axis=1, keepdims=True)


def owner_weights(rows, ez, first_owned, last_owned, high_owned):
    lane = lane_of((rows, LANES))
    row = lax.broadcasted_iota(jnp.int32, (rows, LANES), 0)
    k, j = lane & 7, (lane >> 3) & 7
    base = jnp.where((k == 0) | (k == 7), 0.5, 1.0)
    first = jnp.where(row < ez, jnp.where(first_owned, 1.0, 0.0), 0.5)
    last = jnp.where(row >= rows - ez, jnp.where(last_owned, 1.0, 0.0), 0.5)
    base = base * jnp.where(j == 0, first, jnp.where(j == 7, last, 1.0))
    high = jnp.where(high_owned, 1.0, 0.0)
    outer = [jnp.where(lane < 64, 0.0, base), base, base, jnp.where(lane < 64, base, high * base)]
    return outer, base


def kernel(
    ng, nd, ez,
    sol_h, res_h, dir_h, geo_h, mass_h, tab_h,
    outs,
    pair_v, dir_v, geo_v, tab_v, early_v,
    face_out, face_in, wrap_in, root_in, relay_in, side_in, side_out, prev_v, next_v, low_v, high_v, part, sums, parts, late_out,
    bulk, load_sem, send_sem, recv_sem, side_recv, last_recv, root_recv, relay_recv, sum_recv, part_recv, go,
):
    me_g, me_d = lax.axis_index("group"), lax.axis_index("dev")

    def at(a, b):
        return (lax.rem(me_g + (a + ng), ng), lax.rem(me_d + (b + nd), nd))

    others = [(a, b) for a in range(ng) for b in range(nd) if (a, b) != (0, 0)]
    others.sort(key=lambda t: (min(t[1], nd - t[1]) != 1, min(t[0], ng - t[0]) > 1))

    pairs = (
        (dir_h, dir_v, 0), (geo_h, geo_v.at[pl.ds(0, 3)], 1), (mass_h, geo_v.at[3], 1),
        (tab_h, tab_v, 1), (res_h, pair_v.at[0], 1), (sol_h, pair_v.at[1], 1),
    )
    loads = [pltpu.make_async_copy(h, v, load_sem.at[n]) for h, v, n in pairs]
    loads[0].start()
    barrier = pltpu.get_barrier_semaphore()
    is_first, is_last, is_near = me_d == 0, me_d == nd - 1, me_d == nd - 2
    odd = (me_g & 1) == 1
    middle = nd // 2 - 1
    is_relay = (me_d == middle) & odd
    own_relay = (me_g | 1, middle)
    partners = [t for t in others if min(t[0], ng - t[0]) < 2 and min(t[1], nd - t[1]) < 2]
    hub = (1 % ng, nd // 2)
    hub_a, hub_b = lax.rem(me_g - hub[0] + ng, ng), lax.rem(me_d - hub[1] + nd, nd)
    at_hub = (hub_a == 0) & (hub_b == 0)
    near_hub = ((hub_a < 2) | (hub_a == ng - 1)) & ((hub_b < 2) | (hub_b == nd - 1))
    @pl.when(is_last)
    def _():
        beside = lax.rem(jnp.where(odd, me_g + 2, me_g + (ng - 1)), ng)
        for target in ((beside, middle), own_relay):
            pl.semaphore_signal(barrier, inc=1, device_id=target, device_id_type=MESH)

    @pl.when(is_relay)
    def _():
        for target in ((me_g, 0), (me_g - 1, 0)):
            pl.semaphore_signal(barrier, inc=1, device_id=target, device_id_type=MESH)

    for a, b in partners:
        if b == 1:

            @pl.when(jnp.logical_not(is_last))
            def _():
                pl.semaphore_signal(barrier, inc=1, device_id=at(a, b), device_id_type=MESH)

        else:
            pl.semaphore_signal(barrier, inc=1, device_id=at(a, b), device_id_type=MESH)

    @pl.when(jnp.logical_not(near_hub))
    def _():
        pl.semaphore_signal(barrier, inc=1, device_id=hub, device_id_type=MESH)

    for load in loads[1:]:
        load.start()

    rows = dir_v.shape[0]
    h, q = rows // 2, ez // 2
    u, span = h + q, 2 * h + 6 * q
    root = min(1, ng - 1)
    is_root = is_first & (me_g == root)
    owns_next = me_d < nd - 7
    is_mid = (me_d >= nd - 6) & (me_d <= nd - 3)
    place = 3 * (nd - 3 - me_d)
    owns_high, owns_low = jnp.logical_not(is_last), is_last & odd

    def i_out(phase, side):
        return face_out.at[phase, pl.ds(u * side, h)]

    def i_in(phase, side):
        return face_in.at[pl.ds(span * phase + h * side, h)]

    def j_out(phase, side):
        return face_out.at[phase, pl.ds(2 * h + q if side == 0 else h, q)]

    def j_in(phase, side, turn):
        return face_in.at[pl.ds(span * phase + 2 * h + q * (3 * side + turn), q)]

    def slot(ref, part_of, group):
        return ref.at[pl.ds(pl.multiple_of(q * (ng * part_of + group), q), q)]

    def drain(count, sem):
        ref = face_in.at[pl.ds(0, count)]
        pltpu.make_async_copy(ref, ref, sem).wait()

    def send(src, dst, recv_to, target):
        return pltpu.make_async_remote_copy(
            src_ref=src, dst_ref=dst, send_sem=send_sem, recv_sem=recv_to,
            device_id=target, device_id_type=MESH,
        )

    weights = weights_of(rows)
    cut = [slice(LANES * b, LANES * b + LANES) for b in range(4)]

    def pack(phase, blocks):
        for side in range(2):
            j_out(phase, side)[...] = pack_j_face(blocks, ez, side)
            i_out(phase, side)[...] = pack_i_face(blocks[3 * side], side)

    def give_j(phase, side, step, sem):
        for turn, a in ((2, 1), (0, -1), (1, 0)):
            send(j_out(phase, side), j_in(phase, side, turn), sem, at(a, step)).start()

    def give_i(phase, sems):
        for side, step in ((0, -1), (1, 1)):
            send(i_out(phase, side), i_in(phase, side), sems[side], at(step, 0)).start()

    def give_rest(phase, sems):
        give_j(phase, 1, 1, sems[2])
        give_i(phase, sems[:2])

    def give_relay(phase, sem):
        dst = relay_in.at[pl.ds(pl.multiple_of(q * (2 * phase + (me_g & 1)), q), q)]
        send(j_out(phase, 0), dst, sem, own_relay).start()

    def turns(phase, side):
        return [j_in(phase, side, turn)[...] for turn in (1, 2, 0)]

    def assembled(phase, blocks):
        blocks = add_i_face(add_i_face(blocks, i_in(phase, 1)[...], 0), i_in(phase, 0)[...], 1)
        return add_j_face(add_j_face(blocks, ez, *turns(phase, 1), 0), ez, *turns(phase, 0), 1)

    d = derivative_table().astype(np.float32)
    loads[0].wait()
    weighted = assemble_inside([weights[b] * dir_v[:, cut[b]] for b in range(4)], ez)
    pack(0, weighted)
    count = jnp.where(at_hub, len(others), len(partners))
    count = jnp.where(is_relay, len(partners) + 4, count)

    @pl.when(jnp.logical_not(is_first))
    def _():
        pl.semaphore_wait(barrier, count)
        give_j(0, 0, -1, recv_sem)
        give_rest(0, [recv_sem] * 3)

    @pl.when(at_hub)
    def _():
        for a, b in others:
            pl.semaphore_signal(go, inc=1, device_id=at(a, b), device_id_type=MESH)

    pltpu.make_async_copy(bulk, bulk, load_sem.at[1]).wait()
    geo_rows = stack([jnp.concatenate([geo_v[1, :, c], geo_v[2, :, c]], axis=1) for c in cut])
    squared = dot(geo_rows, tab_v[:, 768:1024])
    squared = squared[:, :LANES] + squared[:, LANES:]
    geo = [[geo_v[c, :, cut[b]].astype(jnp.float32) for b in range(4)] for c in range(3)]
    mass = [geo_v[3, :, c].astype(jnp.float32) for c in cut]
    diag = along_i((d * d).T, geo[0])
    diag = [diag[b] + squared[rows * b : rows * b + rows] + mass[b] for b in range(4)]
    diag = assemble_inside(diag, ez)
    pack(1, diag)
    residual = [pair_v[0, :, c] for c in cut]
    spread_res = [weights[b] * residual[b] for b in range(4)]
    mixed = assemble_inside(spread_res, ez)
    pack(2, mixed)

    @pl.when(is_first)
    def _():
        pl.semaphore_wait(barrier, len(partners) - 2)
        give_relay(0, relay_recv.at[me_g & 1])
        give_relay(1, relay_recv.at[2])
        give_relay(2, relay_recv.at[2])
        give_rest(0, [recv_sem] * 3)

    @pl.when(jnp.logical_not(is_first))
    def _():
        give_j(1, 0, -1, side_recv.at[1])
        give_j(2, 0, -1, side_recv.at[1])

    give_rest(1, [side_recv.at[0]] * 3)
    give_rest(2, [side_recv.at[0]] * 3)
    owned, face_owned = owner_weights(rows, ez, False, owns_next, owns_high)

    def pass_on(phase, core, sem):
        for turn, a in ((2, 1), (0, -1), (1, 0)):
            target = lax.rem(me_g + (core - 1 + a + ng), ng)
            src = relay_in.at[pl.ds(q * (2 * phase + core), q)]
            send(src, j_in(phase, 0, turn), sem, (target, nd - 1)).start()

    @pl.when(is_relay)
    def _():
        for core in (1, 0):
            drain(q, relay_recv.at[core])
            pass_on(0, core, recv_sem)
        drain(4 * q, relay_recv.at[2])
        for phase in (1, 2):
            for core in (1, 0):
                pass_on(phase, core, side_recv.at[1])

    @pl.when(jnp.logical_not(at_hub))
    def _():
        pl.semaphore_wait(go, 1)

    def nearly(phase, blocks):
        blocks = add_i_face(add_i_face(blocks, i_in(phase, 1)[...], 0), i_in(phase, 0)[...], 1)
        return add_j_face(blocks, ez, *turns(phase, 1), 0)

    def gather_sides():
        drain(2 * (2 * h + 3 * q), side_recv.at[0])
        for b, x in enumerate(nearly(1, [early_v[0, :, c] for c in cut])):
            early_v[0, :, cut[b]] = x
            early_v[2, :, cut[b]] = 1.0 / x
        for b, x in enumerate(nearly(2, [early_v[1, :, c] for c in cut])):
            early_v[1, :, cut[b]] = x

    for b, c in enumerate(cut):
        early_v[0, :, c] = diag[b]
        early_v[1, :, c] = mixed[b]

    @pl.when(is_last)
    def _():
        gather_sides()

    @pl.when(is_last & odd)
    def _():
        lane = lane_of((h, LANES))
        row = lax.broadcasted_iota(jnp.int32, (h, LANES), 0) + jnp.where(lane < 64, 0, h)
        j, k = (lane >> 3) & 7, lane & 7
        fit = jnp.where(j == 0, jnp.where(row < ez, 0.0, 0.5), 1.0)
        fit = jnp.where(j == 7, jnp.where(row < rows - ez, 0.5, 0.0), fit)
        fit = fit * jnp.where((k == 0) | (k == 7), 0.5, 1.0)
        side_out[...] = fit * pack_i_face(early_v[2, :, cut[3]], 1)
        dst = side_in.at[pl.ds(pl.multiple_of((me_g >> 1) * h, q), h)]
        send(side_out, dst, root_recv.at[0], (root, 0)).start()

    drain(span, recv_sem)
    smooth = assembled(0, weighted)

    high, low = halves(stack(smooth))
    grads = dot(jnp.concatenate([high, low], axis=1), tab_v[:, :512])
    grads = grads[:, :256] + grads[:, 256:]
    grad_i = along_i(d, smooth)
    flux_i = [geo[0][b] * grad_i[b] for b in range(4)]
    flux = jnp.concatenate(
        [stack(geo[1]) * grads[:, :LANES], stack(geo[2]) * grads[:, LANES:]], axis=1
    )
    high, low = halves(flux)
    back = dot(jnp.concatenate([high, low], axis=0), tab_v[:, 512:768])
    back = back[: 4 * rows] + back[4 * rows :]
    back = back[:, :LANES] + back[:, LANES:]
    local = along_i(d.T, flux_i)
    local = [local[b] + back[rows * b : rows * b + rows] + mass[b] * smooth[b] for b in range(4)]

    for side in range(2):
        j_out(3, side)[...] = summed_j_face(local, ez, side)
        i_out(3, side)[...] = summed_i_face(local[3 * side], ez, side)

    @pl.when(is_last)
    def _():
        start = pl.multiple_of((me_g & 1) * h, q)
        dst = wrap_in.at[pl.ds(pl.multiple_of(me_g * u, q), u)]
        send(face_out.at[3, pl.ds(start, u)], dst, root_recv.at[1], (root, 0)).start()

    def wrap_target(a):
        return lax.rem(me_g + (a + ng), ng)

    def give_wrap(first):
        for turn, a in ((2, 1), (0, -1), (1, 0)):
            target = wrap_target(a)
            wanted = target == 0 if first else (target != 0) & (target != root)

            @pl.when(is_last & wanted)
            def _():
                send(j_out(3, 1), j_in(3, 1, turn), last_recv.at[3], (target, 0)).start()

    @pl.when(is_last)
    def _():
        send(j_out(3, 0), slot(root_in, 5, me_g), root_recv.at[1], (root, 0)).start()

    give_wrap(True)

    @pl.when(is_near)
    def _():
        send(j_out(3, 1), slot(root_in, 2, me_g), root_recv.at[0], (root, 0)).start()
        send(j_out(3, 0), slot(root_in, 3, me_g), root_recv.at[0], (root, 0)).start()

    @pl.when(is_mid | (me_d == nd - 7))
    def _():
        where = jnp.where(me_d == nd - 3, 4, 5 + place)
        send(j_out(3, 1), slot(root_in, where, me_g), root_recv.at[0], (root, 0)).start()

    @pl.when(is_mid)
    def _():
        send(j_out(3, 0), slot(root_in, 9 + place, me_g), root_recv.at[0], (root, 0)).start()

    give_i(3, [last_recv.at[0], last_recv.at[1]])
    give_j(3, 0, -1, last_recv.at[2])

    @pl.when(jnp.logical_not(is_last))
    def _():
        give_j(3, 1, 1, last_recv.at[3])

    @pl.when(is_first & (me_g != root))
    def _():
        send(j_out(3, 0), slot(root_in, 0, me_g), root_recv.at[0], (root, 0)).start()

    inside = assemble_inside(local, ez)

    @pl.when(jnp.logical_not(is_last))
    def _():
        gather_sides()

    drain(6 * q, side_recv.at[1])
    inverse = add_j_face([early_v[0, rows - ez :, c] for c in cut], ez, *turns(1, 0), 1)
    inverse = [1.0 / x for x in inverse]
    if rows > ez:
        kept = slice(0, rows - ez)
        inverse = [jnp.concatenate([early_v[2, kept, cut[b]], inverse[b]], axis=0) for b in range(4)]
    mixed = [early_v[1, :, c] for c in cut]

    def shared(side):
        lane = lane_of((q, LANES))
        ends = ((lane & 7) == 0) | ((lane & 7) == 7)
        share = jnp.where((lane < 64) & ((lane & 31) < 8), 0.0, jnp.where(ends, 0.5, 1.0))
        return share * pack_j_face(inverse, ez, side)

    @pl.when(is_first | is_near | is_mid)
    def _():
        side_out[pl.ds(0, q)] = shared(0)

    @pl.when(is_mid)
    def _():
        send(side_out.at[pl.ds(0, q)], slot(root_in, 10 + place, me_g), root_recv.at[0], (root, 0)).start()

    @pl.when(is_first & (me_g != root))
    def _():
        send(side_out.at[pl.ds(0, q)], slot(root_in, 1, me_g), root_recv.at[0], (root, 0)).start()

    @pl.when(is_near)
    def _():
        side_out[pl.ds(q, q)] = shared(1)
        dst = root_in.at[pl.ds(pl.multiple_of(q * (6 * ng + 2 * me_g), q), 2 * q)]
        send(side_out.at[pl.ds(0, 2 * q)], dst, root_recv.at[0], (root, 0)).start()

    dual = add_j_face(mixed, ez, *turns(2, 0), 1)
    norm_now = total_of([spread_res[b] * residual[b] * inverse[b] for b in range(4)])
    curvature = total_of([smooth[b] * local[b] for b in range(4)])
    cross = total_of([local[b] * dual[b] * inverse[b] for b in range(4)])
    share = [owned[b] * inverse[b] for b in range(4)]
    order = sorted(range(len(others)), key=lambda n: (others[n][1] != 1, others[n][1] != 0))

    def tell(row, table, sem, which=None):
        for n in order:
            a, b = others[n]
            if which is not None and which != (b == 1):
                continue
            send(part.at[pl.ds(row, 1)], table.at[pl.ds(n, 1)], sem, at(a, b)).start()

    lane = lane_of((1, LANES))
    early = jnp.where(lane < 32, norm_now, jnp.where(lane < 64, curvature, cross))
    part[pl.ds(0, 1)] = early

    @pl.when(jnp.logical_not(is_last))
    def _():
        tell(0, sums, sum_recv)

    @pl.when(is_last)
    def _():
        tell(0, sums, sum_recv, True)


    def hold(ref, side):
        for n, value in enumerate(turns(3, side)):
            ref[pl.ds(q * n, q)] = value

    def held(ref):
        return [ref[pl.ds(q * n, q)] for n in range(3)]

    @pl.when(owns_high)
    def _():
        drain(h, last_recv.at[0])
        high_v[...] = i_in(3, 0)[...]

    @pl.when(is_last)
    def _():
        high_v[...] = jnp.zeros_like(high_v)

    @pl.when(owns_next)
    def _():
        drain(3 * q, last_recv.at[2])
        hold(next_v, 0)

    @pl.when(jnp.logical_not(owns_next))
    def _():
        next_v[...] = jnp.zeros_like(next_v)

    mostly = add_i_face(inside, high_v[...], 1)
    mostly = add_j_face(mostly, ez, *held(next_v), 1)
    quad = stack([share[b] * mostly[b] * mostly[b] for b in range(4)])
    quad = jnp.sum(quad, axis=0, keepdims=True)
    part[pl.ds(1, 1)] = quad

    @pl.when(owns_low)
    def _():
        face = pack_i_face(mostly[0], 0)
        fit = pack_i_face(face_owned * inverse[0], 0)
        drain(h, last_recv.at[1])
        met = i_in(3, 1)[...]
        low_v[...] = met
        face = face + met
        part[pl.ds(1, 1)] = quad + jnp.sum(face * face * fit, axis=0, keepdims=True)

    @pl.when(jnp.logical_not(is_last))
    def _():
        tell(1, parts, part_recv)

    @pl.when(is_last)
    def _():
        tell(1, parts, part_recv)
        tell(0, sums, sum_recv, False)

    give_wrap(False)

    @pl.when(is_root)
    def _():
        slot(root_in, 0, me_g)[...] = j_out(3, 0)[...]
        slot(root_in, 1, me_g)[...] = side_out[pl.ds(0, q)]
        drain((19 * ng - 2) * q + ng // 2 * h, root_recv.at[0])

        def far(g):
            return wrap_in[pl.ds(u * g + (0 if g & 1 else h), q)]

        def across(g):
            return wrap_in[pl.ds(u * g + (q if g & 1 else 0), h)]

        def got(part_of, g):
            return root_in[pl.ds(q * (ng * part_of + g), q)]

        def paired(g, n):
            return root_in[pl.ds(q * (6 * ng + 2 * g + n), q)]

        spot = lane_of((q, LANES))
        seam = (spot >= 64) & ((spot & 31) >= 24)
        total = None
        groups = range(ng)
        seams = (
            ([got(3, g) + got(4, g) for g in groups], [paired(g, 0) for g in groups]),
            ([got(8, g) + got(9, g) for g in groups], [got(10, g) for g in groups]),
            ([got(11, g) + got(12, g) for g in groups], [got(13, g) for g in groups]),
            ([got(14, g) + got(15, g) for g in groups], [got(16, g) for g in groups]),
            ([got(17, g) + got(18, g) for g in groups], [got(19, g) for g in groups]),
        )

        def add_seams(total, seams):
            for faces, fits in seams:
                for g in groups:
                    face = faces[g] + jnp.where(seam, roll(faces[(g + 1) % ng], 88), 0.0)
                    term = face * face * fits[g]
                    total = term if total is None else total + term
            return total

        total = add_seams(total, seams)
        drain(ng * (u + q), root_recv.at[1])
        seams = (
            ([got(2, g) + got(5, g) for g in groups], [paired(g, 1) for g in groups]),
            ([got(0, g) + far(g) for g in groups], [got(1, g) for g in groups]),
        )
        total = add_seams(total, seams)
        for g in range(1, ng, 2):
            face = across(g) + across((g + 1) % ng)
            term = face * face * side_in[pl.ds(h * (g // 2), h)]
            for n in range(0, h, q):
                total = total + term[n : n + q]
        total = jnp.sum(total, axis=0, keepdims=True)
        parts[pl.ds(len(others), 1)] = total
        late_out[...] = total
        for n, shift in enumerate((0, ng - 1, 1)):
            g = lax.rem(me_g + shift, ng)
            prev_v[pl.ds(q * n, q)] = wrap_in[pl.ds(pl.multiple_of(u * g + h * (1 - (g & 1)), q), q)]

    heard = [(g, b) for b in range(nd) for g in range(ng) if (g, b) != (root, 0)]

    @pl.when(is_root)
    def _():
        for target in heard:
            send(late_out, parts.at[pl.ds(len(others), 1)], part_recv, target).start()

    @pl.when(jnp.logical_not(owns_low))
    def _():
        drain(h, last_recv.at[1])
        low_v[...] = i_in(3, 1)[...]

    @pl.when(is_last)
    def _():
        drain(h, last_recv.at[0])
        high_v[...] = i_in(3, 0)[...]

    @pl.when(jnp.logical_not(owns_next))
    def _():
        drain(3 * q, last_recv.at[2])
        hold(next_v, 0)

    @pl.when(jnp.logical_not(is_root))
    def _():
        drain(3 * q, last_recv.at[3])
        hold(prev_v, 1)

    applied = add_i_face(add_i_face(inside, low_v[...], 0), high_v[...], 1)
    applied = add_j_face(add_j_face(applied, ez, *held(prev_v), 0), ez, *held(next_v), 1)

    drain(len(others), sum_recv)
    everyone = early + jnp.sum(sums[pl.ds(0, len(others))], axis=0, keepdims=True)
    norm_now, curvature, cross = (everyone[:, 32 * n : 32 * n + 1] for n in range(3))
    step = norm_now / curvature
    shrunk = norm_now - 2.0 * step * cross
    scale = step * step
    moved = []
    for b, c in enumerate(cut):
        outs[0, :, c] = pair_v[1, :, c] + step * smooth[b]
        out = residual[b] - step * applied[b]
        outs[1, :, c] = out
        moved.append(out * inverse[b])

    @pl.when(is_root)
    def _():
        drain(len(others), part_recv)

    @pl.when(jnp.logical_not(is_root))
    def _():
        drain(len(others) + 1, part_recv)

    quad = part[pl.ds(1, 1)] + jnp.sum(parts[...], axis=0, keepdims=True)
    quad = jnp.sum(quad, axis=1, keepdims=True)
    ratio = (shrunk + scale * quad) / norm_now
    for b, c in enumerate(cut):
        outs[2, :, c] = moved[b] + ratio * smooth[b]
    common = 4 * span + 2 * len(others)
    roles = [
        (is_root, len(heard) - 6 * q),
        (is_first & jnp.logical_not(is_root), 2 * q - 6 * q),
        (is_near, 4 * q),
        (is_mid & is_relay, 21 * q),
        (is_mid & jnp.logical_not(is_relay), 3 * q),
        ((me_d == nd - 7) & is_relay, 19 * q),
        ((me_d == nd - 7) & jnp.logical_not(is_relay), q),
        ((me_d > 0) & (me_d < nd - 7) & is_relay, 18 * q),
        ((me_d > 0) & (me_d < nd - 7) & jnp.logical_not(is_relay), 0),
    ]
    skipped = sum(jnp.where(wrap_target(a) == root, 1, 0) for a in (-1, 0, 1))
    for n in range(4):
        roles.append((is_last & odd & (skipped == n), u + h + q - n * q))
        roles.append((is_last & jnp.logical_not(odd) & (skipped == n), u + q - n * q))

    for role, extra in roles:

        @pl.when(role)
        def _():
            drain(common + extra, send_sem)


def deliver(stacked, *refs):
    for n in range(3):
        pltpu.make_async_copy(stacked.at[n], refs[n], refs[3]).start()
    pltpu.make_async_copy(stacked, stacked, refs[3]).wait()


def on_device(solution, residual, direction, geometry, mass):
    dims = solution.shape
    ng, nd = lax.axis_size("group"), lax.axis_size("dev")
    ez, points = dims[2], dims[3]
    rows = dims[0] * dims[1] * ez
    flat = (rows, points)
    f32, bf16 = jnp.float32, jnp.bfloat16
    table = jnp.asarray(tables())
    h, q = rows // 2, ez // 2
    u, q8 = h + q, 8
    spare = max(20 * ng * q + ng * (u + h), 4 * (2 * h + 6 * q) + 3 * ng * nd + 32 * q)
    bulk = (2 * rows * points * 4 + 4 * rows * points * 2 + table.size * 2) // (4 * LANES)
    spare = -(-spare // q8) * q8
    stacked = pl.pallas_call(
        functools.partial(kernel, ng, nd, ez),
        out_shape=pltpu.VMEM((3,) + flat, f32),
        in_specs=[pl.BlockSpec(memory_space=pltpu.HBM)] * 6,
        out_specs=pl.BlockSpec(memory_space=pltpu.VMEM),
        scratch_shapes=[
            pltpu.VMEM((2,) + flat, f32),
            pltpu.VMEM(flat, f32),
            pltpu.VMEM((4,) + flat, bf16),
            pltpu.VMEM(table.shape, bf16),
            pltpu.VMEM((3,) + flat, f32),
            pltpu.VMEM((4, 2 * u, LANES), f32),
            pltpu.VMEM((spare, LANES), f32),
            pltpu.VMEM((ng * u, LANES), f32),
            pltpu.VMEM((20 * ng * q, LANES), f32),
            pltpu.VMEM((6 * q, LANES), f32),
            pltpu.VMEM((ng // 2 * h, LANES), f32),
            pltpu.VMEM((h, LANES), f32),
            pltpu.VMEM((3 * q, LANES), f32),
            pltpu.VMEM((3 * q, LANES), f32),
            pltpu.VMEM((h, LANES), f32),
            pltpu.VMEM((h, LANES), f32),
            pltpu.VMEM((2, LANES), f32),
            pltpu.VMEM((ng * nd, LANES), f32),
            pltpu.VMEM((ng * nd, LANES), f32),
            pltpu.VMEM((1, LANES), f32),
            pltpu.VMEM((bulk, LANES), f32),
            pltpu.SemaphoreType.DMA((2,)),
            pltpu.SemaphoreType.DMA,
            pltpu.SemaphoreType.DMA,
            pltpu.SemaphoreType.DMA((2,)),
            pltpu.SemaphoreType.DMA((4,)),
            pltpu.SemaphoreType.DMA((2,)),
            pltpu.SemaphoreType.DMA((3,)),
            pltpu.SemaphoreType.DMA,
            pltpu.SemaphoreType.DMA,
            pltpu.SemaphoreType.REGULAR,
        ],
        compiler_params=pltpu.CompilerParams(collective_id=0, has_side_effects=True, vmem_limit_bytes=8 << 20),
    )(
        pltpu.with_memory_space_constraint(solution.reshape(flat), pltpu.HBM),
        pltpu.with_memory_space_constraint(residual.reshape(flat), pltpu.HBM),
        pltpu.with_memory_space_constraint(direction.reshape(flat), pltpu.HBM),
        pltpu.with_memory_space_constraint(geometry.reshape((3,) + flat), pltpu.HBM),
        pltpu.with_memory_space_constraint(mass.reshape(flat), pltpu.HBM),
        pltpu.with_memory_space_constraint(table, pltpu.HBM),
    )
    outs = pl.pallas_call(
        deliver,
        out_shape=[jax.ShapeDtypeStruct(flat, f32)] * 3,
        in_specs=[pl.BlockSpec(memory_space=pl.ANY)],
        out_specs=[pl.BlockSpec(memory_space=pltpu.HBM)] * 3,
        scratch_shapes=[pltpu.SemaphoreType.DMA],
        compiler_params=pltpu.CompilerParams(vmem_limit_bytes=8 << 20),
    )(stacked)
    return tuple(x.reshape(dims) for x in outs)


def solution(mesh):
    spec = P("group", "dev", None, None)
    return jax.shard_map(
        on_device,
        mesh=mesh,
        in_specs=(spec, spec, spec, P(None, "group", "dev", None, None), spec),
        out_specs=(spec, spec, spec),
        check_vma=False,
    )
```
